32 devices in a mesh: dp: 4 (over y, z), tp: 8 (over x, core).
Axes of the slice: x: 4, y: 2, z: 2, core: 2. Of those that a mesh axis runs over, the one named last changes fastest.
The devices are a block of a 4x4x8 slice.
Arguments:
- x_seq: bfloat16 [24, 2048, 2048], P('dp', 'tp'), parts along dimension 0
- ln_gain: float32 [2048], replicated
- ln_bias: float32 [2048], replicated
- w_qkv: bfloat16 [2048, 8, 3, 256], P(None, 'tp')
- w_out: bfloat16 [2048, 2048], P('tp')
- w_up: bfloat16 [2048, 8192], P(None, 'tp')
- w_down: bfloat16 [8192, 2048], P('tp')
Outputs:
- output: bfloat16 [24, 2048, 2048], P('dp', 'tp'), parts along dimension 0
There are 4 independent parts. The reference program is written for one: setup_inputs(seed, part) draws one part's arguments, and reference() takes and returns one part's arrays. A program takes and returns all parts, laid end to end along the dimension named above; an argument that names none is the same for every part.
All inputs are finite; a program needn't handle non-finite values.
Results may differ from the reference program's by a relative error of at most 0.0116155.
Values are sent between devices in bfloat16 or wider.
A program may use at most 768 MiB of HBM per device.

```python
import jax
import jax.numpy as jnp
from jax import lax

D = 2048
HEADS = 8
KV_HEADS = 8
HEAD = 256
FF = 8192
BATCH = 6
SEQ = 2048

LN_EPS = 1e-5
GROUP_Q = HEADS // KV_HEADS


def normal_weights(key_w, shape, fan_in):
    return (jax.random.normal(key_w, shape, jnp.float32) * fan_in ** -0.5).astype(jnp.bfloat16)


def setup_inputs(seed: int = 0, part: int = 0) -> dict:
    root_key = jax.random.key(seed)
    key_x, key_c, key_g, key_b, key_qkv, key_o, key_up, key_dn = jax.random.split(root_key, 8)
    key_x = jax.random.fold_in(key_x, part)
    key_c = jax.random.fold_in(key_c, part)
    noise = jax.random.normal(key_x, (BATCH, SEQ, D), jnp.float32)
    shared = jax.random.normal(key_c, (BATCH, 1, D), jnp.float32)
    x_seq = ((noise + shared) * 0.7071).astype(jnp.bfloat16)
    ln_gain = 1.0 + 0.5 * jax.random.normal(key_g, (D,), jnp.float32)
    ln_bias = 0.5 * jax.random.normal(key_b, (D,), jnp.float32)
    w_qkv = normal_weights(key_qkv, (D, KV_HEADS, GROUP_Q + 2, HEAD), D)
    w_out = normal_weights(key_o, (HEADS * HEAD, D), HEADS * HEAD)
    w_up = normal_weights(key_up, (D, FF), D)
    w_down = normal_weights(key_dn, (FF, D), FF)
    return {"x_seq": x_seq, "ln_gain": ln_gain, "ln_bias": ln_bias, "w_qkv": w_qkv,
            "w_out": w_out, "w_up": w_up, "w_down": w_down}


def layer_norm(x_f32, ln_gain, ln_bias):
    row_mean = jnp.mean(x_f32, axis=-1, keepdims=True)
    centered = x_f32 - row_mean
    variance = jnp.mean(centered * centered, axis=-1, keepdims=True)
    return centered * lax.rsqrt(variance + LN_EPS) * ln_gain + ln_bias


def reference(x_seq, ln_gain, ln_bias, w_qkv, w_out, w_up, w_down):
    tokens = x_seq.reshape(BATCH * SEQ, D)
    normed = layer_norm(tokens.astype(jnp.float32), ln_gain, ln_bias).astype(jnp.bfloat16)
    proj_qkv = jnp.dot(normed, w_qkv.reshape(D, KV_HEADS * (GROUP_Q + 2) * HEAD),
                       preferred_element_type=jnp.float32).astype(jnp.bfloat16)
    proj_qkv = proj_qkv.reshape(BATCH, SEQ, KV_HEADS, GROUP_Q + 2, HEAD)
    proj_qkv = proj_qkv.transpose(0, 2, 3, 1, 4).reshape(BATCH * KV_HEADS, GROUP_Q + 2, SEQ, HEAD)
    causal = jnp.arange(SEQ)[:, None] >= jnp.arange(SEQ)[None, :]

    def one_group(group_item):
        query_rows = group_item[:GROUP_Q].astype(jnp.float32)
        key_rows = group_item[GROUP_Q].astype(jnp.float32)
        value_rows = group_item[GROUP_Q + 1].astype(jnp.float32)
        scores = jnp.einsum("jsh,th->jst", query_rows, key_rows) * (HEAD ** -0.5)
        scores = jnp.where(causal, scores, -jnp.inf)
        attn_prob = jax.nn.softmax(scores, axis=-1).astype(jnp.bfloat16)
        context = jnp.einsum("jst,th->jsh", attn_prob.astype(jnp.float32), value_rows)
        return context.astype(jnp.bfloat16)

    context = lax.map(one_group, proj_qkv)
    context = context.reshape(BATCH, KV_HEADS, GROUP_Q, SEQ, HEAD).transpose(0, 3, 1, 2, 4)
    context = context.reshape(BATCH * SEQ, HEADS * HEAD)
    attn_part = jnp.dot(context, w_out, preferred_element_type=jnp.float32)
    hidden = jnp.dot(normed, w_up, preferred_element_type=jnp.float32)
    activated = jax.nn.gelu(hidden, approximate=False).astype(jnp.bfloat16)
    mlp_part = jnp.dot(activated, w_down, preferred_element_type=jnp.float32)
    branch = (attn_part + mlp_part).astype(jnp.bfloat16)
    out_rows = (tokens.astype(jnp.float32) + branch.astype(jnp.float32)).astype(jnp.bfloat16)
    return out_rows.reshape(BATCH, SEQ, D)
```

```python
import jax
import jax.numpy as jnp
from jax import lax
from jax.sharding import PartitionSpec as P

LN_EPS = 1e-5


def layer_norm(x_f32, ln_gain, ln_bias):
    row_mean = jnp.mean(x_f32, axis=-1, keepdims=True)
    centered = x_f32 - row_mean
    variance = jnp.mean(centered * centered, axis=-1, keepdims=True)
    return centered * lax.rsqrt(variance + LN_EPS) * ln_gain + ln_bias


def solution(mesh):
    def local_layer(x_blk, ln_gain, ln_bias, w_qkv, w_out, w_up, w_down):
        kv_local, group_width, head_dim = w_qkv.shape[1:]
        group_q = group_width - 2
        w_heads = w_out.reshape(kv_local, group_q, head_dim, w_out.shape[-1])

        def one_sequence(x_seq):
            x_full = lax.all_gather(x_seq, "tp", axis=0, tiled=True)
            seq_len = x_full.shape[0]
            normed = layer_norm(x_full.astype(jnp.float32), ln_gain, ln_bias).astype(jnp.bfloat16)
            proj_qkv = jnp.einsum("sd,dgjh->gjsh", normed, w_qkv,
                                  preferred_element_type=jnp.float32).astype(jnp.bfloat16)
            queries = proj_qkv[:, :group_q]
            key_rows = proj_qkv[:, group_q]
            value_rows = proj_qkv[:, group_q + 1]
            scores = jnp.einsum("gjsh,gth->gjst", queries, key_rows,
                                preferred_element_type=jnp.float32) * (head_dim ** -0.5)
            causal = (lax.broadcasted_iota(jnp.int32, (seq_len, seq_len), 0)
                      >= lax.broadcasted_iota(jnp.int32, (seq_len, seq_len), 1))
            scores = jnp.where(causal, scores, -jnp.inf)
            attn_prob = jax.nn.softmax(scores, axis=-1).astype(jnp.bfloat16)
            context = jnp.einsum("gjst,gth->gjsh", attn_prob, value_rows,
                                 preferred_element_type=jnp.float32).astype(jnp.bfloat16)
            attn_part = jnp.einsum("gjsh,gjhd->sd", context, w_heads, preferred_element_type=jnp.float32)
            hidden = jnp.einsum("sd,df->sf", normed, w_up, preferred_element_type=jnp.float32)
            activated = jax.nn.gelu(hidden, approximate=False).astype(jnp.bfloat16)
            mlp_part = jnp.einsum("sf,fd->sd", activated, w_down, preferred_element_type=jnp.float32)
            branch_part = (attn_part + mlp_part).astype(jnp.bfloat16)
            branch = lax.psum_scatter(branch_part, "tp", scatter_dimension=0, tiled=True)
            return (x_seq.astype(jnp.float32) + branch.astype(jnp.float32)).astype(jnp.bfloat16)

        return jnp.stack([one_sequence(x_blk[i]) for i in range(x_blk.shape[0])])

    return jax.shard_map(
        local_layer, mesh=mesh,
        in_specs=(P("dp", "tp", None), P(), P(), P(None, "tp", None, None),
                  P("tp", None), P(None, "tp"), P("tp", None)),
        out_specs=P("dp", "tp", None), check_vma=False)
```

```python
import functools

import jax
import jax.numpy as jnp
from jax import lax
from jax.experimental import pallas as pl
from jax.experimental.pallas import tpu as pltpu
from jax.sharding import PartitionSpec as P

LN_EPS = 1e-5
MESH = pl.DeviceIdType.MESH
BF16 = jnp.bfloat16
F32 = jnp.float32
LOG2E = 1.4426950408889634
VMEM_LIMIT = 67_043_328


def layer_kernel(dims, x, gain, bias, w_qkv, w_out, w_up, w_dn,
                 y, xg, part, r1, fin, fin2,
                 wq, wu, wd, n, qkv, xt, ho, stage, r1v, addv, acc, m_s, l_s,
                 own_s, own_r, sib_s, sib_r, fwd_s, fwd_r, w_l, w_s, w_r,
                 h1_s, h1_r, h2n_s, h2n_r, h2d_s, h2d_r, sp_s, sp_r,
                 xt_sem, st_sem, ld_sem, fl_sem, fo_sem):
    chips, n_seq, rows, d_model, head, ff, chunk, ln_rows = dims
    ns = n_seq // 2
    half = rows // 2
    blk = 2 * rows
    scale = LOG2E * head ** -0.5

    me = lax.axis_index("tp")
    c, k = lax.div(me, 2), lax.rem(me, 2)
    o = 1 - k
    right, left, opp = lax.rem(c + 1, chips), lax.rem(c + chips - 1, chips), lax.rem(c + 2, chips)

    def dev(chip, core):
        return {"tp": 2 * chip + core}

    def row(chip, core, extra=0):
        return pl.multiple_of((2 * chip + core) * rows + extra, half)

    def remote(src, dst, send, recv, to):
        return pltpu.make_async_remote_copy(src_ref=src, dst_ref=dst, send_sem=send, recv_sem=recv,
                                            device_id=to, device_id_type=MESH)

    def own(s, kk, d):
        return remote(x.at[2 * s + kk], xg.at[s, pl.ds(row(c, k), rows)],
                      own_s.at[s, kk, d], own_r.at[s, k, d], dev(right if d == 0 else left, kk))

    def own_in(s, j, d):
        blk_ref = xg.at[s, pl.ds(row(left if d == 0 else right, j), rows)]
        return remote(blk_ref, blk_ref, own_s.at[s, j, d], own_r.at[s, j, d], dev(c, k))

    def sib(s):
        return remote(x.at[2 * s + o], xg.at[s, pl.ds(row(c, k), rows)], sib_s.at[s], sib_r.at[s], dev(c, o))

    def sib_in(s):
        ref = xg.at[s, pl.ds(row(c, o), rows)]
        return remote(ref, ref, sib_s.at[s], sib_r.at[s], dev(c, o))

    def fwd(s, j, d):
        at = row(left, j) if d == 0 else row(right, j, half)
        ref = xg.at[s, pl.ds(at, half)]
        return remote(ref, ref, fwd_s.at[s, j, d], fwd_r.at[s, j, d], dev(right if d == 0 else left, k))

    def fwd_in(s, j, d):
        ref = xg.at[s, pl.ds(row(opp, j, d * half), half)]
        return remote(ref, ref, fwd_s.at[s, j, d], fwd_r.at[s, j, d], dev(c, k))

    def hop1(s, j, d):
        return remote(part.at[s, pl.ds(row(opp, j, d * half), half)], r1.at[s, d, j],
                      h1_s.at[s, j, d], h1_r.at[s, j, d], dev(right if d == 0 else left, k))

    def hop1_in(s, j, d):
        return remote(r1.at[s, d, j], r1.at[s, d, j], h1_s.at[s, j, d], h1_r.at[s, j, d], dev(c, k))

    def hop2n(s, j, d):
        to = right if d == 0 else left
        off = (1 - d) * half
        return remote(part.at[s, pl.ds(row(to, j, off), half)], fin.at[2 * s + k, d, pl.ds(off, half)],
                      h2n_s.at[s, j, d], h2n_r.at[s, k, d], dev(to, j))

    def hop2n_in(s, kk, d):
        ref = fin.at[2 * s + kk, d, pl.ds((1 - d) * half, half)]
        return remote(ref, ref, h2n_s.at[s, 0, d], h2n_r.at[s, kk, d], dev(c, k))

    def hop2d(s, j, d):
        to = right if d == 0 else left
        return remote(addv.at[lax.rem(s, 2), d, j], fin.at[2 * s + k, d, pl.ds(d * half, half)],
                      h2d_s.at[s, j, d], h2d_r.at[s, k, d], dev(to, j))

    def hop2d_in(s, kk, d):
        ref = fin.at[2 * s + kk, d, pl.ds(d * half, half)]
        return remote(ref, ref, h2d_s.at[s, 0, d], h2d_r.at[s, kk, d], dev(c, k))

    def sibp(s):
        return remote(part.at[s, pl.ds(row(c, o), rows)], fin2.at[s], sp_s.at[s], sp_r.at[s], dev(c, o))

    def sibp_in(s):
        return remote(fin2.at[s], fin2.at[s], sp_s.at[s], sp_r.at[s], dev(c, o))

    both = [(j, d) for j in range(2) for d in range(2)]

    def weight_pairs():
        for t in range(3):
            yield w_qkv.at[t], wq.at[:, pl.ds(pl.multiple_of((2 * t + k) * head, head), head)], \
                wq.at[:, pl.ds(pl.multiple_of((2 * t + o) * head, head), head)]
        yield w_up, wu.at[:, pl.ds(pl.multiple_of(k * ff, ff), ff)], wu.at[:, pl.ds(pl.multiple_of(o * ff, ff), ff)]
        yield w_out, wd.at[pl.ds(pl.multiple_of(k * head, head), head)], \
            wd.at[pl.ds(pl.multiple_of(o * head, head), head)]
        yield w_dn, wd.at[pl.ds(pl.multiple_of(2 * head + k * ff, head), ff)], \
            wd.at[pl.ds(pl.multiple_of(2 * head + o * ff, head), ff)]

    def weights_local(i, src, mine):
        return pltpu.make_async_copy(src, mine, w_l.at[i])

    def wait_weights(lo, hi):
        for i, (src, mine, theirs) in enumerate(weight_pairs()):
            if lo <= i < hi:
                weights_local(i, src, mine).wait()
                remote(theirs, theirs, w_s.at[i], w_r.at[i], dev(c, o)).wait_recv()

    barrier = pltpu.get_barrier_semaphore()
    for to in (dev(c, o), dev(right, 0), dev(right, 1), dev(left, 0), dev(left, 1)):
        pl.semaphore_signal(barrier, inc=1, device_id=to, device_id_type=MESH)
    pl.semaphore_wait(barrier, 5)

    for kk in (k, o):
        for d in range(2):
            own(0, kk, d).start()
    sib(0).start()
    for i, (src, mine, theirs) in enumerate(weight_pairs()):
        weights_local(i, src, mine).start()
        remote(src, mine, w_s.at[i], w_r.at[i], dev(c, o)).start()
    for s in range(1, ns):
        sib(s).start()
    for j in (k, o):
        for d in range(2):
            own_in(0, j, d).wait_recv()
            fwd(0, j, d).start()
    for kk in (k, o):
        for d in range(2):
            own(1, kk, d).start()
    for d in range(2):
        own(2, k, d).start()

    def tile_start(s, slot, cb):
        for j in range(2):
            mine = (cb == c) & (k == j)
            dst = xt.at[slot, pl.ds(j * rows, rows)]

            @pl.when(mine)
            def _():
                pltpu.make_async_copy(x.at[2 * s + k], dst, xt_sem.at[slot, j]).start()

            @pl.when(jnp.logical_not(mine))
            def _():
                pltpu.make_async_copy(xg.at[s, pl.ds(row(cb, j), rows)], dst, xt_sem.at[slot, j]).start()

    def tile_wait(s, slot, cb):
        for j in range(2):
            pltpu.make_async_copy(xg.at[s, pl.ds(row(cb, j), rows)], xt.at[slot, pl.ds(j * rows, rows)],
                                  xt_sem.at[slot, j]).wait()

    def block_a(i):
        return lax.rem(c + jnp.where(i == 0, 0, jnp.where(i == 1, 3, jnp.where(i == 2, 1, 2))), chips)

    def block_b(i):
        return lax.rem(c + jnp.where(i == 0, 2, jnp.where(i == 1, 1, jnp.where(i == 2, 3, 0))), chips)

    def project(slot, cb):
        base = pl.multiple_of(cb * blk, blk)

        def norm(g, _):
            r0 = pl.multiple_of(g * ln_rows, ln_rows)
            v = xt[slot, pl.ds(r0, ln_rows), :].astype(F32)
            mean = jnp.mean(v, axis=-1, keepdims=True)
            cen = v - mean
            var = jnp.mean(cen * cen, axis=-1, keepdims=True)
            out = cen * lax.rsqrt(var + LN_EPS) * gain[...] + bias[...]
            n[pl.ds(pl.multiple_of(base + r0, ln_rows), ln_rows), :] = out.astype(BF16)
            return 0

        lax.fori_loop(0, blk // ln_rows, norm, 0)

        def proj(g, _):
            cols = pl.ds(pl.multiple_of(g * 2 * head, 2 * head), 2 * head)
            qkv[pl.ds(base, blk), cols] = jnp.dot(
                n[pl.ds(base, blk), :], wq[:, cols], preferred_element_type=F32).astype(BF16)
            return 0

        lax.fori_loop(0, 3, proj, 0)

    def dot_t(a, b):
        return lax.dot_general(a, b, (((1,), (1,)), ((), ())), preferred_element_type=F32)

    def attend(cb):
        base = pl.multiple_of(cb * blk, blk)
        mine = pl.ds(base, blk)
        causal = (lax.broadcasted_iota(jnp.int32, (blk, blk), 0)
                  >= lax.broadcasted_iota(jnp.int32, (blk, blk), 1))
        for h in range(2):
            q, key, val = (qkv[mine, pl.ds((2 * t + h) * head, head)] for t in range(3))
            sc = jnp.where(causal, dot_t(q, key), -jnp.inf)
            top = jnp.max(sc, axis=-1, keepdims=True)
            p = jnp.exp2((sc - top) * scale)
            m_s[h] = top
            l_s[h] = jnp.sum(p, axis=-1, keepdims=True)
            acc[h] = jnp.dot(p.astype(BF16), val, preferred_element_type=F32)

        def earlier(t, _):
            there = pl.ds(pl.multiple_of(t * blk, blk), blk)
            for h in range(2):
                q = qkv[mine, pl.ds(h * head, head)]
                key = qkv[there, pl.ds((2 + h) * head, head)]
                val = qkv[there, pl.ds((4 + h) * head, head)]
                sc = dot_t(q, key)
                old = m_s[h]
                top = jnp.maximum(old, jnp.max(sc, axis=-1, keepdims=True))
                p = jnp.exp2((sc - top) * scale)
                fade = jnp.exp2((old - top) * scale)
                m_s[h] = top
                l_s[h] = l_s[h] * fade + jnp.sum(p, axis=-1, keepdims=True)
                acc[h] = acc[h] * fade + jnp.dot(p.astype(BF16), val, preferred_element_type=F32)
            return 0

        lax.fori_loop(0, cb, earlier, 0)
        for h in range(2):
            ho[:, pl.ds(h * head, head)] = (acc[h] / l_s[h]).astype(BF16)

    def stage_copy(s, cb):
        return pltpu.make_async_copy(stage, part.at[s, pl.ds(pl.multiple_of(cb * blk, blk), blk)], st_sem)

    def mlp(s, i, cb):
        base = pl.multiple_of(cb * blk, blk)

        def up(g, _):
            hid = jnp.dot(n[pl.ds(base, blk), :], wu[:, pl.ds(pl.multiple_of(g * chunk, chunk), chunk)],
                          preferred_element_type=F32)
            act = 0.5 * hid * (1.0 + lax.erf(hid * 0.7071067811865476))
            ho[:, pl.ds(pl.multiple_of(2 * head + g * chunk, 2 * head), chunk)] = act.astype(BF16)
            return 0

        lax.fori_loop(0, 2 * ff // chunk, up, 0)

        @pl.when((s > 0) | (i > 0))
        def _():
            stage_copy(s, cb).wait()

        def down(g, _):
            cols = pl.ds(pl.multiple_of(g * chunk, chunk), chunk)
            stage[:, cols] = jnp.dot(ho[...], wd[:, cols], preferred_element_type=F32).astype(BF16)
            return 0

        lax.fori_loop(0, d_model // chunk, down, 0)
        stage_copy(s, cb).start()

    def add_and_send(s):
        slot = lax.rem(s, 2)

        @pl.when(s >= 2)
        def _():
            for j, d in both:
                hop2d(s - 2, j, d).wait_send()

        def loads(j, d):
            at = row(right, j) if d == 0 else row(left, j, half)
            return (pltpu.make_async_copy(part.at[s, pl.ds(at, half)], addv.at[slot, d, j], ld_sem.at[0, j, d]),
                    pltpu.make_async_copy(r1.at[s, d, j], r1v.at[d, j], ld_sem.at[1, j, d]))

        for j, d in both:
            hop1_in(s, j, d).wait_recv()
            for ld in loads(j, d):
                ld.start()
        for j, d in both:
            for ld in loads(j, d):
                ld.wait()

            def add(g, _):
                rr = pl.ds(pl.multiple_of(g * ln_rows, ln_rows), ln_rows)
                addv[slot, d, j, rr, :] = (addv[slot, d, j, rr, :].astype(F32)
                                           + r1v[d, j, rr, :].astype(F32)).astype(BF16)
                return 0

            lax.fori_loop(0, half // ln_rows, add, 0)
            hop2d(s, j, d).start()

    def final_loads(s, rel):
        kk = k if rel == 0 else o
        b0 = rel * 4 * rows
        srcs = (x.at[2 * s + kk],
                part.at[s, pl.ds(row(c, k), rows)] if rel == 0 else fin2.at[s],
                fin.at[2 * s + kk, 0], fin.at[2 * s + kk, 1])
        return [pltpu.make_async_copy(src, n.at[pl.ds(b0 + a * rows, rows)], fl_sem.at[rel, a])
                for a, src in enumerate(srcs)]

    def final_store(s, rel):
        return pltpu.make_async_copy(n.at[pl.ds(rel * 4 * rows, rows)], y.at[2 * s + (k if rel == 0 else o)],
                                     fo_sem.at[rel])

    def final(s):
        for rel in range(2):
            kk = k if rel == 0 else o
            for d in range(2):
                hop2n_in(s, kk, d).wait_recv()
                hop2d_in(s, kk, d).wait_recv()
            if rel == 1:
                sibp_in(s).wait_recv()

            @pl.when(s > 0)
            def _():
                final_store(s, rel).wait()

            for ld in final_loads(s, rel):
                ld.start()
        for rel in range(2):
            for ld in final_loads(s, rel):
                ld.wait()

            def total(g, _):
                def piece(a):
                    return n[pl.ds(pl.multiple_of(rel * 4 * rows + a * rows + g * ln_rows, ln_rows), ln_rows), :]

                branch = (piece(1).astype(F32) + piece(2).astype(F32) + piece(3).astype(F32)).astype(BF16)
                res = (piece(0).astype(F32) + branch.astype(F32)).astype(BF16)
                n[pl.ds(pl.multiple_of(rel * 4 * rows + g * ln_rows, ln_rows), ln_rows), :] = res
                return 0

            lax.fori_loop(0, rows // ln_rows, total, 0)
            final_store(s, rel).start()

    wait_weights(0, 3)

    def sequence(s, _):
        sib_in(s).wait_recv()
        tile_start(s, 0, block_a(0))

        def stage_a(i, _):
            slot = lax.rem(i, 2)
            cb = block_a(i)

            @pl.when(i == 3)
            def _():
                for j, d in both:
                    fwd_in(s, j, d).wait_recv()
                tile_start(s, slot, cb)

            tile_wait(s, slot, cb)

            @pl.when(i < 2)
            def _():
                tile_start(s, 1 - slot, block_a(i + 1))

            project(slot, cb)
            return 0

        lax.fori_loop(0, 4, stage_a, 0)

        @pl.when(s == 0)
        def _():
            wait_weights(3, 6)

        def stage_b(i, _):
            cb = block_b(i)
            attend(cb)
            mlp(s, i, cb)

            @pl.when((s == 0) & (i == 2))
            def _():
                for j, d in both:
                    own_in(1, j, d).wait_recv()
                    fwd(1, j, d).start()
                for d in range(2):
                    own(2, o, d).start()

            @pl.when((s < 2) & (i == 3))
            def _():
                for j, d in both:
                    hop1(s, j, d).start()

            @pl.when((s == 1) & (i == 1))
            def _():
                for j, d in both:
                    own_in(2, j, d).wait_recv()
                    fwd(2, j, d).start()
                for j, d in both:
                    hop2n(0, j, d).start()

            @pl.when((s == 1) & (i == 2))
            def _():
                add_and_send(0)

            @pl.when((s == 1) & (i == 3))
            def _():
                for j, d in both:
                    hop2n(1, j, d).start()

            @pl.when((s > 0) & (i == 1))
            def _():
                sibp(s - 1).start()

            @pl.when((s == 2) & (i == 1))
            def _():
                for j, d in both:
                    hop1(2, j, d).start()

            return 0

        lax.fori_loop(0, 4, stage_b, 0)
        return 0

    lax.fori_loop(0, ns, sequence, 0)

    last = ns - 1
    stage_copy(last, block_b(3)).wait()
    add_and_send(1)
    for j, d in both:
        hop2n(last, j, d).start()
    sibp(last).start()
    final(0)
    add_and_send(last)
    final(1)
    final(last)
    for rel in range(2):
        final_store(last, rel).wait()

    for s in range(ns):
        for j, d in both:
            own(s, j, d).wait_send()
            fwd(s, j, d).wait_send()
            hop1(s, j, d).wait_send()
            hop2n(s, j, d).wait_send()
            if s >= ns - 2:
                hop2d(s, j, d).wait_send()
        sib(s).wait_send()
        sibp(s).wait_send()
    for i, (src, mine, theirs) in enumerate(weight_pairs()):
        remote(src, mine, w_s.at[i], w_r.at[i], dev(c, o)).wait_send()


def solution(mesh):
    tp = mesh.shape["tp"]

    def local_layer(x_blk, ln_gain, ln_bias, w_qkv, w_out, w_up, w_down):
        n_seq, rows, d_model = x_blk.shape
        head = w_qkv.shape[3]
        ff = w_up.shape[1]
        chips, ns, seq, blk, half = tp // 2, n_seq // 2, rows * tp, 2 * rows, rows // 2
        chunk = min(512, d_model, ff)
        ln_rows = min(32, half)
        dims = (chips, n_seq, rows, d_model, head, ff, chunk, ln_rows)
        dma = pltpu.SemaphoreType.DMA
        anyspace = pl.BlockSpec(memory_space=pl.ANY)
        vmem = pl.BlockSpec(memory_space=pltpu.VMEM)

        def hbm(*shape):
            return jax.ShapeDtypeStruct(shape, BF16)

        outs = pl.pallas_call(
            functools.partial(layer_kernel, dims),
            name="layer",
            out_shape=(hbm(n_seq, rows, d_model), hbm(ns, seq, d_model), hbm(ns, seq, d_model),
                       hbm(ns, 2, 2, half, d_model), hbm(n_seq, 2, rows, d_model), hbm(ns, rows, d_model)),
            in_specs=[anyspace, vmem, vmem, anyspace, anyspace, anyspace, anyspace],
            out_specs=(anyspace,) * 6,
            scratch_shapes=[
                pltpu.VMEM((d_model, 6 * head), BF16),
                pltpu.VMEM((d_model, 2 * ff), BF16),
                pltpu.VMEM((2 * head + 2 * ff, d_model), BF16),
                pltpu.VMEM((seq, d_model), BF16),
                pltpu.VMEM((seq, 6 * head), BF16),
                pltpu.VMEM((2, blk, d_model), BF16),
                pltpu.VMEM((blk, 2 * head + 2 * ff), BF16),
                pltpu.VMEM((blk, d_model), BF16),
                pltpu.VMEM((2, 2, half, d_model), BF16),
                pltpu.VMEM((2, 2, 2, half, d_model), BF16),
                pltpu.VMEM((2, blk, head), F32),
                pltpu.VMEM((2, blk, 1), F32),
                pltpu.VMEM((2, blk, 1), F32),
                dma((ns, 2, 2)), dma((ns, 2, 2)), dma((ns,)), dma((ns,)), dma((ns, 2, 2)), dma((ns, 2, 2)),
                dma((6,)), dma((6,)), dma((6,)),
                dma((ns, 2, 2)), dma((ns, 2, 2)), dma((ns, 2, 2)), dma((ns, 2, 2)), dma((ns, 2, 2)),
                dma((ns, 2, 2)), dma((ns,)), dma((ns,)),
                dma((2, 2)), dma, dma((2, 2, 2)), dma((2, 4)), dma((2,)),
            ],
            compiler_params=pltpu.CompilerParams(
                collective_id=0, has_side_effects=True, vmem_limit_bytes=VMEM_LIMIT),
        )(x_blk, ln_gain.reshape(1, d_model), ln_bias.reshape(1, d_model),
          jnp.transpose(w_qkv[:, 0], (1, 0, 2)), w_out, w_up, w_down)
        return outs[0]

    return jax.shard_map(
        local_layer, mesh=mesh,
        in_specs=(P("dp", "tp", None), P(), P(), P(None, "tp", None, None),
                  P("tp", None), P(None, "tp"), P("tp", None)),
        out_specs=P("dp", "tp", None), check_vma=False)
```

```python
import functools

import jax
import jax.numpy as jnp
from jax import lax
from jax.experimental import pallas as pl
from jax.experimental.pallas import tpu as pltpu
from jax.sharding import PartitionSpec as P

LN_EPS = 1e-5
MESH = pl.DeviceIdType.MESH
BF16 = jnp.bfloat16
F32 = jnp.float32
LOG2E = 1.4426950408889634
VMEM_LIMIT = 67_043_328

PHASES = (("a", 0), ("a", 1), ("m", 0), ("m", 1), ("a", 2), ("m", 2))
QKV, UP0, UP1, DN0, DN1, OUT = range(6)


def layer_kernel(dims, x, gain, bias, w_qkv, w_out, w_up, w_dn,
                 y, xg, nbuf, obuf, sibin, mid, fin,
                 wq, wu, wd, nt, xt, qkv, ot, ho, stage, cin, tbuf, acc, m_s, l_s,
                 w_l, wx_s, wx_r, wf_s, wf_r, xm_s, xm_r, xp_s, xp_r, xf_s, xf_r, xd_s, xd_r,
                 sp_s, sp_r, t_s, t_r, p_s, p_r,
                 xt_sem, no_sem, oo_sem, nl_sem, ol_sem, cl_sem, yo_sem):
    span, rows, d_model, head, ff, chunk, ln_rows = dims
    half = rows // 2
    blk = 2 * rows
    scale = LOG2E * head ** -0.5

    g, me = lax.axis_index("dp"), lax.axis_index("tp")
    c, j = lax.div(me, 2), lax.rem(me, 2)
    o = 1 - j
    pair = lax.div(c, 2)
    mate = c + 1 - 2 * lax.rem(c, 2)
    part = 3 - c
    far = 3 - mate
    zb, yb = lax.rem(g, 2), lax.rem(lax.div(g, span), 2)
    gz, gy = g + 1 - 2 * zb, g + span * (1 - 2 * yb)

    def dev(chip, core, group=g):
        return {"dp": group, "tp": 2 * chip + core}

    sib, mt, pt, zd, yd = dev(c, o), dev(mate, j), dev(part, j), dev(c, j, gz), dev(c, j, gy)

    def remote(src, dst, send, recv, to):
        return pltpu.make_async_remote_copy(src_ref=src, dst_ref=dst, send_sem=send, recv_sem=recv,
                                            device_id=to, device_id_type=MESH)

    def row(chip, core, extra=0):
        return pl.multiple_of((2 * chip + core) * rows + extra, half)

    quarter = 2 * yb + zb
    q_z, q_y, q_zy = quarter + 1 - 2 * zb, quarter + 2 - 4 * yb, 3 - quarter

    def w_rows(piece):
        return {QKV: d_model, UP0: d_model // 2, UP1: d_model // 2, DN0: ff // 2, DN1: ff // 2, OUT: head}[piece] // 4

    def w_at(piece, q, side, hold):
        n = w_rows(piece)
        size = n if side is None else n // 2
        off = q * n + (0 if side is None else side * size)
        if piece in (UP1, DN1):
            off = off + 4 * n
        if hold and piece in (DN0, DN1):
            off = off + ff
        if hold and piece == OUT:
            off = off + 2 * ff + head
        at = pl.ds(pl.multiple_of(off, n // 2), size)
        if piece == QKV:
            return wq.at[:, at, pl.ds(head, head)] if hold else w_qkv.at[:, at, :]
        if piece in (UP0, UP1):
            return wu.at[at, pl.ds(ff, ff)] if hold else w_up.at[at, :]
        return wd.at[at, :] if hold else (w_out if piece == OUT else w_dn).at[at, :]

    def w_own(i):
        src, dst = ((w_qkv, wq.at[:, :, pl.ds(0, head)]), (w_up, wu.at[:, pl.ds(0, ff)]),
                    (w_dn, wd.at[pl.ds(0, ff), :]), (w_out, wd.at[pl.ds(2 * ff, head), :]))[i]
        return pltpu.make_async_copy(src, dst, w_l.at[i])

    def wx(k):
        return remote(w_at(k, quarter, None, False), w_at(k, quarter, None, True), wx_s.at[k], wx_r.at[k], pt)

    def wx_in(k):
        ref = w_at(k, quarter, None, True)
        return remote(ref, ref, wx_s.at[k], wx_r.at[k], pt)

    def wf(k, i):
        ref = (w_at(k, quarter, None, True) if i < 2 else w_at(k, q_y, 1, True) if i == 2 else w_at(k, q_z, 0, True))
        return remote(ref, ref, wf_s.at[k, i], wf_r.at[k, i], yd if i in (1, 3) else zd)

    def wf_in(k, i):
        ref = w_at(k, (q_z, q_y, q_zy, q_zy)[i], (None, None, 1, 0)[i], True)
        return remote(ref, ref, wf_s.at[k, i], wf_r.at[k, i], yd if i in (1, 3) else zd)

    def pass_quarter(k):
        wx_in(k).wait_recv()
        wf(k, 0).start()
        wf(k, 1).start()

    def pass_halves(k):
        wf_in(k, 0).wait_recv()
        wf_in(k, 1).wait_recv()
        wf(k, 2).start()
        wf(k, 3).start()

    def have(k):
        wf_in(k, 2).wait_recv()
        wf_in(k, 3).wait_recv()

    def own_seq(s):
        return 2 * s + pair

    def other_seq(s):
        return 2 * s + 1 - pair

    def xm(s):
        return remote(x.at[own_seq(s)], xg.at[s, pl.ds(row(c, j), rows)], xm_s.at[s], xm_r.at[s], mt)

    def xm_in(s):
        ref = xg.at[s, pl.ds(row(mate, j), rows)]
        return remote(ref, ref, xm_s.at[s], xm_r.at[s], mt)

    def xp(s, h):
        return remote(x.at[other_seq(s), pl.ds(h * half, half)], xg.at[s, pl.ds(row(c, j, h * half), half)],
                      xp_s.at[s, h], xp_r.at[s, h], pt)

    def xp_in(s, h):
        ref = xg.at[s, pl.ds(row(part, j, h * half), half)]
        return remote(ref, ref, xp_s.at[s, h], xp_r.at[s, h], pt)

    def xf(s, h):
        ref = xg.at[s, pl.ds(row(part, j, h * half), half)]
        return remote(ref, ref, xf_s.at[s, h], xf_r.at[s, h], mt)

    def xf_in(s, h):
        ref = xg.at[s, pl.ds(row(far, j, h * half), half)]
        return remote(ref, ref, xf_s.at[s, h], xf_r.at[s, h], mt)

    def xd(s, i, core=j):
        if i == 0:
            dst = xg.at[s, pl.ds(row(c, core), rows)]
            return remote(x.at[own_seq(s)], dst, xd_s.at[s, i], xd_r.at[s, i], sib)
        ref = (xg.at[s, pl.ds(row(mate, core), rows)] if i == 1 else
               xg.at[s, pl.ds(row(part if i < 4 else far, core, (i % 2) * half), half)])
        return remote(ref, ref, xd_s.at[s, i], xd_r.at[s, i], sib)

    def xd_in(s, i):
        return xd(s, i, o)

    def relay_mate(s):
        xm_in(s).wait_recv()
        xd(s, 1).start()

    def relay_part(s, h):
        xp_in(s, h).wait_recv()
        xf(s, h).start()
        xd(s, 2 + h).start()

    def relay_far(s):
        for h in range(2):
            xf_in(s, h).wait_recv()
            xd(s, 4 + h).start()

    barrier = pltpu.get_barrier_semaphore()
    for to in (sib, mt, pt, zd, yd):
        pl.semaphore_signal(barrier, inc=1, device_id=to, device_id_type=MESH)
    pl.semaphore_wait(barrier, 5)

    wx(QKV).start()
    xm(0).start()
    xp(0, 0).start()
    xp(0, 1).start()
    for i in range(4):
        w_own(i).start()
    xd(0, 0).start()
    wx(UP0).start()
    for s in (1, 2):
        xd(s, 0).start()
    for h in range(2):
        xp(1, h).start()
    for k in (UP1, DN0, DN1, OUT):
        wx(k).start()
    for h in range(2):
        xp(2, h).start()

    pass_quarter(QKV)
    relay_mate(0)
    relay_part(0, 0)
    pass_halves(QKV)
    relay_part(0, 1)
    xm(1).start()
    w_own(0).wait()
    have(QKV)

    events = {
        (0, "tile", 1): [lambda: pass_quarter(UP0)],
        (0, "tile", 3): [lambda: pass_halves(UP0)],
        (0, "att", 3): [lambda: relay_mate(1), lambda: relay_part(1, 0), lambda: relay_part(1, 1)],
        (1, "tile", 0): [lambda: pass_quarter(UP1)],
        (1, "tile", 2): [lambda: pass_quarter(DN0), lambda: pass_halves(UP1)],
        (1, "tile", 3): [lambda: xm(2).start(), lambda: pass_quarter(DN1)],
        (1, "att", 1): [lambda: pass_quarter(OUT), lambda: pass_halves(DN0)],
        (1, "att", 3): [lambda: pass_halves(DN1), lambda: pass_halves(OUT)],
        (2, "mlp", 0): [lambda: relay_mate(2), lambda: relay_part(2, 0), lambda: relay_part(2, 1)],
    }

    def at(step, phase, i):
        for (p, st, k), acts in events.items():
            if st == step:
                @pl.when((phase == p) & (i == k))
                def _(acts=acts):
                    for act in acts:
                        act()

    def tile_chip(i):
        return jnp.where(i == 0, c, jnp.where(i == 1, mate, jnp.where(i == 2, part, far)))

    def mlp_chip(i):
        return jnp.where(i == 0, far, jnp.where(i == 1, mate, jnp.where(i == 2, part, c)))

    def tile_half(slot, core):
        return xt.at[slot, pl.ds(pl.multiple_of(core * rows, rows), rows)]

    def tile_copy(s, slot, i, core):
        return pltpu.make_async_copy(xg.at[s, pl.ds(row(tile_chip(i), core), rows)], tile_half(slot, core),
                                     xt_sem.at[slot, 0 if core is j else 1])

    def tile_start(s, slot, i):
        for kind, needs in enumerate(((0,), (1,), (2, 3), (4, 5))):
            @pl.when(i == kind)
            def _(needs=needs):
                for n in needs:
                    xd_in(s, n).wait_recv()

        @pl.when(i == 0)
        def _():
            pltpu.make_async_copy(x.at[own_seq(s)], tile_half(slot, j), xt_sem.at[slot, 0]).start()

        @pl.when(i > 0)
        def _():
            tile_copy(s, slot, i, j).start()

        tile_copy(s, slot, i, o).start()

    def tile_wait(s, slot, i):
        tile_copy(s, slot, i, j).wait()
        tile_copy(s, slot, i, o).wait()

    def n_out(s, slot, cb):
        return pltpu.make_async_copy(nt.at[slot], nbuf.at[s, pl.ds(pl.multiple_of(cb * blk, blk), blk)],
                                     no_sem.at[slot])

    def o_out(s, slot, cb):
        return pltpu.make_async_copy(ot.at[slot], obuf.at[s, pl.ds(pl.multiple_of(cb * blk, blk), blk)],
                                     oo_sem.at[slot])

    def project(slot, cb):
        def norm(r, _):
            rr = pl.ds(pl.multiple_of(r * ln_rows, ln_rows), ln_rows)
            v = xt[slot, rr, :].astype(F32)
            mean = jnp.mean(v, axis=-1, keepdims=True)
            cen = v - mean
            var = jnp.mean(cen * cen, axis=-1, keepdims=True)
            nt[slot, rr, :] = (cen * lax.rsqrt(var + LN_EPS) * gain[...] + bias[...]).astype(BF16)
            return 0

        lax.fori_loop(0, blk // ln_rows, norm, 0)
        base = pl.ds(pl.multiple_of(cb * blk, blk), blk)

        def proj(t, _):
            qkv[base, pl.ds(pl.multiple_of(t * 2 * head, 2 * head), 2 * head)] = jnp.dot(
                nt[slot], wq[t], preferred_element_type=F32).astype(BF16)
            return 0

        lax.fori_loop(0, 3, proj, 0)

    def dot_t(a, b):
        return lax.dot_general(a, b, (((1,), (1,)), ((), ())), preferred_element_type=F32)

    def attend(slot, cb):
        mine = pl.ds(pl.multiple_of(cb * blk, blk), blk)
        causal = (lax.broadcasted_iota(jnp.int32, (blk, blk), 0)
                  >= lax.broadcasted_iota(jnp.int32, (blk, blk), 1))
        for h in range(2):
            q, key, val = (qkv[mine, pl.ds((2 * t + h) * head, head)] for t in range(3))
            sc = jnp.where(causal, dot_t(q, key), -jnp.inf)
            top = jnp.max(sc, axis=-1, keepdims=True)
            p = jnp.exp2((sc - top) * scale)
            m_s[h] = top
            l_s[h] = jnp.sum(p, axis=-1, keepdims=True)
            acc[h] = jnp.dot(p.astype(BF16), val, preferred_element_type=F32)

        def earlier(t, _):
            there = pl.ds(pl.multiple_of(t * blk, blk), blk)
            for h in range(2):
                q = qkv[mine, pl.ds(h * head, head)]
                key = qkv[there, pl.ds((2 + h) * head, head)]
                val = qkv[there, pl.ds((4 + h) * head, head)]
                sc = dot_t(q, key)
                old = m_s[h]
                top = jnp.maximum(old, jnp.max(sc, axis=-1, keepdims=True))
                p = jnp.exp2((sc - top) * scale)
                fade = jnp.exp2((old - top) * scale)
                m_s[h] = top
                l_s[h] = l_s[h] * fade + jnp.sum(p, axis=-1, keepdims=True)
                acc[h] = acc[h] * fade + jnp.dot(p.astype(BF16), val, preferred_element_type=F32)
            return 0

        lax.fori_loop(0, cb, earlier, 0)
        for h in range(2):
            ot[slot, :, pl.ds(h * head, head)] = (acc[h] / l_s[h]).astype(BF16)

    def sp(s, i):
        return remote(stage.at[pl.ds(pl.multiple_of(o * rows, rows), rows)], sibin.at[s, i],
                      sp_s.at[s, i], sp_r.at[s, i], sib)

    def sp_in(s, i):
        return remote(sibin.at[s, i], sibin.at[s, i], sp_s.at[s, i], sp_r.at[s, i], sib)

    def to_mate(s, i):
        return remote(tbuf.at[i], mid.at[s, i], t_s.at[s, i], t_r.at[s, i], mt)

    def from_mate(s, i):
        return remote(mid.at[s, i], mid.at[s, i], t_s.at[s, i], t_r.at[s, i], mt)

    def to_part(s):
        return remote(tbuf.at[2], fin.at[s], p_s.at[s], p_r.at[s], pt)

    def from_part(s):
        return remote(fin.at[s], fin.at[s], p_s.at[s], p_r.at[s], pt)

    def cin_load(src, slot):
        return pltpu.make_async_copy(src, cin.at[slot], cl_sem.at[slot])

    def y_store(q, slot):
        return pltpu.make_async_copy(cin.at[slot], y.at[q], yo_sem.at[slot - 2])

    def add_loads(s, kind):
        loads = [cin_load(sibin.at[s, kind], 0)]
        if kind >= 2:
            loads.append(cin_load(mid.at[s, kind - 2], 1))
        if kind == 3:
            loads.append(cin_load(x.at[own_seq(s)], 2))
        return loads

    def add_start(s, kind):
        sp_in(s, kind).wait_recv()
        if kind >= 2:
            from_mate(s, kind - 2).wait_recv()

        @pl.when(s > 0)
        def _():
            if kind < 2:
                to_mate(s - 1, kind).wait_send()
            elif kind == 2:
                to_part(s - 1).wait_send()
            else:
                y_store(own_seq(s), 2).wait()

        for ld in add_loads(s, kind):
            ld.start()

    def add_finish(s, kind):
        for ld in add_loads(s, kind):
            ld.wait()

        def add(r, _):
            rr = pl.ds(pl.multiple_of(r * ln_rows, ln_rows), ln_rows)
            mine = pl.ds(pl.multiple_of(j * rows + r * ln_rows, ln_rows), ln_rows)
            total = stage[mine, :].astype(F32) + cin[0, rr, :].astype(F32)
            if kind >= 2:
                total = total + cin[1, rr, :].astype(F32)
            total = total.astype(BF16)
            if kind == 3:
                cin[2, rr, :] = (cin[2, rr, :].astype(F32) + total.astype(F32)).astype(BF16)
            else:
                tbuf[kind, rr, :] = total
            return 0

        lax.fori_loop(0, rows // ln_rows, add, 0)
        sp(s, kind).wait_send()
        if kind < 2:
            to_mate(s, kind).start()
        elif kind == 2:
            to_part(s).start()
        else:
            y_store(own_seq(s), 2).start()

    def other_loads(s):
        return cin_load(fin.at[s], 0), cin_load(x.at[other_seq(s)], 3)

    def finish_other(s):
        from_part(s).wait_recv()

        @pl.when(s > 0)
        def _():
            y_store(other_seq(s), 3).wait()

        for ld in other_loads(s):
            ld.start()
        for ld in other_loads(s):
            ld.wait()

        def add(r, _):
            rr = pl.ds(pl.multiple_of(r * ln_rows, ln_rows), ln_rows)
            cin[3, rr, :] = (cin[3, rr, :].astype(F32) + cin[0, rr, :].astype(F32)).astype(BF16)
            return 0

        lax.fori_loop(0, rows // ln_rows, add, 0)
        y_store(other_seq(s), 3).start()

    def n_load(s, slot, i):
        return pltpu.make_async_copy(nbuf.at[s, pl.ds(pl.multiple_of(mlp_chip(i) * blk, blk), blk)], nt.at[slot],
                                     nl_sem.at[slot])

    def o_load(s, slot, i):
        return pltpu.make_async_copy(obuf.at[s, pl.ds(pl.multiple_of(mlp_chip(i) * blk, blk), blk)],
                                     ho.at[slot, :, pl.ds(2 * ff, 2 * head)], ol_sem.at[slot])

    def mlp_block(phase, s, i):
        slot = lax.rem(i, 2)
        chunks = 2 * ff // chunk
        n_load(s, slot, i).wait()

        def up(t, _):
            cols = pl.ds(pl.multiple_of(t * chunk, chunk), chunk)
            hid = jnp.dot(nt[slot], wu[:, cols], preferred_element_type=F32)
            ho[slot, :, cols] = (0.5 * hid * (1.0 + lax.erf(hid * 0.7071067811865476))).astype(BF16)
            return 0

        def pending(act):
            for kind in range(3):
                @pl.when(i == kind + 1)
                def _(kind=kind):
                    act(s, kind)

            @pl.when((i == 0) & (phase == 3))
            def _():
                act(s - 1, 3)

        def ups(u, _):
            lax.fori_loop(u * (chunks // 2), (u + 1) * (chunks // 2), up, 0)

            @pl.when(u == 0)
            def _():
                pending(add_start)

                @pl.when(i < 3)
                def _():
                    n_load(s, 1 - slot, i + 1).start()
                    o_load(s, 1 - slot, i + 1).start()

            return 0

        lax.fori_loop(0, 2, ups, 0)
        pending(add_finish)
        o_load(s, slot, i).wait()

        @pl.when((phase == 2) & (i == 0))
        def _():
            for k in (DN0, DN1, OUT):
                have(k)
            w_own(2).wait()
            w_own(3).wait()

        def down(t, _):
            cols = pl.ds(pl.multiple_of(t * chunk, chunk), chunk)
            stage[:, cols] = jnp.dot(ho[slot], wd[:, cols], preferred_element_type=F32).astype(BF16)
            return 0

        lax.fori_loop(0, d_model // chunk, down, 0)
        for kind in range(4):
            @pl.when(i == kind)
            def _(kind=kind):
                sp(s, kind).start()

    def pick(values, phase):
        out = jnp.int32(values[0])
        for p in range(1, len(values)):
            out = jnp.where(phase == p, values[p], out)
        return out

    def run(phase, _):
        s = pick([s for _, s in PHASES], phase)
        is_a = pick([int(kind == "a") for kind, _ in PHASES], phase) == 1

        @pl.when(is_a)
        def _():
            tile_start(s, 0, 0)

            def tile(i, _):
                slot = lax.rem(i, 2)
                cb = tile_chip(i)

                @pl.when(i == 3)
                def _():
                    relay_far(s)
                    tile_start(s, slot, i)

                tile_wait(s, slot, i)

                @pl.when(i < 2)
                def _():
                    tile_start(s, 1 - slot, i + 1)

                @pl.when(i >= 2)
                def _():
                    n_out(s, slot, cb).wait()

                project(slot, cb)
                n_out(s, slot, cb).start()

                @pl.when((phase == 4) & (i == 0))
                def _():
                    add_start(s - 1, 3)
                    add_finish(s - 1, 3)

                at("tile", phase, i)
                return 0

            lax.fori_loop(0, 4, tile, 0)

            def att(i, _):
                slot = lax.rem(i, 2)

                @pl.when(i >= 2)
                def _():
                    o_out(s, slot, i).wait()

                attend(slot, i)
                o_out(s, slot, i).start()
                at("att", phase, i)
                return 0

            lax.fori_loop(0, 4, att, 0)
            for slot in range(2):
                n_out(s, slot, 0).wait()
                o_out(s, slot, 0).wait()

        @pl.when(jnp.logical_not(is_a))
        def _():
            n_load(s, 0, 0).start()
            o_load(s, 0, 0).start()

            @pl.when(phase == 2)
            def _():
                for k in (UP0, UP1):
                    have(k)
                w_own(1).wait()

            def block(i, _):
                mlp_block(phase, s, i)
                at("mlp", phase, i)

                @pl.when((s > 0) & (i == 2))
                def _():
                    finish_other(s - 1)

                return 0

            lax.fori_loop(0, 4, block, 0)

        return 0

    lax.fori_loop(0, len(PHASES), run, 0)

    add_start(jnp.int32(2), 3)
    add_finish(jnp.int32(2), 3)
    finish_other(jnp.int32(2))

    for s in range(3):
        xm(s).wait_send()
        for h in range(2):
            xp(s, h).wait_send()
            xf(s, h).wait_send()
        for i in range(6):
            xd(s, i).wait_send()
    for k in range(6):
        wx(k).wait_send()
        for i in range(4):
            wf(k, i).wait_send()
    to_mate(2, 0).wait_send()
    to_mate(2, 1).wait_send()
    to_part(2).wait_send()
    y_store(own_seq(2), 2).wait()
    y_store(other_seq(2), 3).wait()


def neighbour_span(groups):
    short = 1
    while short * short * 4 <= groups:
        short *= 2
    return groups // short


def solution(mesh):
    tp, groups = mesh.shape["tp"], mesh.shape["dp"]
    span = neighbour_span(groups)
    assert tp == 8 and groups % (2 * span) == 0 and span % 2 == 0

    def local_layer(x_blk, ln_gain, ln_bias, w_qkv, w_out, w_up, w_down):
        n_seq, rows, d_model = x_blk.shape
        head = w_qkv.shape[3]
        ff = w_up.shape[1]
        ns, seq, blk = n_seq // 2, rows * tp, 2 * rows
        assert ns == 3 and w_qkv.shape[1:3] == (1, 3)
        chunk = min(512, d_model, ff)
        ln_rows = min(32, rows // 2)
        dims = (span, rows, d_model, head, ff, chunk, ln_rows)
        dma = pltpu.SemaphoreType.DMA
        anyspace = pl.BlockSpec(memory_space=pl.ANY)
        vmem = pl.BlockSpec(memory_space=pltpu.VMEM)

        def hbm(*shape):
            return jax.ShapeDtypeStruct(shape, BF16)

        outs = pl.pallas_call(
            functools.partial(layer_kernel, dims),
            name="layer",
            out_shape=(hbm(n_seq, rows, d_model), hbm(ns, seq, d_model), hbm(ns, seq, d_model), hbm(ns, seq, 2 * head),
                       hbm(ns, 4, rows, d_model), hbm(ns, 2, rows, d_model), hbm(ns, rows, d_model)),
            in_specs=[anyspace, vmem, vmem, anyspace, anyspace, anyspace, anyspace],
            out_specs=(anyspace,) * 7,
            scratch_shapes=[
                pltpu.VMEM((3, d_model, 2 * head), BF16),
                pltpu.VMEM((d_model, 2 * ff), BF16),
                pltpu.VMEM((2 * ff + 2 * head, d_model), BF16),
                pltpu.VMEM((2, blk, d_model), BF16),
                pltpu.VMEM((2, blk, d_model), BF16),
                pltpu.VMEM((seq, 6 * head), BF16),
                pltpu.VMEM((2, blk, 2 * head), BF16),
                pltpu.VMEM((2, blk, 2 * ff + 2 * head), BF16),
                pltpu.VMEM((blk, d_model), BF16),
                pltpu.VMEM((4, rows, d_model), BF16),
                pltpu.VMEM((3, rows, d_model), BF16),
                pltpu.VMEM((2, blk, head), F32),
                pltpu.VMEM((2, blk, 1), F32),
                pltpu.VMEM((2, blk, 1), F32),
                dma((4,)), dma((6,)), dma((6,)), dma((6, 4)), dma((6, 4)),
                dma((ns,)), dma((ns,)), dma((ns, 2)), dma((ns, 2)), dma((ns, 2)), dma((ns, 2)),
                dma((ns, 6)), dma((ns, 6)),
                dma((ns, 4)), dma((ns, 4)), dma((ns, 2)), dma((ns, 2)), dma((ns,)), dma((ns,)),
                dma((2, 2)), dma((2,)), dma((2,)), dma((2,)), dma((2,)), dma((4,)), dma((2,)),
            ],
            compiler_params=pltpu.CompilerParams(
                collective_id=0, has_side_effects=True, vmem_limit_bytes=VMEM_LIMIT),
        )(x_blk, ln_gain.reshape(1, d_model), ln_bias.reshape(1, d_model),
          jnp.transpose(w_qkv[:, 0], (1, 0, 2)), w_out, w_up, w_down)
        return outs[0]

    return jax.shard_map(
        local_layer, mesh=mesh,
        in_specs=(P("dp", "tp", None), P(), P(), P(None, "tp", None, None),
                  P("tp", None), P(None, "tp"), P("tp", None)),
        out_specs=P("dp", "tp", None), check_vma=False)
```

```python
import functools

import jax
import jax.numpy as jnp
from jax import lax
from jax.experimental import pallas as pl
from jax.experimental.pallas import tpu as pltpu
from jax.sharding import PartitionSpec as P

LN_EPS = 1e-5
MESH = pl.DeviceIdType.MESH
BF16 = jnp.bfloat16
F32 = jnp.float32
LOG2E = 1.4426950408889634
VMEM_LIMIT = 67_043_328

PHASES = (("a", 0), ("a", 1), ("m", 0), ("m", 1), ("a", 2), ("m", 2))
QKV, UP0, UP1, DN0, DN1, OUT = range(6)


def layer_kernel(dims, x, gain, bias, w_qkv, w_out, w_up, w_dn,
                 y, xg, nbuf, obuf, sibin, mid, fin,
                 wq, wu, wd, nt, xt, qkv, ot, ho, stage, cin, tbuf, acc, m_s, l_s,
                 w_l, wx_s, wx_r, wf_s, wf_r, xm_s, xm_r, xp_s, xp_r, xf_s, xf_r, xd_s, xd_r,
                 sp_s, sp_r, t_s, t_r, p_s, p_r,
                 xt_sem, no_sem, oo_sem, nl_sem, ol_sem, cl_sem, yo_sem):
    span, rows, d_model, head, ff, chunk, ln_rows = dims
    half = rows // 2
    blk = 2 * rows
    scale = LOG2E * head ** -0.5

    g, me = lax.axis_index("dp"), lax.axis_index("tp")
    c, j = lax.div(me, 2), lax.rem(me, 2)
    o = 1 - j
    pair = lax.div(c, 2)
    mate = c + 1 - 2 * lax.rem(c, 2)
    part = 3 - c
    far = 3 - mate
    zb, yb = lax.rem(g, 2), lax.rem(lax.div(g, span), 2)
    gz, gy = g + 1 - 2 * zb, g + span * (1 - 2 * yb)

    def dev(chip, core, group=g):
        return {"dp": group, "tp": 2 * chip + core}

    sib, mt, pt, zd, yd = dev(c, o), dev(mate, j), dev(part, j), dev(c, j, gz), dev(c, j, gy)

    def remote(src, dst, send, recv, to):
        return pltpu.make_async_remote_copy(src_ref=src, dst_ref=dst, send_sem=send, recv_sem=recv,
                                            device_id=to, device_id_type=MESH)

    def row(chip, core, extra=0):
        return pl.multiple_of((2 * chip + core) * rows + extra, half)

    quarter = 2 * yb + zb
    q_z, q_y, q_zy = quarter + 1 - 2 * zb, quarter + 2 - 4 * yb, 3 - quarter

    def w_rows(piece):
        return {QKV: d_model, UP0: d_model // 2, UP1: d_model // 2, DN0: ff // 2, DN1: ff // 2, OUT: head}[piece] // 4

    def w_at(piece, q, side, hold):
        n = w_rows(piece)
        size = n if side is None else n // 2
        off = q * n + (0 if side is None else side * size)
        if piece in (UP1, DN1):
            off = off + 4 * n
        if hold and piece in (DN0, DN1):
            off = off + ff
        if hold and piece == OUT:
            off = off + 2 * ff + head
        at = pl.ds(pl.multiple_of(off, n // 2), size)
        if piece == QKV:
            return wq.at[:, at, pl.ds(head, head)] if hold else w_qkv.at[:, at, :]
        if piece in (UP0, UP1):
            return wu.at[at, pl.ds(ff, ff)] if hold else w_up.at[at, :]
        return wd.at[at, :] if hold else (w_out if piece == OUT else w_dn).at[at, :]

    def w_own(i):
        src, dst = ((w_qkv, wq.at[:, :, pl.ds(0, head)]), (w_up, wu.at[:, pl.ds(0, ff)]),
                    (w_dn, wd.at[pl.ds(0, ff), :]), (w_out, wd.at[pl.ds(2 * ff, head), :]))[i]
        return pltpu.make_async_copy(src, dst, w_l.at[i])

    def wx(k):
        return remote(w_at(k, quarter, None, False), w_at(k, quarter, None, True), wx_s.at[k], wx_r.at[k], pt)

    def wx_in(k):
        ref = w_at(k, quarter, None, True)
        return remote(ref, ref, wx_s.at[k], wx_r.at[k], pt)

    def wf(k, i):
        ref = (w_at(k, quarter, None, True) if i < 2 else w_at(k, q_y, 1, True) if i == 2 else w_at(k, q_z, 0, True))
        return remote(ref, ref, wf_s.at[k, i], wf_r.at[k, i], yd if i in (1, 3) else zd)

    def wf_in(k, i):
        ref = w_at(k, (q_z, q_y, q_zy, q_zy)[i], (None, None, 1, 0)[i], True)
        return remote(ref, ref, wf_s.at[k, i], wf_r.at[k, i], yd if i in (1, 3) else zd)

    def pass_quarter(k):
        wx_in(k).wait_recv()
        wf(k, 0).start()
        wf(k, 1).start()

    def pass_halves(k):
        wf_in(k, 0).wait_recv()
        wf_in(k, 1).wait_recv()
        wf(k, 2).start()
        wf(k, 3).start()

    def have(k):
        wf_in(k, 2).wait_recv()
        wf_in(k, 3).wait_recv()

    def own_seq(s):
        return 2 * s + pair

    def other_seq(s):
        return 2 * s + 1 - pair

    def xm(s):
        return remote(x.at[own_seq(s)], xg.at[s, pl.ds(row(c, j), rows)], xm_s.at[s], xm_r.at[s], mt)

    def xm_in(s):
        ref = xg.at[s, pl.ds(row(mate, j), rows)]
        return remote(ref, ref, xm_s.at[s], xm_r.at[s], mt)

    def xp(s, h):
        return remote(x.at[other_seq(s), pl.ds(h * half, half)], xg.at[s, pl.ds(row(c, j, h * half), half)],
                      xp_s.at[s, h], xp_r.at[s, h], pt)

    def xp_in(s, h):
        ref = xg.at[s, pl.ds(row(part, j, h * half), half)]
        return remote(ref, ref, xp_s.at[s, h], xp_r.at[s, h], pt)

    def xf(s, h):
        ref = xg.at[s, pl.ds(row(part, j, h * half), half)]
        return remote(ref, ref, xf_s.at[s, h], xf_r.at[s, h], mt)

    def xf_in(s, h):
        ref = xg.at[s, pl.ds(row(far, j, h * half), half)]
        return remote(ref, ref, xf_s.at[s, h], xf_r.at[s, h], mt)

    def xd(s, i, core=j):
        if i == 0:
            dst = xg.at[s, pl.ds(row(c, core), rows)]
            return remote(x.at[own_seq(s)], dst, xd_s.at[s, i], xd_r.at[s, i], sib)
        ref = (xg.at[s, pl.ds(row(mate, core), rows)] if i == 1 else
               xg.at[s, pl.ds(row(part if i < 4 else far, core, (i % 2) * half), half)])
        return remote(ref, ref, xd_s.at[s, i], xd_r.at[s, i], sib)

    def xd_in(s, i):
        return xd(s, i, o)

    def relay_mate(s):
        xm_in(s).wait_recv()
        xd(s, 1).start()

    def relay_part(s, h):
        xp_in(s, h).wait_recv()
        xf(s, h).start()
        xd(s, 2 + h).start()

    def relay_far(s):
        for h in range(2):
            xf_in(s, h).wait_recv()
            xd(s, 4 + h).start()

    def send_x(s):
        xm(s).start()
        xd(s, 0).start()
        for h in range(2):
            xp(s, h).start()

    barrier = pltpu.get_barrier_semaphore()
    for to in (sib, mt, pt, zd, yd):
        pl.semaphore_signal(barrier, inc=1, device_id=to, device_id_type=MESH)
    pl.semaphore_wait(barrier, 5)

    wx(QKV).start()
    xm(0).start()
    for i in range(4):
        w_own(i).start()
    xd(0, 0).start()
    xp(0, 0).start()
    xp(0, 1).start()

    pass_quarter(QKV)
    relay_mate(0)
    relay_part(0, 0)
    wx(UP0).start()
    pass_halves(QKV)
    relay_part(0, 1)
    send_x(1)
    w_own(0).wait()
    have(QKV)

    events = {
        (0, "tile", 1): [lambda: pass_quarter(UP0)],
        (0, "tile", 3): [lambda: wx(UP1).start(), lambda: pass_halves(UP0)],
        (0, "att", 1): [lambda: wx(DN0).start()],
        (0, "att", 3): [lambda: relay_mate(1), lambda: relay_part(1, 0), lambda: relay_part(1, 1),
                        lambda: wx(DN1).start()],
        (1, "tile", 0): [lambda: pass_quarter(UP1), lambda: wx(OUT).start()],
        (1, "tile", 2): [lambda: pass_quarter(DN0), lambda: pass_halves(UP1)],
        (1, "tile", 3): [lambda: send_x(2), lambda: pass_quarter(DN1)],
        (1, "att", 1): [lambda: pass_quarter(OUT), lambda: pass_halves(DN0)],
        (1, "att", 3): [lambda: pass_halves(DN1), lambda: pass_halves(OUT)],
        (2, "mlp", 0): [lambda: relay_mate(2), lambda: relay_part(2, 0), lambda: relay_part(2, 1)],
    }

    def at(step, phase, i):
        for (p, st, k), acts in events.items():
            if st == step:
                @pl.when((phase == p) & (i == k))
                def _(acts=acts):
                    for act in acts:
                        act()

    def tile_chip(i):
        return jnp.where(i == 0, c, jnp.where(i == 1, mate, jnp.where(i == 2, part, far)))

    def mlp_chip(i):
        return jnp.where(i == 0, far, jnp.where(i == 1, mate, jnp.where(i == 2, part, c)))

    def tile_half(slot, core):
        return xt.at[slot, pl.ds(pl.multiple_of(core * rows, rows), rows)]

    def tile_copy(s, slot, i, core):
        return pltpu.make_async_copy(xg.at[s, pl.ds(row(tile_chip(i), core), rows)], tile_half(slot, core),
                                     xt_sem.at[slot, 0 if core is j else 1])

    def tile_start(s, slot, i):
        for kind, needs in enumerate(((0,), (1,), (2, 3), (4, 5))):
            @pl.when(i == kind)
            def _(needs=needs):
                for n in needs:
                    xd_in(s, n).wait_recv()

        @pl.when(i == 0)
        def _():
            pltpu.make_async_copy(x.at[own_seq(s)], tile_half(slot, j), xt_sem.at[slot, 0]).start()

        @pl.when(i > 0)
        def _():
            tile_copy(s, slot, i, j).start()

        tile_copy(s, slot, i, o).start()

    def tile_wait(s, slot, i):
        tile_copy(s, slot, i, j).wait()
        tile_copy(s, slot, i, o).wait()

    def n_out(s, slot, cb):
        return pltpu.make_async_copy(nt.at[slot], nbuf.at[s, pl.ds(pl.multiple_of(cb * blk, blk), blk)],
                                     no_sem.at[slot])

    def o_out(s, slot, cb):
        return pltpu.make_async_copy(ot.at[slot], obuf.at[s, pl.ds(pl.multiple_of(cb * blk, blk), blk)],
                                     oo_sem.at[slot])

    def project(slot, cb):
        def norm(r, _):
            rr = pl.ds(pl.multiple_of(r * ln_rows, ln_rows), ln_rows)
            v = xt[slot, rr, :].astype(F32)
            mean = jnp.mean(v, axis=-1, keepdims=True)
            cen = v - mean
            var = jnp.mean(cen * cen, axis=-1, keepdims=True)
            nt[slot, rr, :] = (cen * lax.rsqrt(var + LN_EPS) * gain[...] + bias[...]).astype(BF16)
            return 0

        lax.fori_loop(0, blk // ln_rows, norm, 0)
        base = pl.ds(pl.multiple_of(cb * blk, blk), blk)

        def proj(t, _):
            qkv[base, pl.ds(pl.multiple_of(t * 2 * head, 2 * head), 2 * head)] = jnp.dot(
                nt[slot], wq[t], preferred_element_type=F32).astype(BF16)
            return 0

        lax.fori_loop(0, 3, proj, 0)

    def dot_t(a, b):
        return lax.dot_general(a, b, (((1,), (1,)), ((), ())), preferred_element_type=F32)

    def attend(slot, cb):
        mine = pl.ds(pl.multiple_of(cb * blk, blk), blk)
        causal = (lax.broadcasted_iota(jnp.int32, (blk, blk), 0)
                  >= lax.broadcasted_iota(jnp.int32, (blk, blk), 1))
        for h in range(2):
            q, key, val = (qkv[mine, pl.ds((2 * t + h) * head, head)] for t in range(3))
            sc = jnp.where(causal, dot_t(q, key), -jnp.inf)
            top = jnp.max(sc, axis=-1, keepdims=True)
            p = jnp.exp2((sc - top) * scale)
            m_s[h] = top
            l_s[h] = jnp.sum(p, axis=-1, keepdims=True)
            acc[h] = jnp.dot(p.astype(BF16), val, preferred_element_type=F32)

        def earlier(t, _):
            there = pl.ds(pl.multiple_of(t * blk, blk), blk)
            for h in range(2):
                q = qkv[mine, pl.ds(h * head, head)]
                key = qkv[there, pl.ds((2 + h) * head, head)]
                val = qkv[there, pl.ds((4 + h) * head, head)]
                sc = dot_t(q, key)
                old = m_s[h]
                top = jnp.maximum(old, jnp.max(sc, axis=-1, keepdims=True))
                p = jnp.exp2((sc - top) * scale)
                fade = jnp.exp2((old - top) * scale)
                m_s[h] = top
                l_s[h] = l_s[h] * fade + jnp.sum(p, axis=-1, keepdims=True)
                acc[h] = acc[h] * fade + jnp.dot(p.astype(BF16), val, preferred_element_type=F32)
            return 0

        lax.fori_loop(0, cb, earlier, 0)
        for h in range(2):
            ot[slot, :, pl.ds(h * head, head)] = (acc[h] / l_s[h]).astype(BF16)

    def sp(s, i):
        return remote(stage.at[pl.ds(pl.multiple_of(o * rows, rows), rows)], sibin.at[s, i],
                      sp_s.at[s, i], sp_r.at[s, i], sib)

    def sp_in(s, i):
        return remote(sibin.at[s, i], sibin.at[s, i], sp_s.at[s, i], sp_r.at[s, i], sib)

    def to_mate(s, i):
        return remote(tbuf.at[i], mid.at[s, i], t_s.at[s, i], t_r.at[s, i], mt)

    def from_mate(s, i):
        return remote(mid.at[s, i], mid.at[s, i], t_s.at[s, i], t_r.at[s, i], mt)

    def to_part(s):
        return remote(tbuf.at[2], fin.at[s], p_s.at[s], p_r.at[s], pt)

    def from_part(s):
        return remote(fin.at[s], fin.at[s], p_s.at[s], p_r.at[s], pt)

    def cin_load(src, slot):
        return pltpu.make_async_copy(src, cin.at[slot], cl_sem.at[slot])

    def y_store(q, slot):
        return pltpu.make_async_copy(cin.at[slot], y.at[q], yo_sem.at[slot - 2])

    def add_loads(s, kind):
        loads = [cin_load(sibin.at[s, kind], 0)]
        if kind >= 2:
            loads.append(cin_load(mid.at[s, kind - 2], 1))
        if kind == 3:
            loads.append(cin_load(x.at[own_seq(s)], 2))
        return loads

    def add_start(s, kind):
        sp_in(s, kind).wait_recv()
        if kind >= 2:
            from_mate(s, kind - 2).wait_recv()

        @pl.when(s > 0)
        def _():
            if kind < 2:
                to_mate(s - 1, kind).wait_send()
            elif kind == 2:
                to_part(s - 1).wait_send()
            else:
                y_store(own_seq(s), 2).wait()

        for ld in add_loads(s, kind):
            ld.start()

    def add_finish(s, kind):
        for ld in add_loads(s, kind):
            ld.wait()

        def add(r, _):
            rr = pl.ds(pl.multiple_of(r * ln_rows, ln_rows), ln_rows)
            mine = pl.ds(pl.multiple_of(j * rows + r * ln_rows, ln_rows), ln_rows)
            total = stage[mine, :].astype(F32) + cin[0, rr, :].astype(F32)
            if kind >= 2:
                total = total + cin[1, rr, :].astype(F32)
            total = total.astype(BF16)
            if kind == 3:
                cin[2, rr, :] = (cin[2, rr, :].astype(F32) + total.astype(F32)).astype(BF16)
            else:
                tbuf[kind, rr, :] = total
            return 0

        lax.fori_loop(0, rows // ln_rows, add, 0)
        sp(s, kind).wait_send()
        if kind < 2:
            to_mate(s, kind).start()
        elif kind == 2:
            to_part(s).start()
        else:
            y_store(own_seq(s), 2).start()

    def other_loads(s):
        return cin_load(fin.at[s], 0), cin_load(x.at[other_seq(s)], 3)

    def finish_other(s):
        from_part(s).wait_recv()

        @pl.when(s > 0)
        def _():
            y_store(other_seq(s), 3).wait()

        for ld in other_loads(s):
            ld.start()
        for ld in other_loads(s):
            ld.wait()

        def add(r, _):
            rr = pl.ds(pl.multiple_of(r * ln_rows, ln_rows), ln_rows)
            cin[3, rr, :] = (cin[3, rr, :].astype(F32) + cin[0, rr, :].astype(F32)).astype(BF16)
            return 0

        lax.fori_loop(0, rows // ln_rows, add, 0)
        y_store(other_seq(s), 3).start()

    def n_load(s, slot, i):
        return pltpu.make_async_copy(nbuf.at[s, pl.ds(pl.multiple_of(mlp_chip(i) * blk, blk), blk)], nt.at[slot],
                                     nl_sem.at[slot])

    def o_load(s, slot, i):
        return pltpu.make_async_copy(obuf.at[s, pl.ds(pl.multiple_of(mlp_chip(i) * blk, blk), blk)],
                                     ho.at[slot, :, pl.ds(2 * ff, 2 * head)], ol_sem.at[slot])

    def mlp_block(phase, s, i):
        slot = lax.rem(i, 2)
        chunks = 2 * ff // chunk
        n_load(s, slot, i).wait()

        def up(t, _):
            cols = pl.ds(pl.multiple_of(t * chunk, chunk), chunk)
            hid = jnp.dot(nt[slot], wu[:, cols], preferred_element_type=F32)
            ho[slot, :, cols] = (0.5 * hid * (1.0 + lax.erf(hid * 0.7071067811865476))).astype(BF16)
            return 0

        def pending(act):
            for kind in range(3):
                @pl.when(i == kind + 1)
                def _(kind=kind):
                    act(s, kind)

            @pl.when((i == 0) & (phase == 3))
            def _():
                act(s - 1, 3)

        def ups(u, _):
            lax.fori_loop(u * (chunks // 2), (u + 1) * (chunks // 2), up, 0)

            @pl.when(u == 0)
            def _():
                pending(add_start)

                @pl.when(i < 3)
                def _():
                    n_load(s, 1 - slot, i + 1).start()
                    o_load(s, 1 - slot, i + 1).start()

            return 0

        lax.fori_loop(0, 2, ups, 0)
        pending(add_finish)
        o_load(s, slot, i).wait()

        @pl.when((phase == 2) & (i == 0))
        def _():
            for k in (DN0, DN1, OUT):
                have(k)
            w_own(2).wait()
            w_own(3).wait()

        def down(t, _):
            cols = pl.ds(pl.multiple_of(t * chunk, chunk), chunk)
            stage[:, cols] = jnp.dot(ho[slot], wd[:, cols], preferred_element_type=F32).astype(BF16)
            return 0

        lax.fori_loop(0, d_model // chunk, down, 0)
        for kind in range(4):
            @pl.when(i == kind)
            def _(kind=kind):
                sp(s, kind).start()

    def pick(values, phase):
        out = jnp.int32(values[0])
        for p in range(1, len(values)):
            out = jnp.where(phase == p, values[p], out)
        return out

    def run(phase, _):
        s = pick([s for _, s in PHASES], phase)
        is_a = pick([int(kind == "a") for kind, _ in PHASES], phase) == 1

        @pl.when(is_a)
        def _():
            tile_start(s, 0, 0)

            def tile(i, _):
                slot = lax.rem(i, 2)
                cb = tile_chip(i)

                @pl.when(i == 3)
                def _():
                    relay_far(s)
                    tile_start(s, slot, i)

                tile_wait(s, slot, i)

                @pl.when(i < 2)
                def _():
                    tile_start(s, 1 - slot, i + 1)

                @pl.when(i >= 2)
                def _():
                    n_out(s, slot, cb).wait()

                project(slot, cb)
                n_out(s, slot, cb).start()

                @pl.when((phase == 4) & (i == 0))
                def _():
                    add_start(s - 1, 3)
                    add_finish(s - 1, 3)

                at("tile", phase, i)
                return 0

            lax.fori_loop(0, 4, tile, 0)

            def att(i, _):
                slot = lax.rem(i, 2)

                @pl.when(i >= 2)
                def _():
                    o_out(s, slot, i).wait()

                attend(slot, i)
                o_out(s, slot, i).start()
                at("att", phase, i)
                return 0

            lax.fori_loop(0, 4, att, 0)
            for slot in range(2):
                n_out(s, slot, 0).wait()
                o_out(s, slot, 0).wait()

        @pl.when(jnp.logical_not(is_a))
        def _():
            n_load(s, 0, 0).start()
            o_load(s, 0, 0).start()

            @pl.when(phase == 2)
            def _():
                for k in (UP0, UP1):
                    have(k)
                w_own(1).wait()

            def block(i, _):
                mlp_block(phase, s, i)
                at("mlp", phase, i)

                @pl.when((s > 0) & (i == 2))
                def _():
                    finish_other(s - 1)

                return 0

            lax.fori_loop(0, 4, block, 0)

        return 0

    lax.fori_loop(0, len(PHASES), run, 0)

    add_start(jnp.int32(2), 3)
    add_finish(jnp.int32(2), 3)
    finish_other(jnp.int32(2))

    for s in range(3):
        xm(s).wait_send()
        for h in range(2):
            xp(s, h).wait_send()
            xf(s, h).wait_send()
        for i in range(6):
            xd(s, i).wait_send()
    for k in range(6):
        wx(k).wait_send()
        for i in range(4):
            wf(k, i).wait_send()
    to_mate(2, 0).wait_send()
    to_mate(2, 1).wait_send()
    to_part(2).wait_send()
    y_store(own_seq(2), 2).wait()
    y_store(other_seq(2), 3).wait()


def neighbour_span(groups):
    short = 1
    while short * short * 4 <= groups:
        short *= 2
    return groups // short


def solution(mesh):
    tp, groups = mesh.shape["tp"], mesh.shape["dp"]
    span = neighbour_span(groups)
    assert tp == 8 and groups % (2 * span) == 0 and span % 2 == 0

    def local_layer(x_blk, ln_gain, ln_bias, w_qkv, w_out, w_up, w_down):
        n_seq, rows, d_model = x_blk.shape
        head = w_qkv.shape[3]
        ff = w_up.shape[1]
        ns, seq, blk = n_seq // 2, rows * tp, 2 * rows
        assert ns == 3 and w_qkv.shape[1:3] == (1, 3)
        chunk = min(512, d_model, ff)
        ln_rows = min(32, rows // 2)
        dims = (span, rows, d_model, head, ff, chunk, ln_rows)
        dma = pltpu.SemaphoreType.DMA
        anyspace = pl.BlockSpec(memory_space=pl.ANY)
        vmem = pl.BlockSpec(memory_space=pltpu.VMEM)

        def hbm(*shape):
            return jax.ShapeDtypeStruct(shape, BF16)

        outs = pl.pallas_call(
            functools.partial(layer_kernel, dims),
            name="layer",
            out_shape=(hbm(n_seq, rows, d_model), hbm(ns, seq, d_model), hbm(ns, seq, d_model), hbm(ns, seq, 2 * head),
                       hbm(ns, 4, rows, d_model), hbm(ns, 2, rows, d_model), hbm(ns, rows, d_model)),
            in_specs=[anyspace, vmem, vmem, anyspace, anyspace, anyspace, anyspace],
            out_specs=(anyspace,) * 7,
            scratch_shapes=[
                pltpu.VMEM((3, d_model, 2 * head), BF16),
                pltpu.VMEM((d_model, 2 * ff), BF16),
                pltpu.VMEM((2 * ff + 2 * head, d_model), BF16),
                pltpu.VMEM((2, blk, d_model), BF16),
                pltpu.VMEM((2, blk, d_model), BF16),
                pltpu.VMEM((seq, 6 * head), BF16),
                pltpu.VMEM((2, blk, 2 * head), BF16),
                pltpu.VMEM((2, blk, 2 * ff + 2 * head), BF16),
                pltpu.VMEM((blk, d_model), BF16),
                pltpu.VMEM((4, rows, d_model), BF16),
                pltpu.VMEM((3, rows, d_model), BF16),
                pltpu.VMEM((2, blk, head), F32),
                pltpu.VMEM((2, blk, 1), F32),
                pltpu.VMEM((2, blk, 1), F32),
                dma((4,)), dma((6,)), dma((6,)), dma((6, 4)), dma((6, 4)),
                dma((ns,)), dma((ns,)), dma((ns, 2)), dma((ns, 2)), dma((ns, 2)), dma((ns, 2)),
                dma((ns, 6)), dma((ns, 6)),
                dma((ns, 4)), dma((ns, 4)), dma((ns, 2)), dma((ns, 2)), dma((ns,)), dma((ns,)),
                dma((2, 2)), dma((2,)), dma((2,)), dma((2,)), dma((2,)), dma((4,)), dma((2,)),
            ],
            compiler_params=pltpu.CompilerParams(
                collective_id=0, has_side_effects=True, vmem_limit_bytes=VMEM_LIMIT),
        )(x_blk, ln_gain.reshape(1, d_model), ln_bias.reshape(1, d_model),
          jnp.transpose(w_qkv[:, 0], (1, 0, 2)), w_out, w_up, w_down)
        return outs[0]

    return jax.shard_map(
        local_layer, mesh=mesh,
        in_specs=(P("dp", "tp", None), P(), P(), P(None, "tp", None, None),
                  P("tp", None), P(None, "tp"), P("tp", None)),
        out_specs=P("dp", "tp", None), check_vma=False)
```

```python
import functools

import jax
import jax.numpy as jnp
from jax import lax
from jax.experimental import pallas as pl
from jax.experimental.pallas import tpu as pltpu
from jax.sharding import PartitionSpec as P

LN_EPS = 1e-5
MESH = pl.DeviceIdType.MESH
BF16 = jnp.bfloat16
F32 = jnp.float32
LOG2E = 1.4426950408889634
VMEM_LIMIT = 67_043_328

W_Q, W_K, W_V, UP0, UP1, DN0, DN1, OUT = range(8)
PIECES = 8
FAR, MATE, PART, OWN = range(4)
TILE, ATT, UP, DOWN = range(4)
ORDER = ("A00", "A01", "A02", "A03", "T00", "T01", "T02", "T03", "A10", "U0F", "A11", "U0M",
         "A12", "A13", "T10", "T11", "T12", "U1F", "T13", "U0P", "D0F", "A20", "A21", "A22",
         "D0M", "D1F", "A23", "U1M", "U2F", "T20", "T21", "D0P", "T22", "D1M", "T23", "U1P",
         "D2F", "D1P", "U2M", "U2P", "U0O", "D2M", "D2P", "D0O", "U1O", "D1O", "U2O", "D2O",
         )
START = ("pqQ0", "pqQ1", "phQ0", "pqQ2", "phQ1", "rm0", "phQ2", "rp00")
BEFORE = {
    0: ("ld00", "ld01"),
    2: ("rp01", "ld02"),
    3: ("pqU0", "rf0", "ld03"),
    4: ("pqU1", "ln0"),
    5: ("phU0",),
    7: ("ld10",),
    8: ("phU1", "rm1", "rp10"),
    9: ("rp11", "lo0", "ln1"),
    10: ("ld11",),
    11: ("pqD0", "ld12", "lo1"),
    13: ("rf1", "pqD1", "ld13"),
    14: ("phD0", "pqO", "ln2"),
    17: ("phD1", "ln3"),
    18: ("rm2", "rp20"),
    19: ("phO", "lo2", "lo3", "ln4"),
    20: ("rp21", "ld20"),
    21: ("ld21",),
    22: ("ld22",),
    23: ("rf2",),
    25: ("ld23",),
    27: ("lo4", "ln5"),
    28: ("ln6",),
    35: ("lo5", "lo6", "ln7"),
    38: ("lo7", "ln8"),
    39: ("lo8", "ln9"),
    40: ("lo9", "ln10"),
    44: ("lo10", "ln11"),
    46: ("lo11",),
}
ADDS = { 22: "0F", 26: "0M", 27: "1F", 33: "0P", 35: "1M", 38: "2F", 39: "1P", 43: "2M", 44: "2P", 45: "0O", 47: "1O" }
LAST_ADDS = ("2O",)

KINDS = "ATUD"
BLOCKS = "FMPO"
ITEMS = tuple((int(x[1]), BLOCKS.index(x[2])) for x in ORDER if x[0] == "U")
SLOTS = 4
PIECE = {"Q0": W_Q, "Q1": W_K, "Q2": W_V, "U0": UP0, "U1": UP1, "D0": DN0, "D1": DN1, "O": OUT}


def code_of(step):
    what, s = KINDS.index(step[0]), int(step[1])
    return 16 * what + (4 * s + int(step[2]) if what < UP else ITEMS.index((s, BLOCKS.index(step[2]))))


def pick(values, i):
    out = None
    p = 0
    while p < len(values):
        q = p + 1
        slope = None
        while q < len(values) and values[q] - values[q - 1] in ((0, 1) if slope is None else (slope,)):
            slope = values[q] - values[q - 1]
            q += 1
        val = (i + (values[p] - p)) if slope == 1 else jnp.int32(values[p])
        out = val if out is None else jnp.where(i >= p, val, out)
        p = q
    return out


def layer_kernel(dims, x, gain, bias, w_qkv, w_out, w_up, w_dn,
                 branch, ng, nout, obuf, ownp, sibin, mid,
                 wq, wu, wd, xt, nt, qk, vt, ot, ho, stage, cin, tbuf, acc, m_s, l_s,
                 w_l, wx_s, wx_r, wf_s, wf_r, nm_s, nm_r, np_s, np_r, nf_s, nf_r, nd_s, nd_r,
                 sp_s, sp_r, op_sem, t_s, t_r, p_s, p_r,
                 ln_sem, xt_sem, oo_sem, nl_sem, ol_sem, cl_sem, br_sem):
    span, rows, d_model, head, ff, chunk, ln_rows, add_rows = dims
    half = rows // 2
    blk = 2 * rows
    scale = LOG2E * head ** -0.5

    g, me = lax.axis_index("dp"), lax.axis_index("tp")
    c, j = lax.div(me, 2), lax.rem(me, 2)
    o = 1 - j
    pair = lax.div(c, 2)
    mate = c + 1 - 2 * lax.rem(c, 2)
    part = 3 - c
    far = 3 - mate
    zb, yb = lax.rem(g, 2), lax.rem(lax.div(g, span), 2)
    gz, gy = g + 1 - 2 * zb, g + span * (1 - 2 * yb)

    def dev(chip, core, group=g):
        return {"dp": group, "tp": 2 * chip + core}

    sib, mt, pt, zd, yd = dev(c, o), dev(mate, j), dev(part, j), dev(c, j, gz), dev(c, j, gy)

    def remote(src, dst, send, recv, to):
        return pltpu.make_async_remote_copy(src_ref=src, dst_ref=dst, send_sem=send, recv_sem=recv,
                                            device_id=to, device_id_type=MESH)

    def row(chip, core, extra=0):
        return pl.multiple_of((2 * chip + core) * rows + extra, half)

    def rowblock(chip):
        return pl.ds(pl.multiple_of(chip * blk, blk), blk)

    quarter = 2 * yb + zb
    q_z, q_y, q_zy = quarter + 1 - 2 * zb, quarter + 2 - 4 * yb, 3 - quarter

    def w_at(piece, q, side, hold):
        n = {UP0: d_model // 8, UP1: d_model // 8, DN0: ff // 8, DN1: ff // 8, OUT: head // 4}.get(piece, d_model // 4)
        size = n if side is None else n // 2
        off = q * n + (0 if side is None else side * size)
        if piece in (UP1, DN1):
            off = off + 4 * n
        if hold and piece in (DN0, DN1):
            off = off + ff
        if hold and piece == OUT:
            off = off + 2 * ff + head
        at = pl.ds(pl.multiple_of(off, n // 2), size)
        if piece <= W_V:
            return wq.at[piece, at, pl.ds(head, head)] if hold else w_qkv.at[piece, at, :]
        if piece <= UP1:
            return wu.at[at, pl.ds(ff, ff)] if hold else w_up.at[at, :]
        return wd.at[at, :] if hold else (w_out if piece == OUT else w_dn).at[at, :]

    def w_own(i):
        src, dst = ((w_qkv, wq.at[:, :, pl.ds(0, head)]), (w_up, wu.at[:, pl.ds(0, ff)]),
                    (w_dn, wd.at[pl.ds(0, ff), :]), (w_out, wd.at[pl.ds(2 * ff, head), :]))[i]
        return pltpu.make_async_copy(src, dst, w_l.at[i])

    def wx(k):
        return remote(w_at(k, quarter, None, False), w_at(k, quarter, None, True), wx_s.at[k], wx_r.at[k], pt)

    def wx_in(k):
        ref = w_at(k, quarter, None, True)
        return remote(ref, ref, wx_s.at[k], wx_r.at[k], pt)

    def wf(k, i):
        ref = (w_at(k, quarter, None, True) if i < 2 else w_at(k, q_y, 1, True) if i == 2 else w_at(k, q_z, 0, True))
        return remote(ref, ref, wf_s.at[k, i], wf_r.at[k, i], yd if i in (1, 3) else zd)

    def wf_in(k, i):
        ref = w_at(k, (q_z, q_y, q_zy, q_zy)[i], (None, None, 1, 0)[i], True)
        return remote(ref, ref, wf_s.at[k, i], wf_r.at[k, i], yd if i in (1, 3) else zd)

    def pass_quarter(k):
        wx_in(k).wait_recv()
        wf(k, 0).start()
        wf(k, 1).start()

    def pass_halves(k):
        wf_in(k, 0).wait_recv()
        wf_in(k, 1).wait_recv()
        wf(k, 2).start()
        wf(k, 3).start()

    def have(k):
        wf_in(k, 2).wait_recv()
        wf_in(k, 3).wait_recv()

    def own_seq(s):
        return 2 * s + pair

    def other_seq(s):
        return 2 * s + 1 - pair

    def n_own(s):
        return ng.at[s, pl.ds(row(c, j), rows)]

    def nm(s):
        return remote(n_own(s), n_own(s), nm_s.at[s], nm_r.at[s], mt)

    def nm_in(s):
        ref = ng.at[s, pl.ds(row(mate, j), rows)]
        return remote(ref, ref, nm_s.at[s], nm_r.at[s], mt)

    def np_(s, h):
        return remote(nout.at[s, pl.ds(h * half, half)], ng.at[s, pl.ds(row(c, j, h * half), half)],
                      np_s.at[s, h], np_r.at[s, h], pt)

    def np_in(s, h):
        ref = ng.at[s, pl.ds(row(part, j, h * half), half)]
        return remote(ref, ref, np_s.at[s, h], np_r.at[s, h], pt)

    def nf(s, h):
        ref = ng.at[s, pl.ds(row(part, j, h * half), half)]
        return remote(ref, ref, nf_s.at[s, h], nf_r.at[s, h], mt)

    def nf_in(s, h):
        ref = ng.at[s, pl.ds(row(far, j, h * half), half)]
        return remote(ref, ref, nf_s.at[s, h], nf_r.at[s, h], mt)

    def nd(s, i, core=j):
        ref = (ng.at[s, pl.ds(row(c if i == 0 else mate, core), rows)] if i < 2 else
               ng.at[s, pl.ds(row(part if i < 4 else far, core, (i % 2) * half), half)])
        return remote(ref, ref, nd_s.at[s, i], nd_r.at[s, i], sib)

    def nd_in(s, i):
        return nd(s, i, o)

    def relay_mate(s):
        nm_in(s).wait_recv()
        nd(s, 1).start()

    def relay_part(s, h):
        np_in(s, h).wait_recv()
        nf(s, h).start()
        nd(s, 2 + h).start()
        if h == 1 and s < 2:
            nm(s + 1).start()

    def relay_far(s):
        for h in range(2):
            nf_in(s, h).wait_recv()
            nd(s, 4 + h).start()

    def ln_buf(b):
        return (xt if b < 4 else nt).at[(b // 2) % 2, pl.ds((b % 2) * rows, rows)]

    def ln_load(b):
        return pltpu.make_async_copy(x.at[own_seq(b // 2) if b % 2 else other_seq(b // 2)], ln_buf(b), ln_sem.at[b])

    def ln_store(b):
        return pltpu.make_async_copy(ln_buf(b), n_own(b // 2) if b % 2 else nout.at[b // 2], ln_sem.at[b])

    def normalise(b):
        ln_load(b).wait()
        buf = ln_buf(b)

        def norm(r, _):
            rr = pl.ds(pl.multiple_of(r * ln_rows, ln_rows), ln_rows)
            v = buf[rr, :].astype(F32)
            mean = jnp.mean(v, axis=-1, keepdims=True)
            cen = v - mean
            var = jnp.mean(cen * cen, axis=-1, keepdims=True)
            buf[rr, :] = (cen * lax.rsqrt(var + LN_EPS) * gain[...] + bias[...]).astype(BF16)
            return 0

        lax.fori_loop(0, rows // ln_rows, norm, 0)
        ln_store(b).start()

    barrier = pltpu.get_barrier_semaphore()
    for to in (sib, mt, pt, zd, yd):
        pl.semaphore_signal(barrier, inc=1, device_id=to, device_id_type=MESH)
    for b in range(6):
        ln_load(b).start()
    for i in range(4):
        w_own(i).start()
    with jax.named_scope("norm0"):
        normalise(0)
    with jax.named_scope("norm1"):
        normalise(1)
    with jax.named_scope("barrier"):
        pl.semaphore_wait(barrier, 5)

    def send_part(s):
        ln_store(2 * s).wait()
        np_(s, 0).start()
        np_(s, 1).start()

    for k in (W_Q, W_K, W_V):
        wx(k).start()
    send_part(0)
    ln_store(1).wait()
    nm(0).start()
    nd(0, 0).start()
    wx(UP0).start()
    wx(UP1).start()
    with jax.named_scope("norm2"):
        normalise(2)
    with jax.named_scope("norm3"):
        normalise(3)
    send_part(1)
    for k in (DN0, DN1, OUT):
        wx(k).start()
    with jax.named_scope("norm4"):
        normalise(4)
    with jax.named_scope("norm5"):
        normalise(5)
    send_part(2)
    for s in (1, 2):
        ln_store(2 * s + 1).wait()
        nd(s, 0).start()

    def tile_chip(i):
        return jnp.where(i == 0, c, jnp.where(i == 1, mate, jnp.where(i == 2, part, far)))

    def mlp_chip(kind):
        return jnp.where(kind == FAR, far, jnp.where(kind == MATE, mate, jnp.where(kind == PART, part, c)))

    def tile_copy(s, i):
        return pltpu.make_async_copy(ng.at[s, rowblock(tile_chip(i))], xt.at[lax.rem(i, 2)], xt_sem.at[lax.rem(i, 2)])

    def tile_start(s, i):
        for n in ((0,), (1,), (2, 3), (4, 5))[i]:
            nd_in(s, n).wait_recv()
        tile_copy(s, jnp.int32(i)).start()

    def tile(index):
        s, i = lax.div(index, 4), lax.rem(index, 4)
        with jax.named_scope("tile_wait"):
            tile_copy(s, i).wait()
        slot = lax.rem(i, 2)
        base = rowblock(tile_chip(i))
        for t in range(2):
            qk[base, pl.ds(t * 2 * head, 2 * head)] = jnp.dot(
                xt[slot], wq[t], preferred_element_type=F32).astype(BF16)
        vt[:, base] = jnp.transpose(jnp.dot(xt[slot], wq[2], preferred_element_type=F32)).astype(BF16)

    def dot_t(a, b):
        return lax.dot_general(a, b, (((1,), (1,)), ((), ())), preferred_element_type=F32)

    def o_out(s, i):
        return pltpu.make_async_copy(ot.at[lax.rem(i, 2)], obuf.at[s, rowblock(i)], oo_sem.at[lax.rem(i, 2)])

    def attend(index):
        s, i = lax.div(index, 4), lax.rem(index, 4)
        slot = lax.rem(i, 2)

        @pl.when(i >= 2)
        def _():
            o_out(s, i).wait()

        mine = rowblock(i)
        causal = (lax.broadcasted_iota(jnp.int32, (blk, blk), 0)
                  <= lax.broadcasted_iota(jnp.int32, (blk, blk), 1))
        for h in range(2):
            hd = pl.ds(h * head, head)
            sc = jnp.where(causal, dot_t(qk[mine, pl.ds((2 + h) * head, head)], qk[mine, hd]), -jnp.inf)
            top = jnp.max(sc, axis=0, keepdims=True)
            p = jnp.exp2((sc - top) * scale)
            m_s[h] = top
            l_s[h] = jnp.sum(p, axis=0, keepdims=True)
            acc[h] = jnp.dot(vt[hd, mine], p.astype(BF16), preferred_element_type=F32)

        def earlier(t, _):
            there = rowblock(t)
            for h in range(2):
                hd = pl.ds(h * head, head)
                sc = dot_t(qk[there, pl.ds((2 + h) * head, head)], qk[mine, hd])
                old = m_s[h]
                top = jnp.maximum(old, jnp.max(sc, axis=0, keepdims=True))
                p = jnp.exp2((sc - top) * scale)
                fade = jnp.exp2((old - top) * scale)
                m_s[h] = top
                l_s[h] = l_s[h] * fade + jnp.sum(p, axis=0, keepdims=True)
                acc[h] = acc[h] * fade + jnp.dot(vt[hd, there], p.astype(BF16), preferred_element_type=F32)
            return 0

        lax.fori_loop(0, i, earlier, 0)
        for h in range(2):
            ot[slot, :, pl.ds(h * head, head)] = jnp.transpose(acc[h] * (1.0 / l_s[h])).astype(BF16)
        o_out(s, i).start()

        @pl.when(i == 3)
        def _():
            o_out(s, i - 1).wait()
            o_out(s, i).wait()

    def sp(s, kind, slot):
        return remote(stage.at[slot, pl.ds(pl.multiple_of(o * rows, rows), rows)], sibin.at[s, kind],
                      sp_s.at[s, kind], sp_r.at[s, kind], sib)

    def own_store(s, kind, slot):
        return pltpu.make_async_copy(stage.at[slot, pl.ds(pl.multiple_of(j * rows, rows), rows)], ownp.at[s, kind],
                                     op_sem.at[slot])

    def to_mate(s, kind):
        return remote(tbuf.at[kind], mid.at[s, kind], t_s.at[s, kind], t_r.at[s, kind], mt)

    def from_mate(s, kind):
        return remote(mid.at[s, kind], mid.at[s, kind], t_s.at[s, kind], t_r.at[s, kind], mt)

    def to_part(s):
        return remote(tbuf.at[PART], branch.at[own_seq(s)], p_s.at[s], p_r.at[s], pt)

    def from_part(s):
        return remote(branch.at[other_seq(s)], branch.at[other_seq(s)], p_s.at[s], p_r.at[s], pt)

    def keep(s):
        return pltpu.make_async_copy(tbuf.at[OWN], branch.at[own_seq(s)], br_sem)

    def add_loads(s, kind):
        srcs = [ownp.at[s, kind], sibin.at[s, kind]] + ([mid.at[s, kind - PART]] if kind >= PART else [])
        return [pltpu.make_async_copy(src, cin.at[n], cl_sem.at[n]) for n, src in enumerate(srcs)]

    def add_start(s, kind):
        remote(sibin.at[s, kind], sibin.at[s, kind], sp_s.at[s, kind], sp_r.at[s, kind], sib).wait_recv()
        if kind >= PART:
            from_mate(s, kind - PART).wait_recv()

        @pl.when(s > 0)
        def _():
            if kind < PART:
                to_mate(s - 1, kind).wait_send()
            elif kind == PART:
                to_part(s - 1).wait_send()
            else:
                keep(s - 1).wait()

        for ld in add_loads(s, kind):
            ld.start()

    def add_finish(s, kind):
        for ld in add_loads(s, kind):
            ld.wait()

        def add(r, _):
            rr = pl.ds(pl.multiple_of(r * add_rows, add_rows), add_rows)
            total = cin[0, rr, :].astype(F32) + cin[1, rr, :].astype(F32)
            if kind >= PART:
                total = total + cin[2, rr, :].astype(F32)
            tbuf[kind, rr, :] = total.astype(BF16)
            return 0

        lax.fori_loop(0, rows // add_rows, add, 0)
        if kind < PART:
            to_mate(s, kind).start()
        elif kind == PART:
            to_part(s).start()
        else:
            keep(s).start()

    def item(k):
        return pick([s for s, _ in ITEMS], k), pick([b for _, b in ITEMS], k)

    def n_load(k):
        s, kind = item(k)
        return pltpu.make_async_copy(ng.at[s, rowblock(mlp_chip(kind))], nt.at[lax.rem(k, 2)], nl_sem.at[lax.rem(k, 2)])

    def o_load(k):
        s, kind = item(k)
        return pltpu.make_async_copy(obuf.at[s, rowblock(mlp_chip(kind))],
                                     ho.at[lax.rem(k, SLOTS), :, pl.ds(2 * ff, 2 * head)], ol_sem.at[lax.rem(k, SLOTS)])

    def mlp_up(k):
        with jax.named_scope("n_wait"):
            n_load(k).wait()

        @pl.when(k == 0)
        def _():
            with jax.named_scope("have_up"):
                have(UP0)
                have(UP1)
                w_own(1).wait()

        src, dst = lax.rem(k, 2), lax.rem(k, SLOTS)

        def up(t, _):
            cols = pl.ds(pl.multiple_of(t * chunk, chunk), chunk)
            hid = jnp.dot(nt[src], wu[:, cols], preferred_element_type=F32)
            ho[dst, :, cols] = (0.5 * hid * (1.0 + lax.erf(hid * 0.7071067811865476))).astype(BF16)
            return 0

        lax.fori_loop(0, 2 * ff // chunk, up, 0, unroll=2)

    def stage_free(k):
        s, kind = item(k)
        sp(s, kind, lax.rem(k, 2)).wait_send()

    def own_stored(k):
        s, kind = item(k)
        own_store(s, kind, lax.rem(k, 2)).wait()

    def mlp_down(k):
        s, kind = item(k)
        slot, src = lax.rem(k, 2), lax.rem(k, SLOTS)
        with jax.named_scope("o_wait"):
            o_load(k).wait()

        @pl.when(k == 0)
        def _():
            with jax.named_scope("have_dn"):
                for p in (DN0, DN1, OUT):
                    have(p)
                w_own(2).wait()
                w_own(3).wait()

        @pl.when(k >= 2)
        def _():
            with jax.named_scope("stage_free"):
                stage_free(k - 2)

        def down(t, _):
            cols = pl.ds(pl.multiple_of(t * chunk, chunk), chunk)
            stage[slot, :, cols] = jnp.dot(ho[src], wd[:, cols], preferred_element_type=F32).astype(BF16)
            return 0

        lax.fori_loop(0, d_model // chunk, down, 0, unroll=2)
        sp(s, kind, slot).start()
        own_store(s, kind, slot).start()

    def act(name):
        what, arg = name[:2], name[2:]
        if what == "pq":
            pass_quarter(PIECE[arg])
        elif what == "ph":
            pass_halves(PIECE[arg])
        elif what == "rm":
            relay_mate(int(arg))
        elif what == "rp":
            relay_part(int(arg[0]), int(arg[1]))
        elif what == "rf":
            relay_far(int(arg))
        elif what == "ld":
            tile_start(int(arg[0]), int(arg[1]))
        elif what == "ln":
            n_load(jnp.int32(int(arg))).start()
        else:
            o_load(jnp.int32(int(arg))).start()

    for name in START:
        with jax.named_scope(name):
            act(name)
    with jax.named_scope("have_qkv"):
        w_own(0).wait()
        for k in (W_Q, W_K, W_V):
            have(k)

    codes = [code_of(step) for step in ORDER]
    adds = [4 * int(ADDS[t][0]) + BLOCKS.index(ADDS[t][1]) if t in ADDS else -1 for t in range(len(ORDER))]
    group = 8

    def adding(code, do):
        for kind in range(4):
            @pl.when((code >= 0) & (lax.rem(code, 4) == kind))
            def _(kind=kind):
                do(lax.div(code, 4), kind)

    def run(t, before):
        for r in range(0, len(ORDER), group):
            @pl.when(lax.div(t, group) == r // group)
            def _(r=r):
                for p in range(r, r + group):
                    if p in BEFORE:
                        @pl.when(t == p)
                        def _(p=p):
                            for name in BEFORE[p]:
                                with jax.named_scope(name):
                                    act(name)

        code, add = pick(codes, t), pick(adds, t)
        with jax.named_scope("add_start"):
            adding(add, add_start)
        what, index = lax.div(code, 16), lax.rem(code, 16)
        names = ("TILE", "ATT", "UP", "DOWN")
        for kind, body in ((TILE, tile), (ATT, attend), (UP, mlp_up), (DOWN, mlp_down)):
            @pl.when(what == kind)
            def _(kind=kind, body=body):
                with jax.named_scope(names[kind]):
                    body(index)

        with jax.named_scope("add_finish"):
            adding(add, add_finish)

        @pl.when(lax.div(before, 16) == DOWN)
        def _():
            own_stored(lax.rem(before, 16))

        return code

    lax.fori_loop(0, len(ORDER), run, jnp.int32(0))
    own_stored(jnp.int32(len(ITEMS) - 1))
    for add in LAST_ADDS:
        s, kind = jnp.int32(int(add[0])), BLOCKS.index(add[1])
        with jax.named_scope("last_add"):
            add_start(s, kind)
            add_finish(s, kind)
    with jax.named_scope("last_part"):
        for s in range(3):
            from_part(s).wait_recv()
    keep(2).wait()

    for k in range(len(ITEMS) - 2, len(ITEMS)):
        stage_free(jnp.int32(k))
    for s in range(3):
        nm(s).wait_send()
        for h in range(2):
            np_(s, h).wait_send()
            nf(s, h).wait_send()
        for i in range(6):
            nd(s, i).wait_send()
    for k in range(PIECES):
        wx(k).wait_send()
        for i in range(4):
            wf(k, i).wait_send()
    to_mate(2, FAR).wait_send()
    to_mate(2, MATE).wait_send()
    to_part(2).wait_send()


def neighbour_span(groups):
    short = 1
    while short * short * 4 <= groups:
        short *= 2
    return groups // short


def solution(mesh):
    tp, groups = mesh.shape["tp"], mesh.shape["dp"]
    span = neighbour_span(groups)
    assert tp == 8 and groups % (2 * span) == 0 and span % 2 == 0

    def local_layer(x_blk, ln_gain, ln_bias, w_qkv, w_out, w_up, w_down):
        n_seq, rows, d_model = x_blk.shape
        head = w_qkv.shape[3]
        ff = w_up.shape[1]
        ns, seq, blk = n_seq // 2, rows * tp, 2 * rows
        assert ns == 3 and w_qkv.shape[1:3] == (1, 3)
        chunk = min(512, d_model, ff)
        ln_rows, add_rows = min(64, rows // 2), min(16, rows // 2)
        dims = (span, rows, d_model, head, ff, chunk, ln_rows, add_rows)
        dma = pltpu.SemaphoreType.DMA
        anyspace = pl.BlockSpec(memory_space=pl.ANY)
        vmem = pl.BlockSpec(memory_space=pltpu.VMEM)

        def hbm(*shape):
            return jax.ShapeDtypeStruct(shape, BF16)

        outs = pl.pallas_call(
            functools.partial(layer_kernel, dims),
            name="layer",
            out_shape=(hbm(n_seq, rows, d_model), hbm(ns, seq, d_model), hbm(ns, rows, d_model), hbm(ns, seq, 2 * head),
                       hbm(ns, 4, rows, d_model), hbm(ns, 4, rows, d_model), hbm(ns, 2, rows, d_model)),
            in_specs=[anyspace, vmem, vmem, anyspace, anyspace, anyspace, anyspace],
            out_specs=(anyspace,) * 7,
            scratch_shapes=[
                pltpu.VMEM((3, d_model, 2 * head), BF16),
                pltpu.VMEM((d_model, 2 * ff), BF16),
                pltpu.VMEM((2 * ff + 2 * head, d_model), BF16),
                pltpu.VMEM((2, blk, d_model), BF16),
                pltpu.VMEM((2, blk, d_model), BF16),
                pltpu.VMEM((seq, 4 * head), BF16),
                pltpu.VMEM((2 * head, seq), BF16),
                pltpu.VMEM((2, blk, 2 * head), BF16),
                pltpu.VMEM((SLOTS, blk, 2 * ff + 2 * head), BF16),
                pltpu.VMEM((2, blk, d_model), BF16),
                pltpu.VMEM((3, rows, d_model), BF16),
                pltpu.VMEM((4, rows, d_model), BF16),
                pltpu.VMEM((2, head, blk), F32),
                pltpu.VMEM((2, 1, blk), F32),
                pltpu.VMEM((2, 1, blk), F32),
                dma((4,)), dma((PIECES,)), dma((PIECES,)), dma((PIECES, 4)), dma((PIECES, 4)),
                dma((ns,)), dma((ns,)), dma((ns, 2)), dma((ns, 2)), dma((ns, 2)), dma((ns, 2)),
                dma((ns, 6)), dma((ns, 6)),
                dma((ns, 4)), dma((ns, 4)), dma((2,)), dma((ns, 2)), dma((ns, 2)), dma((ns,)), dma((ns,)),
                dma((6,)), dma((2,)), dma((2,)), dma((2,)), dma((SLOTS,)), dma((3,)), dma,
            ],
            compiler_params=pltpu.CompilerParams(
                collective_id=0, has_side_effects=True, vmem_limit_bytes=VMEM_LIMIT),
        )(x_blk, ln_gain.reshape(1, d_model), ln_bias.reshape(1, d_model),
          jnp.transpose(w_qkv[:, 0], (1, 0, 2)), w_out, w_up, w_down)
        return (x_blk.astype(F32) + outs[0].astype(F32)).astype(BF16)

    return jax.shard_map(
        local_layer, mesh=mesh,
        in_specs=(P("dp", "tp", None), P(), P(), P(None, "tp", None, None),
                  P("tp", None), P(None, "tp"), P("tp", None)),
        out_specs=P("dp", "tp", None), check_vma=False)
```

```python
import functools

import jax
import jax.numpy as jnp
from jax import lax
from jax.experimental import pallas as pl
from jax.experimental.pallas import tpu as pltpu
from jax.sharding import PartitionSpec as P

LN_EPS = 1e-5
MESH = pl.DeviceIdType.MESH
BF16 = jnp.bfloat16
F32 = jnp.float32
LOG2E = 1.4426950408889634
VMEM_LIMIT = 67_043_328

W_Q, W_K, W_V, UP0, UP1, DN0, DN1, DN2, DN3, OUT = range(10)
PIECES = 10
FAR, MATE, PART, OWN = range(4)
TILE, ATT, UP, DOWN = range(4)
INTER = ("Q0", "Q1", "Q2", "n0", "U1", "U0", "n1", "D1", "D3", "O", "D0", "D2", "n2")
ORDER = ("A00", "A01", "A02", "A03", "T00", "T01", "T02", "T03", "A10", "A11", "A12", "U0F",
         "U0M", "U1P", "A13", "U1F", "T10", "T11", "T12", "T13", "A20", "D0F", "A21", "D0M",
         "A22", "A23", "D1P", "T20", "U1M", "D1F", "U0P", "D1M", "U2F", "D0P", "T21", "T22",
         "T23", "D2F", "U2M", "U2P", "U1O", "D2M", "U0O", "D2P", "D1O", "D0O", "U2O", "D2O",
         )
START = ("pqQ0", "pqQ1", "phQ0", "pqQ2", "phQ1", "rm0", "phQ2", "rp00")
BEFORE = {
    0: ("ld00", "ld01"),
    2: ("rp01", "ld02"),
    3: ("pqU1", "rf0", "ld03"),
    4: ("pqU0", "ln0"),
    5: ("phU1",),
    7: ("ld10",),
    8: ("phU0", "rm1", "rp10"),
    9: ("ld11",),
    10: ("rp11", "ld12"),
    11: ("pqD1", "ln1", "ow0", "lo0"),
    12: ("pqD3", "ln2", "lo1"),
    13: ("phD1", "pqO", "rf1"),
    14: ("pqD0", "phD3", "ld13"),
    15: ("ln3", "ln4"),
    16: ("pqD2", "phO"),
    18: ("phD0",),
    19: ("rm2", "rp20", "ld20"),
    20: ("phD2", "ow1", "lo2", "lo3"),
    21: ("rp21", "ld21"),
    23: ("ad0F", "ld22"),
    24: ("rf2",),
    25: ("ld23",),
    28: ("ln5", "lo4"),
    30: ("ln6", "lo5"),
    32: ("ln7",),
    35: ("ad0P",),
    37: ("ow2", "lo6"),
    38: ("ln8", "lo7"),
    39: ("ln9", "lo8"),
    40: ("ad1P", "ln10", "lo9"),
    42: ("ln11", "lo10"),
    45: ("ad2P",),
    46: ("lo11",),
}
ADDS = { 25: "0M", 31: "1F", 33: "1M", 39: "2F", 43: "2M", 46: "1O", 47: "0O" }
LAST_ADDS = ("2O",)

KINDS = "ATUD"
BLOCKS = "FMPO"
ITEMS = tuple((int(x[1]), BLOCKS.index(x[2])) for x in ORDER if x[0] == "U")
SLOTS = 4
PIECE = {"Q0": W_Q, "Q1": W_K, "Q2": W_V, "U0": UP0, "U1": UP1,
         "D0": DN0, "D1": DN1, "D2": DN2, "D3": DN3, "O": OUT}


def code_of(step):
    what, s = KINDS.index(step[0]), int(step[1])
    return 16 * what + (4 * s + int(step[2]) if what < UP else ITEMS.index((s, BLOCKS.index(step[2]))))


def pick(values, i, bits):
    per = 30 // bits
    words = [sum(v << bits * p for p, v in enumerate(values[w:w + per])) for w in range(0, len(values), per)]
    word, at = lax.div(i, per), lax.rem(i, per)
    packed = jnp.int32(words[0])
    for w in range(1, len(words)):
        packed = jnp.where(word == w, words[w], packed)
    out = packed
    for p in range(1, per):
        out = jnp.where(at == p, lax.div(packed, 1 << bits * p), out)
    return lax.rem(out, 1 << bits)


def sums():
    seq = []
    for t in range(len(ORDER)):
        seq += [(name[2:], t) for name in BEFORE.get(t, ()) if name[:2] == "ad"]
        if t in ADDS:
            seq.append((ADDS[t], t))
    seq += [(name, None) for name in LAST_ADDS]
    last, before = {}, {}
    for name, _ in seq:
        before[name] = last.get(name[1], -1)
        last[name[1]] = int(name[0])
    assert len(seq) == len(ITEMS)
    return before, last


BEFORE_SUM, LAST_SUM = sums()


def layer_kernel(dims, x, gain, bias, w_qkv, w_out, w_up, w_dn,
                 branch, ng, nout, obuf, ownp, sibin, mid,
                 wq, wu, wd, xt, nt, qk, vt, ot, ho, stage, cin, tbuf, acc, m_s, l_s,
                 w_l, wx_s, wx_r, wf_s, wf_r, nm_s, nm_r, np_s, np_r, nf_s, nf_r, nd_s, nd_r,
                 sp_s, sp_r, op_sem, t_s, t_r, p_s, p_r,
                 ln_sem, xt_sem, oo_sem, nl_sem, ol_sem, cl_sem, br_sem):
    span, rows, d_model, head, ff, chunk, ln_rows, add_rows = dims
    half = rows // 2
    blk = 2 * rows
    scale = LOG2E * head ** -0.5

    g, me = lax.axis_index("dp"), lax.axis_index("tp")
    c, j = lax.div(me, 2), lax.rem(me, 2)
    o = 1 - j
    pair = lax.div(c, 2)
    mate = c + 1 - 2 * lax.rem(c, 2)
    part = 3 - c
    far = 3 - mate
    zb, yb = lax.rem(g, 2), lax.rem(lax.div(g, span), 2)
    gz, gy = g + 1 - 2 * zb, g + span * (1 - 2 * yb)

    def dev(chip, core, group=g):
        return {"dp": group, "tp": 2 * chip + core}

    sib, mt, pt, zd, yd = dev(c, o), dev(mate, j), dev(part, j), dev(c, j, gz), dev(c, j, gy)

    def remote(src, dst, send, recv, to):
        return pltpu.make_async_remote_copy(src_ref=src, dst_ref=dst, send_sem=send, recv_sem=recv,
                                            device_id=to, device_id_type=MESH)

    def row(chip, core, extra=0):
        return pl.multiple_of((2 * chip + core) * rows + extra, half)

    def rowblock(chip):
        return pl.ds(pl.multiple_of(chip * blk, blk), blk)

    quarter = 2 * yb + zb
    q_z, q_y, q_zy = quarter + 1 - 2 * zb, quarter + 2 - 4 * yb, 3 - quarter

    def w_at(piece, q, side, hold):
        n = head // 4 if piece == OUT else ff // 16 if piece >= DN0 else d_model // 8 if piece >= UP0 else d_model // 4
        size = n if side is None else n // 2
        off = q * n + (0 if side is None else side * size)
        if UP0 <= piece <= DN3:
            off = off + (piece - (UP0 if piece <= UP1 else DN0)) * 4 * n
        if hold and DN0 <= piece <= DN3:
            off = off + ff
        if hold and piece == OUT:
            off = off + 2 * ff + head
        at = pl.ds(pl.multiple_of(off, n // 2), size)
        if piece <= W_V:
            return wq.at[piece, at, pl.ds(head, head)] if hold else w_qkv.at[piece, at, :]
        if piece <= UP1:
            return wu.at[at, pl.ds(ff, ff)] if hold else w_up.at[at, :]
        return wd.at[at, :] if hold else (w_out if piece == OUT else w_dn).at[at, :]

    def w_own(i):
        src, dst = ((w_qkv, wq.at[:, :, pl.ds(0, head)]), (w_up, wu.at[:, pl.ds(0, ff)]),
                    (w_dn, wd.at[pl.ds(0, ff), :]), (w_out, wd.at[pl.ds(2 * ff, head), :]))[i]
        return pltpu.make_async_copy(src, dst, w_l.at[i])

    def wx(k):
        return remote(w_at(k, quarter, None, False), w_at(k, quarter, None, True), wx_s.at[k], wx_r.at[k], pt)

    def wx_in(k):
        ref = w_at(k, quarter, None, True)
        return remote(ref, ref, wx_s.at[k], wx_r.at[k], pt)

    def wf(k, i):
        ref = (w_at(k, quarter, None, True) if i < 2 else w_at(k, q_y, 1, True) if i == 2 else w_at(k, q_z, 0, True))
        return remote(ref, ref, wf_s.at[k, i], wf_r.at[k, i], yd if i in (1, 3) else zd)

    def wf_in(k, i):
        ref = w_at(k, (q_z, q_y, q_zy, q_zy)[i], (None, None, 1, 0)[i], True)
        return remote(ref, ref, wf_s.at[k, i], wf_r.at[k, i], yd if i in (1, 3) else zd)

    def pass_quarter(k):
        wx_in(k).wait_recv()
        wf(k, 0).start()
        wf(k, 1).start()

    def pass_halves(k):
        wf_in(k, 0).wait_recv()
        wf_in(k, 1).wait_recv()
        wf(k, 2).start()
        wf(k, 3).start()

    def have(k):
        wf_in(k, 2).wait_recv()
        wf_in(k, 3).wait_recv()

    def own_seq(s):
        return 2 * s + pair

    def other_seq(s):
        return 2 * s + 1 - pair

    def n_own(s):
        return ng.at[s, pl.ds(row(c, j), rows)]

    def nm(s):
        return remote(n_own(s), n_own(s), nm_s.at[s], nm_r.at[s], mt)

    def nm_in(s):
        ref = ng.at[s, pl.ds(row(mate, j), rows)]
        return remote(ref, ref, nm_s.at[s], nm_r.at[s], mt)

    def np_(s, h):
        return remote(nout.at[s, pl.ds(h * half, half)], ng.at[s, pl.ds(row(c, j, h * half), half)],
                      np_s.at[s, h], np_r.at[s, h], pt)

    def np_in(s, h):
        ref = ng.at[s, pl.ds(row(part, j, h * half), half)]
        return remote(ref, ref, np_s.at[s, h], np_r.at[s, h], pt)

    def nf(s, h):
        ref = ng.at[s, pl.ds(row(part, j, h * half), half)]
        return remote(ref, ref, nf_s.at[s, h], nf_r.at[s, h], mt)

    def nf_in(s, h):
        ref = ng.at[s, pl.ds(row(far, j, h * half), half)]
        return remote(ref, ref, nf_s.at[s, h], nf_r.at[s, h], mt)

    def nd(s, i, core=j):
        ref = (ng.at[s, pl.ds(row(c if i == 0 else mate, core), rows)] if i < 2 else
               ng.at[s, pl.ds(row(part if i < 4 else far, core, (i % 2) * half), half)])
        return remote(ref, ref, nd_s.at[s, i], nd_r.at[s, i], sib)

    def nd_in(s, i):
        return nd(s, i, o)

    def relay_mate(s):
        nm_in(s).wait_recv()
        nd(s, 1).start()

    def relay_part(s, h):
        np_in(s, h).wait_recv()
        nf(s, h).start()
        nd(s, 2 + h).start()
        if h == 1 and s < 2:
            nm(s + 1).start()

    def relay_far(s):
        for h in range(2):
            nf_in(s, h).wait_recv()
            nd(s, 4 + h).start()

    def ln_buf(b):
        return (xt if b < 4 else nt).at[(b // 2) % 2, pl.ds((b % 2) * rows, rows)]

    def ln_load(b):
        return pltpu.make_async_copy(x.at[own_seq(b // 2) if b % 2 else other_seq(b // 2)], ln_buf(b), ln_sem.at[b])

    def ln_store(b):
        return pltpu.make_async_copy(ln_buf(b), n_own(b // 2) if b % 2 else nout.at[b // 2], ln_sem.at[b])

    def normalise(b):
        ln_load(b).wait()
        buf = ln_buf(b)

        def norm(r, _):
            rr = pl.ds(pl.multiple_of(r * ln_rows, ln_rows), ln_rows)
            v = buf[rr, :].astype(F32)
            mean = jnp.mean(v, axis=-1, keepdims=True)
            cen = v - mean
            var = jnp.mean(cen * cen, axis=-1, keepdims=True)
            buf[rr, :] = (cen * lax.rsqrt(var + LN_EPS) * gain[...] + bias[...]).astype(BF16)
            return 0

        lax.fori_loop(0, rows // ln_rows, norm, 0)
        ln_store(b).start()

    barrier = pltpu.get_barrier_semaphore()
    for to in (sib, mt, pt, zd, yd):
        pl.semaphore_signal(barrier, inc=1, device_id=to, device_id_type=MESH)
    for b in range(6):
        ln_load(b).start()
    for i in range(4):
        w_own(i).start()
    with jax.named_scope("norm0"):
        normalise(0)
    with jax.named_scope("norm1"):
        normalise(1)
    with jax.named_scope("barrier"):
        pl.semaphore_wait(barrier, 5)

    def send_part(s):
        ln_store(2 * s).wait()
        np_(s, 0).start()
        np_(s, 1).start()

    for name in INTER:
        if name[0] != "n":
            wx(PIECE[name]).start()
            continue
        s = int(name[1])
        if s > 0:
            normalise(2 * s)
            normalise(2 * s + 1)
        send_part(s)
        ln_store(2 * s + 1).wait()
        if s == 0:
            nm(0).start()
        nd(s, 0).start()

    def tile_chip(i):
        return jnp.where(i == 0, c, jnp.where(i == 1, mate, jnp.where(i == 2, part, far)))

    def mlp_chip(kind):
        return jnp.where(kind == FAR, far, jnp.where(kind == MATE, mate, jnp.where(kind == PART, part, c)))

    def tile_copy(s, i):
        return pltpu.make_async_copy(ng.at[s, rowblock(tile_chip(i))], xt.at[lax.rem(i, 2)], xt_sem.at[lax.rem(i, 2)])

    def tile_start(s, i):
        for n in ((0,), (1,), (2, 3), (4, 5))[i]:
            nd_in(s, n).wait_recv()
        tile_copy(s, jnp.int32(i)).start()

    def tile(index):
        s, i = lax.div(index, 4), lax.rem(index, 4)
        with jax.named_scope("tile_wait"):
            tile_copy(s, i).wait()
        slot = lax.rem(i, 2)
        base = rowblock(tile_chip(i))
        for t in range(2):
            qk[base, pl.ds(t * 2 * head, 2 * head)] = jnp.dot(
                xt[slot], wq[t], preferred_element_type=F32).astype(BF16)
        vt[:, base] = jnp.transpose(jnp.dot(xt[slot], wq[2], preferred_element_type=F32)).astype(BF16)

    def dot_t(a, b):
        return lax.dot_general(a, b, (((1,), (1,)), ((), ())), preferred_element_type=F32)

    def o_out(s, i):
        return pltpu.make_async_copy(ot.at[lax.rem(i, 2)], obuf.at[s, rowblock(i)], oo_sem.at[lax.rem(i, 2)])

    def attend(index):
        s, i = lax.div(index, 4), lax.rem(index, 4)
        slot = lax.rem(i, 2)

        @pl.when(i >= 2)
        def _():
            o_out(s, i).wait()

        mine = rowblock(i)
        causal = (lax.broadcasted_iota(jnp.int32, (blk, blk), 0)
                  <= lax.broadcasted_iota(jnp.int32, (blk, blk), 1))
        for h in range(2):
            hd = pl.ds(h * head, head)
            sc = jnp.where(causal, dot_t(qk[mine, pl.ds((2 + h) * head, head)], qk[mine, hd]), -jnp.inf)
            top = jnp.max(sc, axis=0, keepdims=True)
            p = jnp.exp2((sc - top) * scale)
            m_s[h] = top
            l_s[h] = jnp.sum(p, axis=0, keepdims=True)
            acc[h] = jnp.dot(vt[hd, mine], p.astype(BF16), preferred_element_type=F32)

        def earlier(t, _):
            there = rowblock(t)
            for h in range(2):
                hd = pl.ds(h * head, head)
                sc = dot_t(qk[there, pl.ds((2 + h) * head, head)], qk[mine, hd])
                old = m_s[h]
                top = jnp.maximum(old, jnp.max(sc, axis=0, keepdims=True))
                p = jnp.exp2((sc - top) * scale)
                fade = jnp.exp2((old - top) * scale)
                m_s[h] = top
                l_s[h] = l_s[h] * fade + jnp.sum(p, axis=0, keepdims=True)
                acc[h] = acc[h] * fade + jnp.dot(vt[hd, there], p.astype(BF16), preferred_element_type=F32)
            return 0

        lax.fori_loop(0, i, earlier, 0)
        for h in range(2):
            ot[slot, :, pl.ds(h * head, head)] = jnp.transpose(acc[h] * (1.0 / l_s[h])).astype(BF16)
        o_out(s, i).start()

    def context_out(s):
        for i in (2, 3):
            o_out(jnp.int32(s), jnp.int32(i)).wait()

    def sp(s, kind, slot):
        return remote(stage.at[slot, pl.ds(pl.multiple_of(o * rows, rows), rows)], sibin.at[s, kind],
                      sp_s.at[s, kind], sp_r.at[s, kind], sib)

    def own_store(s, kind, slot):
        return pltpu.make_async_copy(stage.at[slot, pl.ds(pl.multiple_of(j * rows, rows), rows)], ownp.at[s, kind],
                                     op_sem.at[slot])

    def to_mate(s, kind):
        return remote(tbuf.at[kind], mid.at[s, kind], t_s.at[s, kind], t_r.at[s, kind], mt)

    def from_mate(s, kind):
        return remote(mid.at[s, kind], mid.at[s, kind], t_s.at[s, kind], t_r.at[s, kind], mt)

    def to_part(s):
        return remote(tbuf.at[PART], branch.at[own_seq(s)], p_s.at[s], p_r.at[s], pt)

    def from_part(s):
        return remote(branch.at[other_seq(s)], branch.at[other_seq(s)], p_s.at[s], p_r.at[s], pt)

    def keep(s):
        return pltpu.make_async_copy(tbuf.at[OWN], branch.at[own_seq(s)], br_sem)

    def sent(s, kind):
        if kind < PART:
            to_mate(s, kind).wait_send()
        elif kind == PART:
            to_part(s).wait_send()
        else:
            keep(s).wait()

    def add_now(name):
        s, kind = jnp.int32(int(name[0])), BLOCKS.index(name[1])
        add_start(s, kind, jnp.int32(BEFORE_SUM[name]))
        add_finish(s, kind)

    def add_loads(s, kind):
        srcs = [ownp.at[s, kind], sibin.at[s, kind]] + ([mid.at[s, kind - PART]] if kind >= PART else [])
        return [pltpu.make_async_copy(src, cin.at[n], cl_sem.at[n]) for n, src in enumerate(srcs)]

    def add_start(s, kind, before):
        remote(sibin.at[s, kind], sibin.at[s, kind], sp_s.at[s, kind], sp_r.at[s, kind], sib).wait_recv()
        if kind >= PART:
            from_mate(s, kind - PART).wait_recv()

        @pl.when(before >= 0)
        def _():
            sent(before, kind)

        for ld in add_loads(s, kind):
            ld.start()

    def add_finish(s, kind):
        for ld in add_loads(s, kind):
            ld.wait()

        def add(r, _):
            rr = pl.ds(pl.multiple_of(r * add_rows, add_rows), add_rows)
            total = cin[0, rr, :].astype(F32) + cin[1, rr, :].astype(F32)
            if kind >= PART:
                total = total + cin[2, rr, :].astype(F32)
            tbuf[kind, rr, :] = total.astype(BF16)
            return 0

        lax.fori_loop(0, rows // add_rows, add, 0)
        if kind < PART:
            to_mate(s, kind).start()
        elif kind == PART:
            to_part(s).start()
        else:
            keep(s).start()

    def item(k):
        both = pick([4 * s + b for s, b in ITEMS], k, 4)
        return lax.div(both, 4), lax.rem(both, 4)

    def n_load(k):
        s, kind = item(k)
        return pltpu.make_async_copy(ng.at[s, rowblock(mlp_chip(kind))], nt.at[lax.rem(k, 2)], nl_sem.at[lax.rem(k, 2)])

    def o_load(k):
        s, kind = item(k)
        return pltpu.make_async_copy(obuf.at[s, rowblock(mlp_chip(kind))],
                                     ho.at[lax.rem(k, SLOTS), :, pl.ds(2 * ff, 2 * head)], ol_sem.at[lax.rem(k, SLOTS)])

    def mlp_up(k):
        with jax.named_scope("n_wait"):
            n_load(k).wait()

        @pl.when(k == 0)
        def _():
            with jax.named_scope("have_up"):
                have(UP0)
                have(UP1)
                w_own(1).wait()

        src, dst = lax.rem(k, 2), lax.rem(k, SLOTS)

        def up(t, _):
            cols = pl.ds(pl.multiple_of(t * chunk, chunk), chunk)
            hid = jnp.dot(nt[src], wu[:, cols], preferred_element_type=F32)
            ho[dst, :, cols] = (0.5 * hid * (1.0 + lax.erf(hid * 0.7071067811865476))).astype(BF16)
            return 0

        lax.fori_loop(0, 2 * ff // chunk, up, 0, unroll=True)

    def stage_free(k):
        s, kind = item(k)
        sp(s, kind, lax.rem(k, 2)).wait_send()

    def own_stored(k):
        s, kind = item(k)
        own_store(s, kind, lax.rem(k, 2)).wait()

    def mlp_down(k):
        s, kind = item(k)
        slot, src = lax.rem(k, 2), lax.rem(k, SLOTS)
        with jax.named_scope("o_wait"):
            o_load(k).wait()

        @pl.when(k == 0)
        def _():
            with jax.named_scope("have_dn"):
                for p in range(DN0, OUT + 1):
                    have(p)
                w_own(2).wait()
                w_own(3).wait()

        @pl.when(k >= 2)
        def _():
            with jax.named_scope("stage_free"):
                stage_free(k - 2)

        def down(t, _):
            cols = pl.ds(pl.multiple_of(t * chunk, chunk), chunk)
            stage[slot, :, cols] = jnp.dot(ho[src], wd[:, cols], preferred_element_type=F32).astype(BF16)
            return 0

        lax.fori_loop(0, d_model // chunk, down, 0, unroll=True)
        sp(s, kind, slot).start()
        own_store(s, kind, slot).start()

    def act(name):
        what, arg = name[:2], name[2:]
        if what == "pq":
            pass_quarter(PIECE[arg])
        elif what == "ph":
            pass_halves(PIECE[arg])
        elif what == "rm":
            relay_mate(int(arg))
        elif what == "rp":
            relay_part(int(arg[0]), int(arg[1]))
        elif what == "rf":
            relay_far(int(arg))
        elif what == "ld":
            tile_start(int(arg[0]), int(arg[1]))
        elif what == "ad":
            add_now(arg)
        elif what == "ow":
            context_out(int(arg))
        elif what == "ln":
            n_load(jnp.int32(int(arg))).start()
        else:
            o_load(jnp.int32(int(arg))).start()

    for name in START:
        with jax.named_scope(name):
            act(name)
    with jax.named_scope("have_qkv"):
        w_own(0).wait()
        for k in (W_Q, W_K, W_V):
            have(k)

    codes = [code_of(step) for step in ORDER]

    def add_code(name):
        return 1 + 4 * int(name[0]) + BLOCKS.index(name[1]) + 12 * (1 + BEFORE_SUM[name])

    adds = [add_code(ADDS[t]) if t in ADDS else 0 for t in range(len(ORDER))]

    def adding(code, do):
        @pl.when(code > 0)
        def _():
            which = lax.rem(code - 1, 12)
            for kind in range(4):
                @pl.when(lax.rem(which, 4) == kind)
                def _(kind=kind):
                    do(lax.div(which, 4), kind, lax.div(code - 1, 12) - 1)

    def events(t, lo, size):
        if not any(p in BEFORE for p in range(lo, lo + size)):
            return
        if size == 1:
            for name in BEFORE[lo]:
                with jax.named_scope(name):
                    act(name)
            return
        size //= 4
        for q in range(lo, lo + 4 * size, size):
            @pl.when(lax.div(t, size) == q // size)
            def _(q=q):
                events(t, q, size)

    def run(t, before):
        events(t, 0, 64)
        code, add = pick(codes, t, 6), pick(adds, t, 6)
        with jax.named_scope("add_start"):
            adding(add, add_start)
        what, index = lax.div(code, 16), lax.rem(code, 16)
        names = ("TILE", "ATT", "UP", "DOWN")
        for kind, body in ((TILE, tile), (ATT, attend), (UP, mlp_up), (DOWN, mlp_down)):
            @pl.when(what == kind)
            def _(kind=kind, body=body):
                with jax.named_scope(names[kind]):
                    body(index)

        with jax.named_scope("add_finish"):
            adding(add, lambda s, kind, _: add_finish(s, kind))

        @pl.when(lax.div(before, 16) == DOWN)
        def _():
            own_stored(lax.rem(before, 16))

        return code

    lax.fori_loop(0, len(ORDER), run, jnp.int32(0))
    own_stored(jnp.int32(len(ITEMS) - 1))
    with jax.named_scope("last_add"):
        for name in LAST_ADDS:
            add_now(name)
    with jax.named_scope("last_part"):
        for s in range(3):
            from_part(s).wait_recv()

    for k in range(len(ITEMS) - 2, len(ITEMS)):
        stage_free(jnp.int32(k))
    for s in range(3):
        nm(s).wait_send()
        for h in range(2):
            np_(s, h).wait_send()
            nf(s, h).wait_send()
        for i in range(6):
            nd(s, i).wait_send()
    for k in range(PIECES):
        wx(k).wait_send()
        for i in range(4):
            wf(k, i).wait_send()
    for name, s in LAST_SUM.items():
        sent(s, BLOCKS.index(name))


def residual_kernel(x, branch, y):
    y[...] = (x[...].astype(F32) + branch[...].astype(F32)).astype(BF16)


def neighbour_span(groups):
    short = 1
    while short * short * 4 <= groups:
        short *= 2
    return groups // short


def solution(mesh):
    tp, groups = mesh.shape["tp"], mesh.shape["dp"]
    span = neighbour_span(groups)
    assert tp == 8 and groups % (2 * span) == 0 and span % 2 == 0

    def local_layer(x_blk, ln_gain, ln_bias, w_qkv, w_out, w_up, w_down):
        n_seq, rows, d_model = x_blk.shape
        head = w_qkv.shape[3]
        ff = w_up.shape[1]
        ns, seq, blk = n_seq // 2, rows * tp, 2 * rows
        assert ns == 3 and w_qkv.shape[1:3] == (1, 3)
        chunk = min(512, d_model, ff)
        ln_rows, add_rows = min(64, rows // 2), min(16, rows // 2)
        dims = (span, rows, d_model, head, ff, chunk, ln_rows, add_rows)
        dma = pltpu.SemaphoreType.DMA
        anyspace = pl.BlockSpec(memory_space=pl.ANY)
        vmem = pl.BlockSpec(memory_space=pltpu.VMEM)

        def hbm(*shape):
            return jax.ShapeDtypeStruct(shape, BF16)

        outs = pl.pallas_call(
            functools.partial(layer_kernel, dims),
            name="layer",
            out_shape=(hbm(n_seq, rows, d_model), hbm(ns, seq, d_model), hbm(ns, rows, d_model), hbm(ns, seq, 2 * head),
                       hbm(ns, 4, rows, d_model), hbm(ns, 4, rows, d_model), hbm(ns, 2, rows, d_model)),
            in_specs=[anyspace, vmem, vmem, anyspace, anyspace, anyspace, anyspace],
            out_specs=(anyspace,) * 7,
            scratch_shapes=[
                pltpu.VMEM((3, d_model, 2 * head), BF16),
                pltpu.VMEM((d_model, 2 * ff), BF16),
                pltpu.VMEM((2 * ff + 2 * head, d_model), BF16),
                pltpu.VMEM((2, blk, d_model), BF16),
                pltpu.VMEM((2, blk, d_model), BF16),
                pltpu.VMEM((seq, 4 * head), BF16),
                pltpu.VMEM((2 * head, seq), BF16),
                pltpu.VMEM((2, blk, 2 * head), BF16),
                pltpu.VMEM((SLOTS, blk, 2 * ff + 2 * head), BF16),
                pltpu.VMEM((2, blk, d_model), BF16),
                pltpu.VMEM((3, rows, d_model), BF16),
                pltpu.VMEM((4, rows, d_model), BF16),
                pltpu.VMEM((2, head, blk), F32),
                pltpu.VMEM((2, 1, blk), F32),
                pltpu.VMEM((2, 1, blk), F32),
                dma((4,)), dma((PIECES,)), dma((PIECES,)), dma((PIECES, 4)), dma((PIECES, 4)),
                dma((ns,)), dma((ns,)), dma((ns, 2)), dma((ns, 2)), dma((ns, 2)), dma((ns, 2)),
                dma((ns, 6)), dma((ns, 6)),
                dma((ns, 4)), dma((ns, 4)), dma((2,)), dma((ns, 2)), dma((ns, 2)), dma((ns,)), dma((ns,)),
                dma((6,)), dma((2,)), dma((2,)), dma((2,)), dma((SLOTS,)), dma((3,)), dma,
            ],
            compiler_params=pltpu.CompilerParams(
                collective_id=0, has_side_effects=True, vmem_limit_bytes=VMEM_LIMIT),
        )(x_blk, ln_gain.reshape(1, d_model), ln_bias.reshape(1, d_model),
          jnp.transpose(w_qkv[:, 0], (1, 0, 2)), w_out, w_up, w_down)
        some = pl.BlockSpec((1, rows // 2, d_model), lambda q, h: (q, h, 0))
        return pl.pallas_call(
            residual_kernel, name="residual", grid=(n_seq, 2), in_specs=[some, some], out_specs=some,
            out_shape=hbm(n_seq, rows, d_model))(x_blk, outs[0])

    return jax.shard_map(
        local_layer, mesh=mesh,
        in_specs=(P("dp", "tp", None), P(), P(), P(None, "tp", None, None),
                  P("tp", None), P(None, "tp"), P("tp", None)),
        out_specs=P("dp", "tp", None), check_vma=False)
```

```python
import functools

import jax
import jax.numpy as jnp
from jax import lax
from jax.experimental import pallas as pl
from jax.experimental.pallas import tpu as pltpu
from jax.sharding import PartitionSpec as P

LN_EPS = 1e-5
MESH = pl.DeviceIdType.MESH
BF16 = jnp.bfloat16
F32 = jnp.float32
LOG2E = 1.4426950408889634
VMEM_LIMIT = 67_043_328

W_Q, W_K, W_V, UP0, UP1, DN0, DN1, DN2, DN3, OUT = range(10)
PIECES = 10
FAR, MATE, PART, OWN = range(4)
TILE, ATT, UP, DOWN = range(4)
INTER = ("Q2", "Q1", "Q0", "n0", "D3", "U0", "U1", "n1", "D0", "D1", "O", "D2", "n2")
ORDER = ("A00", "A01", "A02", "A03", "T00", "T01", "T02", "T03", "A10", "A11", "A12", "U0F",
         "U1M", "U0M", "A13", "T10", "T11", "T12", "U1F", "T13", "D0F", "A20", "D1M", "U0P",
         "D0M", "A21", "U1P", "A22", "D1F", "D0P", "A23", "T20", "T21", "D1P", "T22", "U2F",
         "T23", "D2F", "U2P", "U2M", "U1O", "D2P", "D2M", "D1O", "U0O", "D0O", "U2O", "D2O",
         )
START = ("pqQ2", "pqQ1", "phQ2", "pqQ0", "phQ1", "nm10", "rm0", "phQ0", "rp00")
BEFORE = {
    0: ("ld00", "ld01"),
    2: ("rp01", "pqD3", "ld02"),
    3: ("phD3", "nm11", "rf0", "pqU0", "ld03", "ln0"),
    4: ("nm20",),
    6: ("pqU1", "rm1"),
    7: ("phU0", "ld10"),
    8: ("rp10", "ld11"),
    10: ("phU1", "rp11", "ld12"),
    11: ("pqD0", "ln1", "ow0", "lo0"),
    12: ("pqD1", "nm21", "ln2"),
    13: ("phD0", "pqO", "rf1", "lo2"),
    14: ("phD1", "pqD2", "ld13", "ln3"),
    15: ("rm2",),
    17: ("phO",),
    18: ("rp20", "ln4"),
    19: ("phD2",),
    20: ("rp21", "ld20", "ow1", "lo1", "lo3"),
    22: ("ad0F",),
    23: ("rf2", "ln5", "lo4"),
    24: ("ld21",),
    26: ("ld22", "lo5"),
    29: ("ld23",),
    30: ("ln6",),
    35: ("ln7",),
    37: ("ow2", "lo6"),
    38: ("ln8", "lo7"),
    39: ("ln9", "lo8"),
    40: ("ln10", "lo9"),
    44: ("ad2M", "ln11", "lo10"),
    46: ("lo11",),
}
ADDS = { 24: "1M", 30: "1F", 31: "0P", 32: "0M", 37: "1P", 39: "2F", 44: "2P", 45: "1O", 47: "0O" }
LAST_ADDS = ("2O",)

KINDS = "ATUD"
BLOCKS = "FMPO"
ITEMS = tuple((int(x[1]), BLOCKS.index(x[2])) for x in ORDER if x[0] == "U")
SLOTS = 4
PIECE = {"Q0": W_Q, "Q1": W_K, "Q2": W_V, "U0": UP0, "U1": UP1,
         "D0": DN0, "D1": DN1, "D2": DN2, "D3": DN3, "O": OUT}


def code_of(step):
    what, s = KINDS.index(step[0]), int(step[1])
    return 16 * what + (4 * s + int(step[2]) if what < UP else ITEMS.index((s, BLOCKS.index(step[2]))))


def pick(values, i, bits):
    per = 30 // bits
    words = [sum(v << bits * p for p, v in enumerate(values[w:w + per])) for w in range(0, len(values), per)]
    word, at = lax.div(i, per), lax.rem(i, per)
    packed = jnp.int32(words[0])
    for w in range(1, len(words)):
        packed = jnp.where(word == w, words[w], packed)
    out = packed
    for p in range(1, per):
        out = jnp.where(at == p, lax.div(packed, 1 << bits * p), out)
    return lax.rem(out, 1 << bits)


def sums():
    seq = []
    for t in range(len(ORDER)):
        seq += [(name[2:], t) for name in BEFORE.get(t, ()) if name[:2] == "ad"]
        if t in ADDS:
            seq.append((ADDS[t], t))
    seq += [(name, None) for name in LAST_ADDS]
    last, before = {}, {}
    for name, _ in seq:
        before[name] = last.get(name[1], -1)
        last[name[1]] = int(name[0])
    assert len(seq) == len(ITEMS)
    return before, last


BEFORE_SUM, LAST_SUM = sums()


def layer_kernel(dims, x, gain, bias, w_qkv, w_out, w_up, w_dn,
                 branch, ng, nout, obuf, ownp, sibin, mid,
                 wq, wu, wd, xt, nt, qk, vt, ot, ho, stage, cin, tbuf, acc, m_s, l_s,
                 w_l, wx_s, wx_r, wf_s, wf_r, nm_s, nm_r, np_s, np_r, nf_s, nf_r, nd_s, nd_r,
                 sp_s, sp_r, op_sem, t_s, t_r, p_s, p_r,
                 ln_sem, xt_sem, oo_sem, nl_sem, ol_sem, cl_sem, br_sem):
    span, rows, d_model, head, ff, chunk, ln_rows, add_rows = dims
    half = rows // 2
    blk = 2 * rows
    scale = LOG2E * head ** -0.5

    g, me = lax.axis_index("dp"), lax.axis_index("tp")
    c, j = lax.div(me, 2), lax.rem(me, 2)
    o = 1 - j
    pair = lax.div(c, 2)
    mate = c + 1 - 2 * lax.rem(c, 2)
    part = 3 - c
    far = 3 - mate
    zb, yb = lax.rem(g, 2), lax.rem(lax.div(g, span), 2)
    gz, gy = g + 1 - 2 * zb, g + span * (1 - 2 * yb)

    def dev(chip, core, group=g):
        return {"dp": group, "tp": 2 * chip + core}

    sib, mt, pt, zd, yd = dev(c, o), dev(mate, j), dev(part, j), dev(c, j, gz), dev(c, j, gy)

    def remote(src, dst, send, recv, to):
        return pltpu.make_async_remote_copy(src_ref=src, dst_ref=dst, send_sem=send, recv_sem=recv,
                                            device_id=to, device_id_type=MESH)

    def row(chip, core, extra=0):
        return pl.multiple_of((2 * chip + core) * rows + extra, half)

    def rowblock(chip):
        return pl.ds(pl.multiple_of(chip * blk, blk), blk)

    quarter = 2 * yb + zb
    q_z, q_y, q_zy = quarter + 1 - 2 * zb, quarter + 2 - 4 * yb, 3 - quarter

    def w_at(piece, q, side, hold):
        n = head // 4 if piece == OUT else ff // 16 if piece >= DN0 else d_model // 8 if piece >= UP0 else d_model // 4
        size = n if side is None else n // 2
        off = q * n + (0 if side is None else side * size)
        if UP0 <= piece <= DN3:
            off = off + (piece - (UP0 if piece <= UP1 else DN0)) * 4 * n
        if hold and DN0 <= piece <= DN3:
            off = off + ff
        if hold and piece == OUT:
            off = off + 2 * ff + head
        at = pl.ds(pl.multiple_of(off, n // 2), size)
        if piece <= W_V:
            return wq.at[piece, at, pl.ds(head, head)] if hold else w_qkv.at[piece, at, :]
        if piece <= UP1:
            return wu.at[at, pl.ds(ff, ff)] if hold else w_up.at[at, :]
        return wd.at[at, :] if hold else (w_out if piece == OUT else w_dn).at[at, :]

    def w_own(i):
        src, dst = ((w_qkv, wq.at[:, :, pl.ds(0, head)]), (w_up, wu.at[:, pl.ds(0, ff)]),
                    (w_dn, wd.at[pl.ds(0, ff), :]), (w_out, wd.at[pl.ds(2 * ff, head), :]))[i]
        return pltpu.make_async_copy(src, dst, w_l.at[i])

    def wx(k):
        return remote(w_at(k, quarter, None, False), w_at(k, quarter, None, True), wx_s.at[k], wx_r.at[k], pt)

    def wx_in(k):
        ref = w_at(k, quarter, None, True)
        return remote(ref, ref, wx_s.at[k], wx_r.at[k], pt)

    def wf(k, i):
        ref = (w_at(k, quarter, None, True) if i < 2 else w_at(k, q_y, 1, True) if i == 2 else w_at(k, q_z, 0, True))
        return remote(ref, ref, wf_s.at[k, i], wf_r.at[k, i], yd if i in (1, 3) else zd)

    def wf_in(k, i):
        ref = w_at(k, (q_z, q_y, q_zy, q_zy)[i], (None, None, 1, 0)[i], True)
        return remote(ref, ref, wf_s.at[k, i], wf_r.at[k, i], yd if i in (1, 3) else zd)

    def pass_quarter(k):
        wx_in(k).wait_recv()
        wf(k, 0).start()
        wf(k, 1).start()

    def pass_halves(k):
        wf_in(k, 0).wait_recv()
        wf_in(k, 1).wait_recv()
        wf(k, 2).start()
        wf(k, 3).start()

    def have(k):
        wf_in(k, 2).wait_recv()
        wf_in(k, 3).wait_recv()

    def own_seq(s):
        return 2 * s + pair

    def other_seq(s):
        return 2 * s + 1 - pair

    def n_own(s):
        return ng.at[s, pl.ds(row(c, j), rows)]

    def nm(s, h):
        ref = ng.at[s, pl.ds(row(c, j, h * half), half)]
        return remote(ref, ref, nm_s.at[s, h], nm_r.at[s, h], mt)

    def nm_in(s, h):
        ref = ng.at[s, pl.ds(row(mate, j, h * half), half)]
        return remote(ref, ref, nm_s.at[s, h], nm_r.at[s, h], mt)

    def np_(s, h):
        return remote(nout.at[s, pl.ds(h * half, half)], ng.at[s, pl.ds(row(c, j, h * half), half)],
                      np_s.at[s, h], np_r.at[s, h], pt)

    def np_in(s, h):
        ref = ng.at[s, pl.ds(row(part, j, h * half), half)]
        return remote(ref, ref, np_s.at[s, h], np_r.at[s, h], pt)

    def nf(s, h):
        ref = ng.at[s, pl.ds(row(part, j, h * half), half)]
        return remote(ref, ref, nf_s.at[s, h], nf_r.at[s, h], mt)

    def nf_in(s, h):
        ref = ng.at[s, pl.ds(row(far, j, h * half), half)]
        return remote(ref, ref, nf_s.at[s, h], nf_r.at[s, h], mt)

    def nd(s, i, core=j):
        ref = (ng.at[s, pl.ds(row(c if i == 0 else mate, core), rows)] if i < 2 else
               ng.at[s, pl.ds(row(part if i < 4 else far, core, (i % 2) * half), half)])
        return remote(ref, ref, nd_s.at[s, i], nd_r.at[s, i], sib)

    def nd_in(s, i):
        return nd(s, i, o)

    def relay_mate(s):
        for h in range(2):
            nm_in(s, h).wait_recv()
        nd(s, 1).start()

    def relay_part(s, h):
        np_in(s, h).wait_recv()
        nf(s, h).start()
        nd(s, 2 + h).start()

    def relay_far(s):
        for h in range(2):
            nf_in(s, h).wait_recv()
            nd(s, 4 + h).start()

    def ln_buf(b):
        return (xt if b < 4 else nt).at[(b // 2) % 2, pl.ds((b % 2) * rows, rows)]

    def ln_load(b):
        return pltpu.make_async_copy(x.at[own_seq(b // 2) if b % 2 else other_seq(b // 2)], ln_buf(b), ln_sem.at[b])

    def ln_store(b):
        return pltpu.make_async_copy(ln_buf(b), n_own(b // 2) if b % 2 else nout.at[b // 2], ln_sem.at[b])

    def normalise(b):
        ln_load(b).wait()
        buf = ln_buf(b)

        def norm(r, _):
            rr = pl.ds(pl.multiple_of(r * ln_rows, ln_rows), ln_rows)
            v = buf[rr, :].astype(F32)
            mean = jnp.mean(v, axis=-1, keepdims=True)
            cen = v - mean
            var = jnp.mean(cen * cen, axis=-1, keepdims=True)
            buf[rr, :] = (cen * lax.rsqrt(var + LN_EPS) * gain[...] + bias[...]).astype(BF16)
            return 0

        lax.fori_loop(0, rows // ln_rows, norm, 0)
        ln_store(b).start()

    barrier = pltpu.get_barrier_semaphore()
    for to in (sib, mt, pt, zd, yd):
        pl.semaphore_signal(barrier, inc=1, device_id=to, device_id_type=MESH)
    for b in range(6):
        ln_load(b).start()
    with jax.named_scope("norm0"):
        normalise(0)
    with jax.named_scope("norm1"):
        normalise(1)
    with jax.named_scope("barrier"):
        pl.semaphore_wait(barrier, 5)

    def send_part(s):
        ln_store(2 * s).wait()
        np_(s, 0).start()
        np_(s, 1).start()

    for name in INTER:
        if name[0] != "n":
            wx(PIECE[name]).start()
            continue
        s = int(name[1])
        if s > 0:
            normalise(2 * s)
            normalise(2 * s + 1)
        send_part(s)
        ln_store(2 * s + 1).wait()
        if s == 0:
            nm(0, 0).start()
            nm(0, 1).start()
        nd(s, 0).start()

    def tile_chip(i):
        return jnp.where(i == 0, c, jnp.where(i == 1, mate, jnp.where(i == 2, part, far)))

    def mlp_chip(kind):
        return jnp.where(kind == FAR, far, jnp.where(kind == MATE, mate, jnp.where(kind == PART, part, c)))

    def tile_copy(s, i):
        return pltpu.make_async_copy(ng.at[s, rowblock(tile_chip(i))], xt.at[lax.rem(i, 2)], xt_sem.at[lax.rem(i, 2)])

    def tile_start(s, i):
        for n in ((0,), (1,), (2, 3), (4, 5))[i]:
            nd_in(s, n).wait_recv()
        tile_copy(s, jnp.int32(i)).start()

    def tile(index):
        s, i = lax.div(index, 4), lax.rem(index, 4)
        with jax.named_scope("tile_wait"):
            tile_copy(s, i).wait()
        slot = lax.rem(i, 2)
        base = rowblock(tile_chip(i))
        for t in range(2):
            qk[base, pl.ds(t * 2 * head, 2 * head)] = jnp.dot(
                xt[slot], wq[t], preferred_element_type=F32).astype(BF16)
        vt[:, base] = jnp.transpose(jnp.dot(xt[slot], wq[2], preferred_element_type=F32)).astype(BF16)

    def dot_t(a, b):
        return lax.dot_general(a, b, (((1,), (1,)), ((), ())), preferred_element_type=F32)

    def o_out(s, i):
        return pltpu.make_async_copy(ot.at[lax.rem(i, 2)], obuf.at[s, rowblock(i)], oo_sem.at[lax.rem(i, 2)])

    def attend(index):
        s, i = lax.div(index, 4), lax.rem(index, 4)
        slot = lax.rem(i, 2)

        @pl.when(i >= 2)
        def _():
            o_out(s, i).wait()

        mine = rowblock(i)
        causal = (lax.broadcasted_iota(jnp.int32, (blk, blk), 0)
                  <= lax.broadcasted_iota(jnp.int32, (blk, blk), 1))
        for h in range(2):
            hd = pl.ds(h * head, head)
            sc = jnp.where(causal, dot_t(qk[mine, pl.ds((2 + h) * head, head)], qk[mine, hd]), -jnp.inf)
            top = jnp.max(sc, axis=0, keepdims=True)
            p = jnp.exp2((sc - top) * scale)
            m_s[h] = top
            l_s[h] = jnp.sum(p, axis=0, keepdims=True)
            acc[h] = jnp.dot(vt[hd, mine], p.astype(BF16), preferred_element_type=F32)

        def earlier(t, _):
            there = rowblock(t)
            for h in range(2):
                hd = pl.ds(h * head, head)
                sc = dot_t(qk[there, pl.ds((2 + h) * head, head)], qk[mine, hd])
                old = m_s[h]
                top = jnp.maximum(old, jnp.max(sc, axis=0, keepdims=True))
                p = jnp.exp2((sc - top) * scale)
                fade = jnp.exp2((old - top) * scale)
                m_s[h] = top
                l_s[h] = l_s[h] * fade + jnp.sum(p, axis=0, keepdims=True)
                acc[h] = acc[h] * fade + jnp.dot(vt[hd, there], p.astype(BF16), preferred_element_type=F32)
            return 0

        lax.fori_loop(0, i, earlier, 0)
        for h in range(2):
            ot[slot, :, pl.ds(h * head, head)] = jnp.transpose(acc[h] * (1.0 / l_s[h])).astype(BF16)
        o_out(s, i).start()

    def context_out(s):
        for i in (2, 3):
            o_out(jnp.int32(s), jnp.int32(i)).wait()

    def sp(s, kind, slot):
        return remote(stage.at[slot, pl.ds(pl.multiple_of(o * rows, rows), rows)], sibin.at[s, kind],
                      sp_s.at[s, kind], sp_r.at[s, kind], sib)

    def own_store(s, kind, slot):
        return pltpu.make_async_copy(stage.at[slot, pl.ds(pl.multiple_of(j * rows, rows), rows)], ownp.at[s, kind],
                                     op_sem.at[slot])

    def to_mate(s, kind):
        return remote(tbuf.at[kind], mid.at[s, kind], t_s.at[s, kind], t_r.at[s, kind], mt)

    def from_mate(s, kind):
        return remote(mid.at[s, kind], mid.at[s, kind], t_s.at[s, kind], t_r.at[s, kind], mt)

    def to_part(s):
        return remote(tbuf.at[PART], branch.at[own_seq(s)], p_s.at[s], p_r.at[s], pt)

    def from_part(s):
        return remote(branch.at[other_seq(s)], branch.at[other_seq(s)], p_s.at[s], p_r.at[s], pt)

    def keep(s):
        return pltpu.make_async_copy(tbuf.at[OWN], branch.at[own_seq(s)], br_sem)

    def sent(s, kind):
        if kind < PART:
            to_mate(s, kind).wait_send()
        elif kind == PART:
            to_part(s).wait_send()
        else:
            keep(s).wait()

    def add_now(name):
        s, kind = jnp.int32(int(name[0])), BLOCKS.index(name[1])
        add_start(s, kind, jnp.int32(BEFORE_SUM[name]))
        add_finish(s, kind)

    def add_loads(s, kind):
        srcs = [ownp.at[s, kind], sibin.at[s, kind]] + ([mid.at[s, kind - PART]] if kind >= PART else [])
        return [pltpu.make_async_copy(src, cin.at[n], cl_sem.at[n]) for n, src in enumerate(srcs)]

    def add_start(s, kind, before):
        remote(sibin.at[s, kind], sibin.at[s, kind], sp_s.at[s, kind], sp_r.at[s, kind], sib).wait_recv()
        if kind >= PART:
            from_mate(s, kind - PART).wait_recv()

        @pl.when(before >= 0)
        def _():
            sent(before, kind)

        for ld in add_loads(s, kind):
            ld.start()

    def add_finish(s, kind):
        for ld in add_loads(s, kind):
            ld.wait()

        def add(r, _):
            rr = pl.ds(pl.multiple_of(r * add_rows, add_rows), add_rows)
            total = cin[0, rr, :].astype(F32) + cin[1, rr, :].astype(F32)
            if kind >= PART:
                total = total + cin[2, rr, :].astype(F32)
            tbuf[kind, rr, :] = total.astype(BF16)
            return 0

        lax.fori_loop(0, rows // add_rows, add, 0)
        if kind < PART:
            to_mate(s, kind).start()
        elif kind == PART:
            to_part(s).start()
        else:
            keep(s).start()

    def item(k):
        both = pick([4 * s + b for s, b in ITEMS], k, 4)
        return lax.div(both, 4), lax.rem(both, 4)

    def n_load(k):
        s, kind = item(k)
        return pltpu.make_async_copy(ng.at[s, rowblock(mlp_chip(kind))], nt.at[lax.rem(k, 2)], nl_sem.at[lax.rem(k, 2)])

    def o_load(k):
        s, kind = item(k)
        return pltpu.make_async_copy(obuf.at[s, rowblock(mlp_chip(kind))],
                                     ho.at[lax.rem(k, SLOTS), :, pl.ds(2 * ff, 2 * head)], ol_sem.at[lax.rem(k, SLOTS)])

    def mlp_up(k):
        with jax.named_scope("n_wait"):
            n_load(k).wait()

        @pl.when(k == 0)
        def _():
            with jax.named_scope("have_up"):
                have(UP0)
                have(UP1)
                w_own(1).wait()

        src, dst = lax.rem(k, 2), lax.rem(k, SLOTS)

        def up(t, _):
            cols = pl.ds(pl.multiple_of(t * chunk, chunk), chunk)
            hid = jnp.dot(nt[src], wu[:, cols], preferred_element_type=F32)
            ho[dst, :, cols] = (0.5 * hid * (1.0 + lax.erf(hid * 0.7071067811865476))).astype(BF16)
            return 0

        lax.fori_loop(0, 2 * ff // chunk, up, 0, unroll=True)

    def stage_free(k):
        s, kind = item(k)
        sp(s, kind, lax.rem(k, 2)).wait_send()

    def own_stored(k):
        s, kind = item(k)
        own_store(s, kind, lax.rem(k, 2)).wait()

    def mlp_down(k):
        s, kind = item(k)
        slot, src = lax.rem(k, 2), lax.rem(k, SLOTS)
        with jax.named_scope("o_wait"):
            o_load(k).wait()

        @pl.when(k == 0)
        def _():
            with jax.named_scope("have_dn"):
                for p in range(DN0, OUT + 1):
                    have(p)
                w_own(2).wait()
                w_own(3).wait()

        @pl.when(k >= 2)
        def _():
            with jax.named_scope("stage_free"):
                stage_free(k - 2)

        def down(t, _):
            cols = pl.ds(pl.multiple_of(t * chunk, chunk), chunk)
            stage[slot, :, cols] = jnp.dot(ho[src], wd[:, cols], preferred_element_type=F32).astype(BF16)
            return 0

        lax.fori_loop(0, d_model // chunk, down, 0, unroll=True)
        sp(s, kind, slot).start()
        own_store(s, kind, slot).start()

    def act(name):
        what, arg = name[:2], name[2:]
        if what == "pq":
            pass_quarter(PIECE[arg])
        elif what == "ph":
            pass_halves(PIECE[arg])
        elif what == "rm":
            relay_mate(int(arg))
        elif what == "rp":
            relay_part(int(arg[0]), int(arg[1]))
        elif what == "rf":
            relay_far(int(arg))
        elif what == "ld":
            tile_start(int(arg[0]), int(arg[1]))
        elif what == "nm":
            nm(int(arg[0]), int(arg[1])).start()
        elif what == "ad":
            add_now(arg)
        elif what == "ow":
            context_out(int(arg))
        elif what == "ln":
            n_load(jnp.int32(int(arg))).start()
        else:
            o_load(jnp.int32(int(arg))).start()

    for i in range(4):
        w_own(i).start()
    for name in START:
        with jax.named_scope(name):
            act(name)
    with jax.named_scope("have_qkv"):
        w_own(0).wait()
        for k in (W_Q, W_K, W_V):
            have(k)

    codes = [code_of(step) for step in ORDER]

    def add_code(name):
        return 1 + 4 * int(name[0]) + BLOCKS.index(name[1]) + 12 * (1 + BEFORE_SUM[name])

    adds = [add_code(ADDS[t]) if t in ADDS else 0 for t in range(len(ORDER))]

    def adding(code, do):
        @pl.when(code > 0)
        def _():
            which = lax.rem(code - 1, 12)
            for kind in range(4):
                @pl.when(lax.rem(which, 4) == kind)
                def _(kind=kind):
                    do(lax.div(which, 4), kind, lax.div(code - 1, 12) - 1)

    def events(t, lo, size):
        if not any(p in BEFORE for p in range(lo, lo + size)):
            return
        if size == 1:
            for name in BEFORE[lo]:
                with jax.named_scope(name):
                    act(name)
            return
        size //= 4
        for q in range(lo, lo + 4 * size, size):
            @pl.when(lax.div(t, size) == q // size)
            def _(q=q):
                events(t, q, size)

    def run(t, before):
        events(t, 0, 64)
        code, add = pick(codes, t, 6), pick(adds, t, 6)
        with jax.named_scope("add_start"):
            adding(add, add_start)
        what, index = lax.div(code, 16), lax.rem(code, 16)
        names = ("TILE", "ATT", "UP", "DOWN")
        for kind, body in ((TILE, tile), (ATT, attend), (UP, mlp_up), (DOWN, mlp_down)):
            @pl.when(what == kind)
            def _(kind=kind, body=body):
                with jax.named_scope(names[kind]):
                    body(index)

        with jax.named_scope("add_finish"):
            adding(add, lambda s, kind, _: add_finish(s, kind))

        @pl.when(lax.div(before, 16) == DOWN)
        def _():
            own_stored(lax.rem(before, 16))

        return code

    lax.fori_loop(0, len(ORDER), run, jnp.int32(0))
    own_stored(jnp.int32(len(ITEMS) - 1))
    with jax.named_scope("last_add"):
        for name in LAST_ADDS:
            add_now(name)
    with jax.named_scope("last_part"):
        for s in range(3):
            from_part(s).wait_recv()

    for k in range(len(ITEMS) - 2, len(ITEMS)):
        stage_free(jnp.int32(k))
    for s in range(3):
        for h in range(2):
            nm(s, h).wait_send()
            np_(s, h).wait_send()
            nf(s, h).wait_send()
        for i in range(6):
            nd(s, i).wait_send()
    for k in range(PIECES):
        wx(k).wait_send()
        for i in range(4):
            wf(k, i).wait_send()
    for name, s in LAST_SUM.items():
        sent(s, BLOCKS.index(name))


def residual_kernel(x, branch, y, xv, bv, x_sem, b_sem, y_sem):
    parts, step = xv.shape[0], min(64, xv.shape[1])

    def loads(p):
        return (pltpu.make_async_copy(x.at[p], xv.at[p], x_sem.at[p]),
                pltpu.make_async_copy(branch.at[p], bv.at[p], b_sem.at[p]))

    def store(p):
        return pltpu.make_async_copy(xv.at[p], y.at[p], y_sem.at[p])

    for p in range(parts):
        for ld in loads(p):
            ld.start()

    def add(p, _):
        for ld in loads(p):
            ld.wait()
        for r in range(0, xv.shape[1], step):
            rr = pl.ds(r, step)
            xv[p, rr, :] = (xv[p, rr, :].astype(F32) + bv[p, rr, :].astype(F32)).astype(BF16)
        store(p).start()
        return 0

    lax.fori_loop(0, parts, add, 0)
    for p in range(parts):
        store(p).wait()


def neighbour_span(groups):
    short = 1
    while short * short * 4 <= groups:
        short *= 2
    return groups // short


def solution(mesh):
    tp, groups = mesh.shape["tp"], mesh.shape["dp"]
    span = neighbour_span(groups)
    assert tp == 8 and groups % (2 * span) == 0 and span % 2 == 0

    def local_layer(x_blk, ln_gain, ln_bias, w_qkv, w_out, w_up, w_down):
        n_seq, rows, d_model = x_blk.shape
        head = w_qkv.shape[3]
        ff = w_up.shape[1]
        ns, seq, blk = n_seq // 2, rows * tp, 2 * rows
        assert ns == 3 and w_qkv.shape[1:3] == (1, 3)
        chunk = min(512, d_model, ff)
        ln_rows, add_rows = min(64, rows // 2), min(16, rows // 2)
        dims = (span, rows, d_model, head, ff, chunk, ln_rows, add_rows)
        dma = pltpu.SemaphoreType.DMA
        anyspace = pl.BlockSpec(memory_space=pl.ANY)
        vmem = pl.BlockSpec(memory_space=pltpu.VMEM)

        def hbm(*shape):
            return jax.ShapeDtypeStruct(shape, BF16)

        outs = pl.pallas_call(
            functools.partial(layer_kernel, dims),
            name="layer",
            out_shape=(hbm(n_seq, rows, d_model), hbm(ns, seq, d_model), hbm(ns, rows, d_model), hbm(ns, seq, 2 * head),
                       hbm(ns, 4, rows, d_model), hbm(ns, 4, rows, d_model), hbm(ns, 2, rows, d_model)),
            in_specs=[anyspace, vmem, vmem, anyspace, anyspace, anyspace, anyspace],
            out_specs=(anyspace,) * 7,
            scratch_shapes=[
                pltpu.VMEM((3, d_model, 2 * head), BF16),
                pltpu.VMEM((d_model, 2 * ff), BF16),
                pltpu.VMEM((2 * ff + 2 * head, d_model), BF16),
                pltpu.VMEM((2, blk, d_model), BF16),
                pltpu.VMEM((2, blk, d_model), BF16),
                pltpu.VMEM((seq, 4 * head), BF16),
                pltpu.VMEM((2 * head, seq), BF16),
                pltpu.VMEM((2, blk, 2 * head), BF16),
                pltpu.VMEM((SLOTS, blk, 2 * ff + 2 * head), BF16),
                pltpu.VMEM((2, blk, d_model), BF16),
                pltpu.VMEM((3, rows, d_model), BF16),
                pltpu.VMEM((4, rows, d_model), BF16),
                pltpu.VMEM((2, head, blk), F32),
                pltpu.VMEM((2, 1, blk), F32),
                pltpu.VMEM((2, 1, blk), F32),
                dma((4,)), dma((PIECES,)), dma((PIECES,)), dma((PIECES, 4)), dma((PIECES, 4)),
                dma((ns, 2)), dma((ns, 2)), dma((ns, 2)), dma((ns, 2)), dma((ns, 2)), dma((ns, 2)),
                dma((ns, 6)), dma((ns, 6)),
                dma((ns, 4)), dma((ns, 4)), dma((2,)), dma((ns, 2)), dma((ns, 2)), dma((ns,)), dma((ns,)),
                dma((6,)), dma((2,)), dma((2,)), dma((2,)), dma((SLOTS,)), dma((3,)), dma,
            ],
            compiler_params=pltpu.CompilerParams(
                collective_id=0, has_side_effects=True, vmem_limit_bytes=VMEM_LIMIT),
        )(x_blk, ln_gain.reshape(1, d_model), ln_bias.reshape(1, d_model),
          jnp.transpose(w_qkv[:, 0], (1, 0, 2)), w_out, w_up, w_down)
        cut = (4 * n_seq, rows // 4, d_model)
        y = pl.pallas_call(
            residual_kernel, name="residual", in_specs=[anyspace, anyspace], out_specs=anyspace,
            out_shape=hbm(*cut),
            scratch_shapes=[pltpu.VMEM(cut, BF16), pltpu.VMEM(cut, BF16), dma(cut[:1]), dma(cut[:1]), dma(cut[:1])],
            compiler_params=pltpu.CompilerParams(vmem_limit_bytes=VMEM_LIMIT),
        )(x_blk.reshape(cut), outs[0].reshape(cut))
        return y.reshape(n_seq, rows, d_model)

    return jax.shard_map(
        local_layer, mesh=mesh,
        in_specs=(P("dp", "tp", None), P(), P(), P(None, "tp", None, None),
                  P("tp", None), P(None, "tp"), P("tp", None)),
        out_specs=P("dp", "tp", None), check_vma=False)
```

```python
import functools

import jax
import jax.numpy as jnp
from jax import lax
from jax.experimental import pallas as pl
from jax.experimental.pallas import tpu as pltpu
from jax.sharding import PartitionSpec as P

LN_EPS = 1e-5
MESH = pl.DeviceIdType.MESH
BF16 = jnp.bfloat16
F32 = jnp.float32
LOG2E = 1.4426950408889634
VMEM_LIMIT = 67_043_328

W_Q, W_K, W_V, UP0, UP1, DN0, DN1, DN2, DN3, OUT = range(10)
PIECES = 10
FAR, MATE, PART, OWN = range(4)
TILE, ATT, UP, DOWN = range(4)
INTER = ("Q2", "Q1", "Q0", "p01", "p00", "U1", "U0", "D2", "p10", "p11", "D1", "D0", "D3", "O", "p21", "p20")
ORDER = ("A00", "A01", "A02", "A03", "T00", "T01", "T02", "T03", "A10", "A11", "U0F", "U0M",
         "U0P", "A12", "A13", "T10", "T11", "T12", "T13", "A20", "D0F", "A21", "D0M", "U1F",
         "A22", "D0P", "A23", "D1F", "U1M", "T20", "U2F", "T21", "D1M", "T22", "T23", "D2F",
         "U1P", "D1P", "U2M", "D2M", "U2P", "D2P", "U0O", "D0O", "U1O", "D1O", "U2O", "D2O",
         )
START = ("pqQ2", "pqQ1", "phQ2", "pqQ0", "phQ1", "rm0", "nm10", "phQ0", "rp01")
BEFORE = {
    0: ("ld00", "ld01"),
    2: ("rp00", "ld02"),
    3: ("pqU1", "rf0", "nm11", "pqU0", "ld03", "ln0"),
    4: ("phU1", "pqD2"),
    5: ("nm20",),
    6: ("rm1",),
    7: ("phU0", "ld10"),
    8: ("rp10", "ld11"),
    9: ("phD2",),
    10: ("rp11", "ln1", "ow0", "lo0"),
    11: ("pqD1", "ln2", "lo1"),
    12: ("pqD0", "ld12", "lo2"),
    13: ("phD1", "pqD3", "rf1", "nm21"),
    14: ("ld13", "ln3"),
    15: ("phD0", "pqO"),
    18: ("phD3", "rm2", "rp21", "ld20"),
    19: ("phO",),
    20: ("rp20", "ld21"),
    22: ("ad0F",),
    23: ("rf2", "ld22", "ln4", "ow1", "lo3"),
    25: ("ld23",),
    28: ("ln5", "lo4"),
    30: ("ln6",),
    35: ("ow2", "lo5"),
    36: ("ln7", "lo6"),
    38: ("ln8", "lo7"),
    40: ("ln9", "lo8"),
    42: ("ln10", "lo9"),
    44: ("ad2P", "ln11", "lo10"),
    46: ("lo11",),
}
ADDS = { 24: "0M", 27: "0P", 29: "1F", 34: "1M", 37: "2F", 39: "1P", 41: "2M", 45: "0O", 47: "1O" }
LAST_ADDS = ("2O",)

KINDS = "ATUD"
BLOCKS = "FMPO"
ITEMS = tuple((int(x[1]), BLOCKS.index(x[2])) for x in ORDER if x[0] == "U")
SLOTS = 4
PIECE = {"Q0": W_Q, "Q1": W_K, "Q2": W_V, "U0": UP0, "U1": UP1,
         "D0": DN0, "D1": DN1, "D2": DN2, "D3": DN3, "O": OUT}


def code_of(step):
    what, s = KINDS.index(step[0]), int(step[1])
    return 16 * what + (4 * s + int(step[2]) if what < UP else ITEMS.index((s, BLOCKS.index(step[2]))))


def pick(values, i, bits):
    per = 30 // bits
    words = [sum(v << bits * p for p, v in enumerate(values[w:w + per])) for w in range(0, len(values), per)]
    word, at = lax.div(i, per), lax.rem(i, per)
    packed = jnp.int32(words[0])
    for w in range(1, len(words)):
        packed = jnp.where(word == w, words[w], packed)
    out = packed
    for p in range(1, per):
        out = jnp.where(at == p, lax.div(packed, 1 << bits * p), out)
    return lax.rem(out, 1 << bits)


def sums():
    seq = []
    for t in range(len(ORDER)):
        seq += [(name[2:], t) for name in BEFORE.get(t, ()) if name[:2] == "ad"]
        if t in ADDS:
            seq.append((ADDS[t], t))
    seq += [(name, None) for name in LAST_ADDS]
    last, before = {}, {}
    for name, _ in seq:
        before[name] = last.get(name[1], -1)
        last[name[1]] = int(name[0])
    assert len(seq) == len(ITEMS)
    return before, last


BEFORE_SUM, LAST_SUM = sums()


def layer_kernel(dims, x, gain, bias, w_qkv, w_out, w_up, w_dn,
                 branch, ng, nout, obuf, ownp, sibin, mid,
                 wq, wu, wd, xt, nt, qk, vt, ot, ho, stage, cin, tbuf, acc, m_s, l_s,
                 w_l, wx_s, wx_r, wf_s, wf_r, nm_s, nm_r, np_s, np_r, nf_s, nf_r, nd_s, nd_r,
                 sp_s, sp_r, op_sem, t_s, t_r, p_s, p_r,
                 ln_sem, xt_sem, oo_sem, nl_sem, ol_sem, cl_sem, br_sem):
    span, rows, d_model, head, ff, chunk, ln_rows, add_rows = dims
    half = rows // 2
    blk = 2 * rows
    scale = LOG2E * head ** -0.5

    g, me = lax.axis_index("dp"), lax.axis_index("tp")
    c, j = lax.div(me, 2), lax.rem(me, 2)
    o = 1 - j
    pair = lax.div(c, 2)
    mate = c + 1 - 2 * lax.rem(c, 2)
    part = 3 - c
    far = 3 - mate
    zb, yb = lax.rem(g, 2), lax.rem(lax.div(g, span), 2)
    gz, gy = g + 1 - 2 * zb, g + span * (1 - 2 * yb)

    def dev(chip, core, group=g):
        return {"dp": group, "tp": 2 * chip + core}

    sib, mt, pt, zd, yd = dev(c, o), dev(mate, j), dev(part, j), dev(c, j, gz), dev(c, j, gy)

    def remote(src, dst, send, recv, to):
        return pltpu.make_async_remote_copy(src_ref=src, dst_ref=dst, send_sem=send, recv_sem=recv,
                                            device_id=to, device_id_type=MESH)

    def row(chip, core, extra=0):
        return pl.multiple_of((2 * chip + core) * rows + extra, half)

    def rowblock(chip):
        return pl.ds(pl.multiple_of(chip * blk, blk), blk)

    quarter = 2 * yb + zb
    q_z, q_y, q_zy = quarter + 1 - 2 * zb, quarter + 2 - 4 * yb, 3 - quarter

    def w_at(piece, q, side, hold):
        n = head // 4 if piece == OUT else ff // 16 if piece >= DN0 else d_model // 8 if piece >= UP0 else d_model // 4
        size = n if side is None else n // 2
        off = q * n + (0 if side is None else side * size)
        if UP0 <= piece <= DN3:
            off = off + (piece - (UP0 if piece <= UP1 else DN0)) * 4 * n
        if hold and DN0 <= piece <= DN3:
            off = off + ff
        if hold and piece == OUT:
            off = off + 2 * ff + head
        at = pl.ds(pl.multiple_of(off, n // 2), size)
        if piece <= W_V:
            return wq.at[piece, at, pl.ds(head, head)] if hold else w_qkv.at[piece, at, :]
        if piece <= UP1:
            return wu.at[at, pl.ds(ff, ff)] if hold else w_up.at[at, :]
        return wd.at[at, :] if hold else (w_out if piece == OUT else w_dn).at[at, :]

    def w_own(i):
        src, dst = ((w_qkv, wq.at[:, :, pl.ds(0, head)]), (w_up, wu.at[:, pl.ds(0, ff)]),
                    (w_dn, wd.at[pl.ds(0, ff), :]), (w_out, wd.at[pl.ds(2 * ff, head), :]))[i]
        return pltpu.make_async_copy(src, dst, w_l.at[i])

    def wx(k):
        return remote(w_at(k, quarter, None, False), w_at(k, quarter, None, True), wx_s.at[k], wx_r.at[k], pt)

    def wx_in(k):
        ref = w_at(k, quarter, None, True)
        return remote(ref, ref, wx_s.at[k], wx_r.at[k], pt)

    def wf(k, i):
        ref = (w_at(k, quarter, None, True) if i < 2 else w_at(k, q_y, 1, True) if i == 2 else w_at(k, q_z, 0, True))
        return remote(ref, ref, wf_s.at[k, i], wf_r.at[k, i], yd if i in (1, 3) else zd)

    def wf_in(k, i):
        ref = w_at(k, (q_z, q_y, q_zy, q_zy)[i], (None, None, 1, 0)[i], True)
        return remote(ref, ref, wf_s.at[k, i], wf_r.at[k, i], yd if i in (1, 3) else zd)

    def pass_quarter(k):
        wx_in(k).wait_recv()
        wf(k, 0).start()
        wf(k, 1).start()

    def pass_halves(k):
        wf_in(k, 0).wait_recv()
        wf_in(k, 1).wait_recv()
        wf(k, 2).start()
        wf(k, 3).start()

    def have(k):
        wf_in(k, 2).wait_recv()
        wf_in(k, 3).wait_recv()

    def own_seq(s):
        return 2 * s + pair

    def other_seq(s):
        return 2 * s + 1 - pair

    def n_own(s):
        return ng.at[s, pl.ds(row(c, j), rows)]

    def nm(s, h):
        ref = ng.at[s, pl.ds(row(c, j, h * half), half)]
        return remote(ref, ref, nm_s.at[s, h], nm_r.at[s, h], mt)

    def nm_in(s, h):
        ref = ng.at[s, pl.ds(row(mate, j, h * half), half)]
        return remote(ref, ref, nm_s.at[s, h], nm_r.at[s, h], mt)

    def np_(s, h):
        return remote(nout.at[s, pl.ds(h * half, half)], ng.at[s, pl.ds(row(c, j, h * half), half)],
                      np_s.at[s, h], np_r.at[s, h], pt)

    def np_in(s, h):
        ref = ng.at[s, pl.ds(row(part, j, h * half), half)]
        return remote(ref, ref, np_s.at[s, h], np_r.at[s, h], pt)

    def nf(s, h):
        ref = ng.at[s, pl.ds(row(part, j, h * half), half)]
        return remote(ref, ref, nf_s.at[s, h], nf_r.at[s, h], mt)

    def nf_in(s, h):
        ref = ng.at[s, pl.ds(row(far, j, h * half), half)]
        return remote(ref, ref, nf_s.at[s, h], nf_r.at[s, h], mt)

    def nd(s, i, core=j):
        ref = (ng.at[s, pl.ds(row(c if i == 0 else mate, core), rows)] if i < 2 else
               ng.at[s, pl.ds(row(part if i < 4 else far, core, (i % 2) * half), half)])
        return remote(ref, ref, nd_s.at[s, i], nd_r.at[s, i], sib)

    def nd_in(s, i):
        return nd(s, i, o)

    def relay_mate(s):
        for h in range(2):
            nm_in(s, h).wait_recv()
        nd(s, 1).start()

    def relay_part(s, h):
        np_in(s, h).wait_recv()
        nf(s, h).start()
        nd(s, 2 + h).start()

    def relay_far(s):
        for h in range(2):
            nf_in(s, h).wait_recv()
            nd(s, 4 + h).start()

    def ln_buf(b):
        return (xt if b < 4 else nt).at[(b // 2) % 2, pl.ds((b % 2) * rows, rows)]

    def ln_load(b):
        return pltpu.make_async_copy(x.at[own_seq(b // 2) if b % 2 else other_seq(b // 2)], ln_buf(b), ln_sem.at[b])

    def ln_store(b):
        return pltpu.make_async_copy(ln_buf(b), n_own(b // 2) if b % 2 else nout.at[b // 2], ln_sem.at[b])

    def normalise(b):
        ln_load(b).wait()
        buf = ln_buf(b)

        def norm(r, _):
            rr = pl.ds(pl.multiple_of(r * ln_rows, ln_rows), ln_rows)
            v = buf[rr, :].astype(F32)
            mean = jnp.mean(v, axis=-1, keepdims=True)
            cen = v - mean
            var = jnp.mean(cen * cen, axis=-1, keepdims=True)
            buf[rr, :] = (cen * lax.rsqrt(var + LN_EPS) * gain[...] + bias[...]).astype(BF16)
            return 0

        lax.fori_loop(0, rows // ln_rows, norm, 0)
        ln_store(b).start()

    barrier = pltpu.get_barrier_semaphore()
    for to in (sib, mt, pt, zd, yd):
        pl.semaphore_signal(barrier, inc=1, device_id=to, device_id_type=MESH)
    for b in range(6):
        ln_load(b).start()
    with jax.named_scope("barrier"):
        pl.semaphore_wait(barrier, 5)

    def prepare(s):
        normalise(2 * s)
        ln_store(2 * s).wait()
        yield
        normalise(2 * s + 1)
        ln_store(2 * s + 1).wait()
        if s == 0:
            nm(0, 0).start()
            nm(0, 1).start()
        nd(s, 0).start()
        yield

    ready = {}
    for name in INTER:
        if name[0] != "p":
            wx(PIECE[name]).start()
            continue
        s, h = int(name[1]), int(name[2])
        if s not in ready:
            ready[s] = prepare(s)
            next(ready[s])
            np_(s, h).start()
        else:
            np_(s, h).start()
            next(ready[s])

    def tile_chip(i):
        return jnp.where(i == 0, c, jnp.where(i == 1, mate, jnp.where(i == 2, part, far)))

    def mlp_chip(kind):
        return jnp.where(kind == FAR, far, jnp.where(kind == MATE, mate, jnp.where(kind == PART, part, c)))

    def tile_copy(s, i):
        return pltpu.make_async_copy(ng.at[s, rowblock(tile_chip(i))], xt.at[lax.rem(i, 2)], xt_sem.at[lax.rem(i, 2)])

    def tile_start(s, i):
        for n in ((0,), (1,), (2, 3), (4, 5))[i]:
            nd_in(s, n).wait_recv()
        tile_copy(s, jnp.int32(i)).start()

    def tile(index):
        s, i = lax.div(index, 4), lax.rem(index, 4)
        with jax.named_scope("tile_wait"):
            tile_copy(s, i).wait()
        slot = lax.rem(i, 2)
        base = rowblock(tile_chip(i))
        for t in range(2):
            qk[base, pl.ds(t * 2 * head, 2 * head)] = jnp.dot(
                xt[slot], wq[t], preferred_element_type=F32).astype(BF16)
        vt[:, base] = jnp.transpose(jnp.dot(xt[slot], wq[2], preferred_element_type=F32)).astype(BF16)

    def dot_t(a, b):
        return lax.dot_general(a, b, (((1,), (1,)), ((), ())), preferred_element_type=F32)

    def o_out(s, i):
        return pltpu.make_async_copy(ot.at[lax.rem(i, 2)], obuf.at[s, rowblock(i)], oo_sem.at[lax.rem(i, 2)])

    def attend(index):
        s, i = lax.div(index, 4), lax.rem(index, 4)
        slot = lax.rem(i, 2)

        @pl.when(i >= 2)
        def _():
            o_out(s, i).wait()

        mine = rowblock(i)
        causal = (lax.broadcasted_iota(jnp.int32, (blk, blk), 0)
                  <= lax.broadcasted_iota(jnp.int32, (blk, blk), 1))
        for h in range(2):
            hd = pl.ds(h * head, head)
            sc = jnp.where(causal, dot_t(qk[mine, pl.ds((2 + h) * head, head)], qk[mine, hd]), -jnp.inf)
            top = jnp.max(sc, axis=0, keepdims=True)
            p = jnp.exp2((sc - top) * scale)
            m_s[h] = top
            l_s[h] = jnp.sum(p, axis=0, keepdims=True)
            acc[h] = jnp.dot(vt[hd, mine], p.astype(BF16), preferred_element_type=F32)

        def earlier(t, _):
            there = rowblock(t)
            for h in range(2):
                hd = pl.ds(h * head, head)
                sc = dot_t(qk[there, pl.ds((2 + h) * head, head)], qk[mine, hd])
                old = m_s[h]
                top = jnp.maximum(old, jnp.max(sc, axis=0, keepdims=True))
                p = jnp.exp2((sc - top) * scale)
                fade = jnp.exp2((old - top) * scale)
                m_s[h] = top
                l_s[h] = l_s[h] * fade + jnp.sum(p, axis=0, keepdims=True)
                acc[h] = acc[h] * fade + jnp.dot(vt[hd, there], p.astype(BF16), preferred_element_type=F32)
            return 0

        lax.fori_loop(0, i, earlier, 0)
        for h in range(2):
            ot[slot, :, pl.ds(h * head, head)] = jnp.transpose(acc[h] * (1.0 / l_s[h])).astype(BF16)
        o_out(s, i).start()

    def context_out(s):
        for i in (2, 3):
            o_out(jnp.int32(s), jnp.int32(i)).wait()

    def sp(s, kind, slot):
        return remote(stage.at[slot, pl.ds(pl.multiple_of(o * rows, rows), rows)], sibin.at[s, kind],
                      sp_s.at[s, kind], sp_r.at[s, kind], sib)

    def own_store(s, kind, slot):
        return pltpu.make_async_copy(stage.at[slot, pl.ds(pl.multiple_of(j * rows, rows), rows)], ownp.at[s, kind],
                                     op_sem.at[slot])

    def to_mate(s, kind):
        return remote(tbuf.at[kind], mid.at[s, kind], t_s.at[s, kind], t_r.at[s, kind], mt)

    def from_mate(s, kind):
        return remote(mid.at[s, kind], mid.at[s, kind], t_s.at[s, kind], t_r.at[s, kind], mt)

    def to_part(s):
        return remote(tbuf.at[PART], branch.at[own_seq(s)], p_s.at[s], p_r.at[s], pt)

    def from_part(s):
        return remote(branch.at[other_seq(s)], branch.at[other_seq(s)], p_s.at[s], p_r.at[s], pt)

    def keep(s):
        return pltpu.make_async_copy(tbuf.at[OWN], branch.at[own_seq(s)], br_sem)

    def sent(s, kind):
        if kind < PART:
            to_mate(s, kind).wait_send()
        elif kind == PART:
            to_part(s).wait_send()
        else:
            keep(s).wait()

    def add_now(name):
        s, kind = jnp.int32(int(name[0])), BLOCKS.index(name[1])
        add_start(s, kind, jnp.int32(BEFORE_SUM[name]))
        add_finish(s, kind)

    def add_loads(s, kind):
        srcs = [ownp.at[s, kind], sibin.at[s, kind]] + ([mid.at[s, kind - PART]] if kind >= PART else [])
        return [pltpu.make_async_copy(src, cin.at[n], cl_sem.at[n]) for n, src in enumerate(srcs)]

    def add_start(s, kind, before):
        remote(sibin.at[s, kind], sibin.at[s, kind], sp_s.at[s, kind], sp_r.at[s, kind], sib).wait_recv()
        if kind >= PART:
            from_mate(s, kind - PART).wait_recv()

        @pl.when(before >= 0)
        def _():
            sent(before, kind)

        for ld in add_loads(s, kind):
            ld.start()

    def add_finish(s, kind):
        for ld in add_loads(s, kind):
            ld.wait()

        def add(r, _):
            rr = pl.ds(pl.multiple_of(r * add_rows, add_rows), add_rows)
            total = cin[0, rr, :].astype(F32) + cin[1, rr, :].astype(F32)
            if kind >= PART:
                total = total + cin[2, rr, :].astype(F32)
            tbuf[kind, rr, :] = total.astype(BF16)
            return 0

        lax.fori_loop(0, rows // add_rows, add, 0)
        if kind < PART:
            to_mate(s, kind).start()
        elif kind == PART:
            to_part(s).start()
        else:
            keep(s).start()

    def item(k):
        both = pick([4 * s + b for s, b in ITEMS], k, 4)
        return lax.div(both, 4), lax.rem(both, 4)

    def n_load(k):
        s, kind = item(k)
        return pltpu.make_async_copy(ng.at[s, rowblock(mlp_chip(kind))], nt.at[lax.rem(k, 2)], nl_sem.at[lax.rem(k, 2)])

    def o_load(k):
        s, kind = item(k)
        return pltpu.make_async_copy(obuf.at[s, rowblock(mlp_chip(kind))],
                                     ho.at[lax.rem(k, SLOTS), :, pl.ds(2 * ff, 2 * head)], ol_sem.at[lax.rem(k, SLOTS)])

    def mlp_up(k):
        with jax.named_scope("n_wait"):
            n_load(k).wait()

        @pl.when(k == 0)
        def _():
            with jax.named_scope("have_up"):
                have(UP0)
                have(UP1)
                w_own(1).wait()

        src, dst = lax.rem(k, 2), lax.rem(k, SLOTS)

        def up(t, _):
            cols = pl.ds(pl.multiple_of(t * chunk, chunk), chunk)
            hid = jnp.dot(nt[src], wu[:, cols], preferred_element_type=F32)
            ho[dst, :, cols] = (0.5 * hid * (1.0 + lax.erf(hid * 0.7071067811865476))).astype(BF16)
            return 0

        lax.fori_loop(0, 2 * ff // chunk, up, 0, unroll=True)

    def stage_free(k):
        s, kind = item(k)
        sp(s, kind, lax.rem(k, 2)).wait_send()

    def own_stored(k):
        s, kind = item(k)
        own_store(s, kind, lax.rem(k, 2)).wait()

    def mlp_down(k):
        s, kind = item(k)
        slot, src = lax.rem(k, 2), lax.rem(k, SLOTS)
        with jax.named_scope("o_wait"):
            o_load(k).wait()

        @pl.when(k == 0)
        def _():
            with jax.named_scope("have_dn"):
                for p in range(DN0, OUT + 1):
                    have(p)
                w_own(2).wait()
                w_own(3).wait()

        @pl.when(k >= 2)
        def _():
            with jax.named_scope("stage_free"):
                stage_free(k - 2)

        def down(r, size):
            def one(t, _):
                cols = pl.ds(pl.multiple_of(t * chunk, chunk), chunk)
                stage[slot, pl.ds(r, size), cols] = jnp.dot(
                    ho[src, pl.ds(r, size), :], wd[:, cols], preferred_element_type=F32).astype(BF16)
                return 0

            lax.fori_loop(0, d_model // chunk, one, 0, unroll=True)

        split = (k == 0) | (k == len(ITEMS) - 1)

        @pl.when(jnp.logical_not(split))
        def _():
            down(0, blk)
            sp(s, kind, slot).start()

        @pl.when(split)
        def _():
            def part_of(p, _):
                down(pl.multiple_of(jnp.where(p == 0, o, j) * rows, rows), rows)

                @pl.when(p == 0)
                def _():
                    sp(s, kind, slot).start()

                return 0

            lax.fori_loop(0, 2, part_of, 0)

        own_store(s, kind, slot).start()

    def act(name):
        what, arg = name[:2], name[2:]
        if what == "pq":
            pass_quarter(PIECE[arg])
        elif what == "ph":
            pass_halves(PIECE[arg])
        elif what == "rm":
            relay_mate(int(arg))
        elif what == "rp":
            relay_part(int(arg[0]), int(arg[1]))
        elif what == "rf":
            relay_far(int(arg))
        elif what == "ld":
            tile_start(int(arg[0]), int(arg[1]))
        elif what == "nm":
            nm(int(arg[0]), int(arg[1])).start()
        elif what == "ad":
            add_now(arg)
        elif what == "ow":
            context_out(int(arg))
        elif what == "ln":
            n_load(jnp.int32(int(arg))).start()
        else:
            o_load(jnp.int32(int(arg))).start()

    for i in range(4):
        w_own(i).start()
    for name in START:
        with jax.named_scope(name):
            act(name)
    with jax.named_scope("have_qkv"):
        w_own(0).wait()
        for k in (W_Q, W_K, W_V):
            have(k)

    codes = [code_of(step) for step in ORDER]

    def add_code(name):
        return 1 + 4 * int(name[0]) + BLOCKS.index(name[1]) + 12 * (1 + BEFORE_SUM[name])

    adds = [add_code(ADDS[t]) if t in ADDS else 0 for t in range(len(ORDER))]

    def adding(code, do):
        @pl.when(code > 0)
        def _():
            which = lax.rem(code - 1, 12)
            for kind in range(4):
                @pl.when(lax.rem(which, 4) == kind)
                def _(kind=kind):
                    do(lax.div(which, 4), kind, lax.div(code - 1, 12) - 1)

    def events(t, lo, size):
        if not any(p in BEFORE for p in range(lo, lo + size)):
            return
        if size == 1:
            for name in BEFORE[lo]:
                with jax.named_scope(name):
                    act(name)
            return
        size //= 4
        for q in range(lo, lo + 4 * size, size):
            @pl.when(lax.div(t, size) == q // size)
            def _(q=q):
                events(t, q, size)

    def run(t, before):
        events(t, 0, 64)
        code, add = pick(codes, t, 6), pick(adds, t, 6)
        with jax.named_scope("add_start"):
            adding(add, add_start)
        what, index = lax.div(code, 16), lax.rem(code, 16)
        names = ("TILE", "ATT", "UP", "DOWN")
        for kind, body in ((TILE, tile), (ATT, attend), (UP, mlp_up), (DOWN, mlp_down)):
            @pl.when(what == kind)
            def _(kind=kind, body=body):
                with jax.named_scope(names[kind]):
                    body(index)

        with jax.named_scope("add_finish"):
            adding(add, lambda s, kind, _: add_finish(s, kind))

        @pl.when(lax.div(before, 16) == DOWN)
        def _():
            own_stored(lax.rem(before, 16))

        return code

    lax.fori_loop(0, len(ORDER), run, jnp.int32(0))
    own_stored(jnp.int32(len(ITEMS) - 1))
    with jax.named_scope("last_add"):
        for name in LAST_ADDS:
            add_now(name)
    for k in range(len(ITEMS) - 2, len(ITEMS)):
        stage_free(jnp.int32(k))
    for s in range(3):
        for h in range(2):
            nm(s, h).wait_send()
            np_(s, h).wait_send()
            nf(s, h).wait_send()
        for i in range(6):
            nd(s, i).wait_send()
    for k in range(PIECES):
        wx(k).wait_send()
        for i in range(4):
            wf(k, i).wait_send()
    with jax.named_scope("last_part"):
        for s in range(3):
            from_part(s).wait_recv()
    for name, s in LAST_SUM.items():
        sent(s, BLOCKS.index(name))


def residual_kernel(x, branch, y, xv, bv, x_sem, b_sem, y_sem):
    parts, step = xv.shape[0], min(64, xv.shape[1])

    def loads(p):
        return (pltpu.make_async_copy(x.at[p], xv.at[p], x_sem.at[p]),
                pltpu.make_async_copy(branch.at[p], bv.at[p], b_sem.at[p]))

    def store(p):
        return pltpu.make_async_copy(xv.at[p], y.at[p], y_sem.at[p])

    for p in range(parts):
        for ld in loads(p):
            ld.start()

    def add(p, _):
        for ld in loads(p):
            ld.wait()
        for r in range(0, xv.shape[1], step):
            rr = pl.ds(r, step)
            xv[p, rr, :] = (xv[p, rr, :].astype(F32) + bv[p, rr, :].astype(F32)).astype(BF16)
        store(p).start()
        return 0

    lax.fori_loop(0, parts, add, 0)
    for p in range(parts):
        store(p).wait()


def neighbour_span(groups):
    short = 1
    while short * short * 4 <= groups:
        short *= 2
    return groups // short


def solution(mesh):
    tp, groups = mesh.shape["tp"], mesh.shape["dp"]
    span = neighbour_span(groups)
    assert tp == 8 and groups % (2 * span) == 0 and span % 2 == 0

    def local_layer(x_blk, ln_gain, ln_bias, w_qkv, w_out, w_up, w_down):
        n_seq, rows, d_model = x_blk.shape
        head = w_qkv.shape[3]
        ff = w_up.shape[1]
        ns, seq, blk = n_seq // 2, rows * tp, 2 * rows
        assert ns == 3 and w_qkv.shape[1:3] == (1, 3)
        chunk = min(512, d_model, ff)
        ln_rows, add_rows = min(64, rows // 2), min(16, rows // 2)
        dims = (span, rows, d_model, head, ff, chunk, ln_rows, add_rows)
        dma = pltpu.SemaphoreType.DMA
        anyspace = pl.BlockSpec(memory_space=pl.ANY)
        vmem = pl.BlockSpec(memory_space=pltpu.VMEM)

        def hbm(*shape):
            return jax.ShapeDtypeStruct(shape, BF16)

        outs = pl.pallas_call(
            functools.partial(layer_kernel, dims),
            name="layer",
            out_shape=(hbm(n_seq, rows, d_model), hbm(ns, seq, d_model), hbm(ns, rows, d_model), hbm(ns, seq, 2 * head),
                       hbm(ns, 4, rows, d_model), hbm(ns, 4, rows, d_model), hbm(ns, 2, rows, d_model)),
            in_specs=[anyspace, vmem, vmem, anyspace, anyspace, anyspace, anyspace],
            out_specs=(anyspace,) * 7,
            scratch_shapes=[
                pltpu.VMEM((3, d_model, 2 * head), BF16),
                pltpu.VMEM((d_model, 2 * ff), BF16),
                pltpu.VMEM((2 * ff + 2 * head, d_model), BF16),
                pltpu.VMEM((2, blk, d_model), BF16),
                pltpu.VMEM((2, blk, d_model), BF16),
                pltpu.VMEM((seq, 4 * head), BF16),
                pltpu.VMEM((2 * head, seq), BF16),
                pltpu.VMEM((2, blk, 2 * head), BF16),
                pltpu.VMEM((SLOTS, blk, 2 * ff + 2 * head), BF16),
                pltpu.VMEM((2, blk, d_model), BF16),
                pltpu.VMEM((3, rows, d_model), BF16),
                pltpu.VMEM((4, rows, d_model), BF16),
                pltpu.VMEM((2, head, blk), F32),
                pltpu.VMEM((2, 1, blk), F32),
                pltpu.VMEM((2, 1, blk), F32),
                dma((4,)), dma((PIECES,)), dma((PIECES,)), dma((PIECES, 4)), dma((PIECES, 4)),
                dma((ns, 2)), dma((ns, 2)), dma((ns, 2)), dma((ns, 2)), dma((ns, 2)), dma((ns, 2)),
                dma((ns, 6)), dma((ns, 6)),
                dma((ns, 4)), dma((ns, 4)), dma((2,)), dma((ns, 2)), dma((ns, 2)), dma((ns,)), dma((ns,)),
                dma((6,)), dma((2,)), dma((2,)), dma((2,)), dma((SLOTS,)), dma((3,)), dma,
            ],
            compiler_params=pltpu.CompilerParams(
                collective_id=0, has_side_effects=True, vmem_limit_bytes=VMEM_LIMIT),
        )(x_blk, ln_gain.reshape(1, d_model), ln_bias.reshape(1, d_model),
          jnp.transpose(w_qkv[:, 0], (1, 0, 2)), w_out, w_up, w_down)
        cut = (4 * n_seq, rows // 4, d_model)
        y = pl.pallas_call(
            residual_kernel, name="residual", in_specs=[anyspace, anyspace], out_specs=anyspace,
            out_shape=hbm(*cut),
            scratch_shapes=[pltpu.VMEM(cut, BF16), pltpu.VMEM(cut, BF16), dma(cut[:1]), dma(cut[:1]), dma(cut[:1])],
            compiler_params=pltpu.CompilerParams(vmem_limit_bytes=VMEM_LIMIT),
        )(x_blk.reshape(cut), outs[0].reshape(cut))
        return y.reshape(n_seq, rows, d_model)

    return jax.shard_map(
        local_layer, mesh=mesh,
        in_specs=(P("dp", "tp", None), P(), P(), P(None, "tp", None, None),
                  P("tp", None), P(None, "tp"), P("tp", None)),
        out_specs=P("dp", "tp", None), check_vma=False)
```

```python
import functools

import jax
import jax.numpy as jnp
from jax import lax
from jax.experimental import pallas as pl
from jax.experimental.pallas import tpu as pltpu
from jax.sharding import PartitionSpec as P

LN_EPS = 1e-5
MESH = pl.DeviceIdType.MESH
BF16 = jnp.bfloat16
F32 = jnp.float32
LOG2E = 1.4426950408889634
VMEM_LIMIT = 67_043_328

W_Q, W_K, W_V, UP0, UP1, DN0, DN1, DN2, DN3, OUT = range(10)
PIECES = 10
FAR, MATE, PART, OWN = range(4)
TILE, ATT, UP, DOWN = range(4)
INTER = ("Q2", "Q0", "Q1", "p01", "p00", "D3", "U0", "U1", "p10", "p11", "D0", "O", "D2", "D1", "p21", "p20")
ORDER = ("A00", "A01", "A02", "A03", "T00", "T01", "T02", "T03", "A10", "A11", "U0F", "A12",
         "U0M", "U1M", "A13", "T10", "T11", "T12", "U1F", "T13", "D0F", "A20", "A21", "A22",
         "D0M", "A23", "T20", "D1M", "D1F", "U0P", "U1P", "D0P", "D1P", "U2F", "T21", "T22",
         "T23", "U2P", "D2F", "U2M", "U0O", "D2P", "D2M", "D0O", "U1O", "D1O", "U2O", "D2O",
         )
START = ("pqQ2", "pqQ0", "phQ2", "pqQ1", "phQ0", "rm0", "nm10", "phQ1", "rp01")
BEFORE = {
    0: ("ld00", "ld01"),
    2: ("rp00", "pqD3", "ld02"),
    3: ("phD3", "pqU0", "nm11", "rf0", "ld03", "ln0"),
    4: ("pqU1", "nm20"),
    6: ("phU0", "rm1"),
    7: ("ld10",),
    8: ("phU1", "rp10", "ld11"),
    10: ("rp11", "ln1", "ow0", "lo0"),
    11: ("pqD0", "ld12"),
    12: ("pqO", "ln2", "lo1"),
    13: ("phD0", "pqD2", "rf1", "nm21"),
    14: ("ld13", "ln3"),
    15: ("pqD1", "phO"),
    17: ("rm2",),
    18: ("phD2", "rp21", "ln4"),
    19: ("phD1",),
    20: ("rp20", "ld20", "ow1", "lo2", "lo3"),
    21: ("ld21",),
    22: ("ad0F", "ld22"),
    23: ("rf2",),
    25: ("ld23",),
    29: ("ln5", "lo4"),
    30: ("ln6", "lo5"),
    33: ("ln7",),
    37: ("ln8", "ow2", "lo6", "lo7"),
    39: ("ln9", "lo8"),
    40: ("ad2F", "ln10", "lo9"),
    44: ("ad2M", "ad2P", "ln11", "lo10"),
    46: ("lo11",),
}
ADDS = { 26: "0M", 30: "1F", 32: "1M", 33: "0P", 39: "1P", 45: "0O", 47: "1O" }
LAST_ADDS = ("2O",)

KINDS = "ATUD"
BLOCKS = "FMPO"
ITEMS = tuple((int(x[1]), BLOCKS.index(x[2])) for x in ORDER if x[0] == "U")
SLOTS = 4
PIECE = {"Q0": W_Q, "Q1": W_K, "Q2": W_V, "U0": UP0, "U1": UP1,
         "D0": DN0, "D1": DN1, "D2": DN2, "D3": DN3, "O": OUT}


def code_of(step):
    what, s = KINDS.index(step[0]), int(step[1])
    return 16 * what + (4 * s + int(step[2]) if what < UP else ITEMS.index((s, BLOCKS.index(step[2]))))


def pick(values, i, bits):
    per = 30 // bits
    words = [sum(v << bits * p for p, v in enumerate(values[w:w + per])) for w in range(0, len(values), per)]
    word, at = lax.div(i, per), lax.rem(i, per)
    packed = jnp.int32(words[0])
    for w in range(1, len(words)):
        packed = jnp.where(word == w, words[w], packed)
    out = packed
    for p in range(1, per):
        out = jnp.where(at == p, lax.div(packed, 1 << bits * p), out)
    return lax.rem(out, 1 << bits)


def sums():
    seq = []
    for t in range(len(ORDER)):
        seq += [(name[2:], t) for name in BEFORE.get(t, ()) if name[:2] == "ad"]
        if t in ADDS:
            seq.append((ADDS[t], t))
    seq += [(name, None) for name in LAST_ADDS]
    last, before = {}, {}
    for name, _ in seq:
        before[name] = last.get(name[1], -1)
        last[name[1]] = int(name[0])
    assert len(seq) == len(ITEMS)
    return before, last


BEFORE_SUM, LAST_SUM = sums()


def layer_kernel(dims, x, gain, bias, w_qkv, w_out, w_up, w_dn,
                 branch, ng, nout, obuf, ownp, sibin, mid,
                 wq, wu, wd, xt, nt, qk, vt, ot, ho, stage, cin, tbuf, acc, m_s, l_s,
                 w_l, wx_s, wx_r, wf_s, wf_r, nm_s, nm_r, np_s, np_r, nf_s, nf_r, nd_s, nd_r,
                 sp_s, sp_r, op_sem, t_s, t_r, p_s, p_r,
                 ln_sem, xt_sem, oo_sem, nl_sem, ol_sem, cl_sem, br_sem):
    span, rows, d_model, head, ff, chunk, ln_rows, add_rows = dims
    half = rows // 2
    blk = 2 * rows
    scale = LOG2E * head ** -0.5

    g, me = lax.axis_index("dp"), lax.axis_index("tp")
    c, j = lax.div(me, 2), lax.rem(me, 2)
    o = 1 - j
    pair = lax.div(c, 2)
    mate = c + 1 - 2 * lax.rem(c, 2)
    part = 3 - c
    far = 3 - mate
    zb, yb = lax.rem(g, 2), lax.rem(lax.div(g, span), 2)
    gz, gy = g + 1 - 2 * zb, g + span * (1 - 2 * yb)

    def dev(chip, core, group=g):
        return {"dp": group, "tp": 2 * chip + core}

    sib, mt, pt, zd, yd = dev(c, o), dev(mate, j), dev(part, j), dev(c, j, gz), dev(c, j, gy)

    def remote(src, dst, send, recv, to):
        return pltpu.make_async_remote_copy(src_ref=src, dst_ref=dst, send_sem=send, recv_sem=recv,
                                            device_id=to, device_id_type=MESH)

    def row(chip, core, extra=0):
        return pl.multiple_of((2 * chip + core) * rows + extra, half)

    def rowblock(chip):
        return pl.ds(pl.multiple_of(chip * blk, blk), blk)

    quarter = 2 * yb + zb
    q_z, q_y, q_zy = quarter + 1 - 2 * zb, quarter + 2 - 4 * yb, 3 - quarter

    def w_at(piece, q, side, hold):
        n = head // 4 if piece == OUT else ff // 16 if piece >= DN0 else d_model // 8 if piece >= UP0 else d_model // 4
        size = n if side is None else n // 2
        off = q * n + (0 if side is None else side * size)
        if UP0 <= piece <= DN3:
            off = off + (piece - (UP0 if piece <= UP1 else DN0)) * 4 * n
        if hold and DN0 <= piece <= DN3:
            off = off + ff
        if hold and piece == OUT:
            off = off + 2 * ff + head
        at = pl.ds(pl.multiple_of(off, n // 2), size)
        if piece <= W_V:
            return wq.at[piece, at, pl.ds(head, head)] if hold else w_qkv.at[piece, at, :]
        if piece <= UP1:
            return wu.at[at, pl.ds(ff, ff)] if hold else w_up.at[at, :]
        return wd.at[at, :] if hold else (w_out if piece == OUT else w_dn).at[at, :]

    def w_own(i):
        src, dst = ((w_qkv, wq.at[:, :, pl.ds(0, head)]), (w_up, wu.at[:, pl.ds(0, ff)]),
                    (w_dn, wd.at[pl.ds(0, ff), :]), (w_out, wd.at[pl.ds(2 * ff, head), :]))[i]
        return pltpu.make_async_copy(src, dst, w_l.at[i])

    def wx(k):
        return remote(w_at(k, quarter, None, False), w_at(k, quarter, None, True), wx_s.at[k], wx_r.at[k], pt)

    def wx_in(k):
        ref = w_at(k, quarter, None, True)
        return remote(ref, ref, wx_s.at[k], wx_r.at[k], pt)

    def wf(k, i):
        ref = (w_at(k, quarter, None, True) if i < 2 else w_at(k, q_y, 1, True) if i == 2 else w_at(k, q_z, 0, True))
        return remote(ref, ref, wf_s.at[k, i], wf_r.at[k, i], yd if i in (1, 3) else zd)

    def wf_in(k, i):
        ref = w_at(k, (q_z, q_y, q_zy, q_zy)[i], (None, None, 1, 0)[i], True)
        return remote(ref, ref, wf_s.at[k, i], wf_r.at[k, i], yd if i in (1, 3) else zd)

    def pass_quarter(k):
        wx_in(k).wait_recv()
        wf(k, 0).start()
        wf(k, 1).start()

    def pass_halves(k):
        wf_in(k, 0).wait_recv()
        wf_in(k, 1).wait_recv()
        wf(k, 2).start()
        wf(k, 3).start()

    def have(k):
        wf_in(k, 2).wait_recv()
        wf_in(k, 3).wait_recv()

    def own_seq(s):
        return 2 * s + pair

    def other_seq(s):
        return 2 * s + 1 - pair

    def n_own(s):
        return ng.at[s, pl.ds(row(c, j), rows)]

    def nm(s, h):
        ref = ng.at[s, pl.ds(row(c, j, h * half), half)]
        return remote(ref, ref, nm_s.at[s, h], nm_r.at[s, h], mt)

    def nm_in(s, h):
        ref = ng.at[s, pl.ds(row(mate, j, h * half), half)]
        return remote(ref, ref, nm_s.at[s, h], nm_r.at[s, h], mt)

    def np_(s, h):
        return remote(nout.at[s, pl.ds(h * half, half)], ng.at[s, pl.ds(row(c, j, h * half), half)],
                      np_s.at[s, h], np_r.at[s, h], pt)

    def np_in(s, h):
        ref = ng.at[s, pl.ds(row(part, j, h * half), half)]
        return remote(ref, ref, np_s.at[s, h], np_r.at[s, h], pt)

    def nf(s, h):
        ref = ng.at[s, pl.ds(row(part, j, h * half), half)]
        return remote(ref, ref, nf_s.at[s, h], nf_r.at[s, h], mt)

    def nf_in(s, h):
        ref = ng.at[s, pl.ds(row(far, j, h * half), half)]
        return remote(ref, ref, nf_s.at[s, h], nf_r.at[s, h], mt)

    def nd(s, i, core=j):
        ref = (ng.at[s, pl.ds(row(c if i == 0 else mate, core), rows)] if i < 2 else
               ng.at[s, pl.ds(row(part if i < 4 else far, core, (i % 2) * half), half)])
        return remote(ref, ref, nd_s.at[s, i], nd_r.at[s, i], sib)

    def nd_in(s, i):
        return nd(s, i, o)

    def relay_mate(s):
        for h in range(2):
            nm_in(s, h).wait_recv()
        nd(s, 1).start()

    def relay_part(s, h):
        np_in(s, h).wait_recv()
        nf(s, h).start()
        nd(s, 2 + h).start()

    def relay_far(s):
        for h in range(2):
            nf_in(s, h).wait_recv()
            nd(s, 4 + h).start()

    def ln_buf(b):
        return (xt if b < 4 else nt).at[(b // 2) % 2, pl.ds((b % 2) * rows, rows)]

    def ln_load(b):
        return pltpu.make_async_copy(x.at[own_seq(b // 2) if b % 2 else other_seq(b // 2)], ln_buf(b), ln_sem.at[b])

    def ln_store(b):
        return pltpu.make_async_copy(ln_buf(b), n_own(b // 2) if b % 2 else nout.at[b // 2], ln_sem.at[b])

    def normalise(b):
        ln_load(b).wait()
        buf = ln_buf(b)

        def norm(r, _):
            rr = pl.ds(pl.multiple_of(r * ln_rows, ln_rows), ln_rows)
            v = buf[rr, :].astype(F32)
            mean = jnp.mean(v, axis=-1, keepdims=True)
            cen = v - mean
            var = jnp.mean(cen * cen, axis=-1, keepdims=True)
            buf[rr, :] = (cen * lax.rsqrt(var + LN_EPS) * gain[...] + bias[...]).astype(BF16)
            return 0

        lax.fori_loop(0, rows // ln_rows, norm, 0)
        ln_store(b).start()

    barrier = pltpu.get_barrier_semaphore()
    for to in (sib, mt, pt, zd, yd):
        pl.semaphore_signal(barrier, inc=1, device_id=to, device_id_type=MESH)
    for b in range(6):
        ln_load(b).start()
    with jax.named_scope("barrier"):
        pl.semaphore_wait(barrier, 5)

    first = next(i for i, name in enumerate(INTER) if name[0] == "p")
    for name in INTER[:first]:
        wx(PIECE[name]).start()
    normalise(0)
    normalise(1)
    begun = set()
    for name in INTER[first:]:
        if name[0] != "p":
            wx(PIECE[name]).start()
            continue
        s, h = int(name[1]), int(name[2])
        if s not in begun:
            if s > 0:
                normalise(2 * s)
                normalise(2 * s + 1)
            ln_store(2 * s).wait()
        np_(s, h).start()
        if s == 0 and s not in begun:
            ln_store(1).wait()
            nm(0, 0).start()
            nm(0, 1).start()
            nd(0, 0).start()
        begun.add(s)
    for s in (1, 2):
        ln_store(2 * s + 1).wait()
        nd(s, 0).start()

    def tile_chip(i):
        return jnp.where(i == 0, c, jnp.where(i == 1, mate, jnp.where(i == 2, part, far)))

    def mlp_chip(kind):
        return jnp.where(kind == FAR, far, jnp.where(kind == MATE, mate, jnp.where(kind == PART, part, c)))

    def tile_copy(s, i):
        return pltpu.make_async_copy(ng.at[s, rowblock(tile_chip(i))], xt.at[lax.rem(i, 2)], xt_sem.at[lax.rem(i, 2)])

    def tile_start(s, i):
        for n in ((0,), (1,), (2, 3), (4, 5))[i]:
            nd_in(s, n).wait_recv()
        tile_copy(s, jnp.int32(i)).start()

    def tile(index):
        s, i = lax.div(index, 4), lax.rem(index, 4)
        with jax.named_scope("tile_wait"):
            tile_copy(s, i).wait()
        slot = lax.rem(i, 2)
        base = rowblock(tile_chip(i))
        for t in range(2):
            qk[base, pl.ds(t * 2 * head, 2 * head)] = jnp.dot(
                xt[slot], wq[t], preferred_element_type=F32).astype(BF16)
        vt[:, base] = jnp.transpose(jnp.dot(xt[slot], wq[2], preferred_element_type=F32)).astype(BF16)

    def dot_t(a, b):
        return lax.dot_general(a, b, (((1,), (1,)), ((), ())), preferred_element_type=F32)

    def o_out(s, i):
        return pltpu.make_async_copy(ot.at[lax.rem(i, 2)], obuf.at[s, rowblock(i)], oo_sem.at[lax.rem(i, 2)])

    def attend(index):
        s, i = lax.div(index, 4), lax.rem(index, 4)
        slot = lax.rem(i, 2)

        @pl.when(i >= 2)
        def _():
            o_out(s, i).wait()

        mine = rowblock(i)
        causal = (lax.broadcasted_iota(jnp.int32, (blk, blk), 0)
                  <= lax.broadcasted_iota(jnp.int32, (blk, blk), 1))
        for h in range(2):
            hd = pl.ds(h * head, head)
            sc = jnp.where(causal, dot_t(qk[mine, pl.ds((2 + h) * head, head)], qk[mine, hd]), -jnp.inf)
            top = jnp.max(sc, axis=0, keepdims=True)
            p = jnp.exp2((sc - top) * scale)
            m_s[h] = top
            l_s[h] = jnp.sum(p, axis=0, keepdims=True)
            acc[h] = jnp.dot(vt[hd, mine], p.astype(BF16), preferred_element_type=F32)

        def earlier(t, _):
            there = rowblock(t)
            for h in range(2):
                hd = pl.ds(h * head, head)
                sc = dot_t(qk[there, pl.ds((2 + h) * head, head)], qk[mine, hd])
                old = m_s[h]
                top = jnp.maximum(old, jnp.max(sc, axis=0, keepdims=True))
                p = jnp.exp2((sc - top) * scale)
                fade = jnp.exp2((old - top) * scale)
                m_s[h] = top
                l_s[h] = l_s[h] * fade + jnp.sum(p, axis=0, keepdims=True)
                acc[h] = acc[h] * fade + jnp.dot(vt[hd, there], p.astype(BF16), preferred_element_type=F32)
            return 0

        lax.fori_loop(0, i, earlier, 0)
        for h in range(2):
            ot[slot, :, pl.ds(h * head, head)] = jnp.transpose(acc[h] * (1.0 / l_s[h])).astype(BF16)
        o_out(s, i).start()

    def context_out(s):
        for i in (2, 3):
            o_out(jnp.int32(s), jnp.int32(i)).wait()

    def sp(s, kind, slot):
        return remote(stage.at[slot, pl.ds(pl.multiple_of(o * rows, rows), rows)], sibin.at[s, kind],
                      sp_s.at[s, kind], sp_r.at[s, kind], sib)

    def own_store(s, kind, slot):
        return pltpu.make_async_copy(stage.at[slot, pl.ds(pl.multiple_of(j * rows, rows), rows)], ownp.at[s, kind],
                                     op_sem.at[slot])

    def to_mate(s, kind):
        return remote(tbuf.at[kind], mid.at[s, kind], t_s.at[s, kind], t_r.at[s, kind], mt)

    def from_mate(s, kind):
        return remote(mid.at[s, kind], mid.at[s, kind], t_s.at[s, kind], t_r.at[s, kind], mt)

    def to_part(s):
        return remote(tbuf.at[PART], branch.at[own_seq(s)], p_s.at[s], p_r.at[s], pt)

    def from_part(s):
        return remote(branch.at[other_seq(s)], branch.at[other_seq(s)], p_s.at[s], p_r.at[s], pt)

    def keep(s):
        return pltpu.make_async_copy(tbuf.at[OWN], branch.at[own_seq(s)], br_sem)

    def sent(s, kind):
        if kind < PART:
            to_mate(s, kind).wait_send()
        elif kind == PART:
            to_part(s).wait_send()
        else:
            keep(s).wait()

    def add_now(name):
        s, kind = jnp.int32(int(name[0])), BLOCKS.index(name[1])
        add_start(s, kind, jnp.int32(BEFORE_SUM[name]))
        add_finish(s, kind)

    def add_loads(s, kind):
        srcs = [ownp.at[s, kind], sibin.at[s, kind]] + ([mid.at[s, kind - PART]] if kind >= PART else [])
        return [pltpu.make_async_copy(src, cin.at[n], cl_sem.at[n]) for n, src in enumerate(srcs)]

    def add_start(s, kind, before):
        remote(sibin.at[s, kind], sibin.at[s, kind], sp_s.at[s, kind], sp_r.at[s, kind], sib).wait_recv()
        if kind >= PART:
            from_mate(s, kind - PART).wait_recv()

        @pl.when(before >= 0)
        def _():
            sent(before, kind)

        for ld in add_loads(s, kind):
            ld.start()

    def add_finish(s, kind):
        for ld in add_loads(s, kind):
            ld.wait()

        def add(r, _):
            rr = pl.ds(pl.multiple_of(r * add_rows, add_rows), add_rows)
            if kind < PART:
                tbuf[kind, rr, :] = cin[0, rr, :] + cin[1, rr, :]
            else:
                tbuf[kind, rr, :] = (cin[0, rr, :].astype(F32) + cin[1, rr, :].astype(F32)
                                     + cin[2, rr, :].astype(F32)).astype(BF16)
            return 0

        lax.fori_loop(0, rows // add_rows, add, 0)
        if kind < PART:
            to_mate(s, kind).start()
        elif kind == PART:
            to_part(s).start()
        else:
            keep(s).start()

    def item(k):
        both = pick([4 * s + b for s, b in ITEMS], k, 4)
        return lax.div(both, 4), lax.rem(both, 4)

    def n_load(k):
        s, kind = item(k)
        return pltpu.make_async_copy(ng.at[s, rowblock(mlp_chip(kind))], nt.at[lax.rem(k, 2)], nl_sem.at[lax.rem(k, 2)])

    def o_load(k):
        s, kind = item(k)
        return pltpu.make_async_copy(obuf.at[s, rowblock(mlp_chip(kind))],
                                     ho.at[lax.rem(k, SLOTS), :, pl.ds(2 * ff, 2 * head)], ol_sem.at[lax.rem(k, SLOTS)])

    def mlp_up(k):
        with jax.named_scope("n_wait"):
            n_load(k).wait()

        @pl.when(k == 0)
        def _():
            with jax.named_scope("have_up"):
                have(UP0)
                have(UP1)
                w_own(1).wait()

        src, dst = lax.rem(k, 2), lax.rem(k, SLOTS)

        def up(t, _):
            cols = pl.ds(pl.multiple_of(t * chunk, chunk), chunk)
            hid = jnp.dot(nt[src], wu[:, cols], preferred_element_type=F32)
            ho[dst, :, cols] = (0.5 * hid * (1.0 + lax.erf(hid * 0.7071067811865476))).astype(BF16)
            return 0

        lax.fori_loop(0, 2 * ff // chunk, up, 0, unroll=True)

    def stage_free(k):
        s, kind = item(k)
        sp(s, kind, lax.rem(k, 2)).wait_send()

    def own_stored(k):
        s, kind = item(k)
        own_store(s, kind, lax.rem(k, 2)).wait()

    def mlp_down(k):
        s, kind = item(k)
        slot, src = lax.rem(k, 2), lax.rem(k, SLOTS)
        with jax.named_scope("o_wait"):
            o_load(k).wait()

        @pl.when(k == 0)
        def _():
            with jax.named_scope("have_dn"):
                for p in range(DN0, OUT + 1):
                    have(p)
                w_own(2).wait()
                w_own(3).wait()

        @pl.when(k >= 2)
        def _():
            with jax.named_scope("stage_free"):
                stage_free(k - 2)

        def down(r, size):
            def one(t, _):
                cols = pl.ds(pl.multiple_of(t * chunk, chunk), chunk)
                stage[slot, pl.ds(r, size), cols] = jnp.dot(
                    ho[src, pl.ds(r, size), :], wd[:, cols], preferred_element_type=F32).astype(BF16)
                return 0

            lax.fori_loop(0, d_model // chunk, one, 0, unroll=True)

        split = (k == 0) | (k == len(ITEMS) - 1)

        @pl.when(jnp.logical_not(split))
        def _():
            down(0, blk)
            sp(s, kind, slot).start()

        @pl.when(split)
        def _():
            def part_of(p, _):
                down(pl.multiple_of(jnp.where(p == 0, o, j) * rows, rows), rows)

                @pl.when(p == 0)
                def _():
                    sp(s, kind, slot).start()

                return 0

            lax.fori_loop(0, 2, part_of, 0)

        own_store(s, kind, slot).start()

    def act(name):
        what, arg = name[:2], name[2:]
        if what == "pq":
            pass_quarter(PIECE[arg])
        elif what == "ph":
            pass_halves(PIECE[arg])
        elif what == "rm":
            relay_mate(int(arg))
        elif what == "rp":
            relay_part(int(arg[0]), int(arg[1]))
        elif what == "rf":
            relay_far(int(arg))
        elif what == "ld":
            tile_start(int(arg[0]), int(arg[1]))
        elif what == "nm":
            nm(int(arg[0]), int(arg[1])).start()
        elif what == "ad":
            add_now(arg)
        elif what == "ow":
            context_out(int(arg))
        elif what == "ln":
            n_load(jnp.int32(int(arg))).start()
        else:
            o_load(jnp.int32(int(arg))).start()

    for i in range(4):
        w_own(i).start()
    for name in START:
        with jax.named_scope(name):
            act(name)
    with jax.named_scope("have_qkv"):
        w_own(0).wait()
        for k in (W_Q, W_K, W_V):
            have(k)

    codes = [code_of(step) for step in ORDER]

    def add_code(name):
        return 1 + 4 * int(name[0]) + BLOCKS.index(name[1]) + 12 * (1 + BEFORE_SUM[name])

    adds = [add_code(ADDS[t]) if t in ADDS else 0 for t in range(len(ORDER))]

    def adding(code, do):
        @pl.when(code > 0)
        def _():
            which = lax.rem(code - 1, 12)
            for kind in range(4):
                @pl.when(lax.rem(which, 4) == kind)
                def _(kind=kind):
                    do(lax.div(which, 4), kind, lax.div(code - 1, 12) - 1)

    def events(t, lo, size):
        if not any(p in BEFORE for p in range(lo, lo + size)):
            return
        if size == 1:
            for name in BEFORE[lo]:
                with jax.named_scope(name):
                    act(name)
            return
        size //= 4
        for q in range(lo, lo + 4 * size, size):
            @pl.when(lax.div(t, size) == q // size)
            def _(q=q):
                events(t, q, size)

    def run(t, before):
        events(t, 0, 64)
        code, add = pick(codes, t, 6), pick(adds, t, 6)
        with jax.named_scope("add_start"):
            adding(add, add_start)
        what, index = lax.div(code, 16), lax.rem(code, 16)
        names = ("TILE", "ATT", "UP", "DOWN")
        for kind, body in ((TILE, tile), (ATT, attend), (UP, mlp_up), (DOWN, mlp_down)):
            @pl.when(what == kind)
            def _(kind=kind, body=body):
                with jax.named_scope(names[kind]):
                    body(index)

        with jax.named_scope("add_finish"):
            adding(add, lambda s, kind, _: add_finish(s, kind))

        @pl.when(lax.div(before, 16) == DOWN)
        def _():
            own_stored(lax.rem(before, 16))

        return code

    lax.fori_loop(0, len(ORDER), run, jnp.int32(0))
    own_stored(jnp.int32(len(ITEMS) - 1))
    with jax.named_scope("last_add"):
        for name in LAST_ADDS:
            add_now(name)
    for k in range(len(ITEMS) - 2, len(ITEMS)):
        stage_free(jnp.int32(k))
    for s in range(3):
        for h in range(2):
            nm(s, h).wait_send()
            np_(s, h).wait_send()
            nf(s, h).wait_send()
        for i in range(6):
            nd(s, i).wait_send()
    for k in range(PIECES):
        wx(k).wait_send()
        for i in range(4):
            wf(k, i).wait_send()
    with jax.named_scope("last_part"):
        for s in range(3):
            from_part(s).wait_recv()
    for name, s in LAST_SUM.items():
        sent(s, BLOCKS.index(name))


def residual_kernel(x, branch, y, xv, bv, x_sem, b_sem, y_sem):
    parts, step = xv.shape[0], min(64, xv.shape[1])

    def loads(p):
        return (pltpu.make_async_copy(x.at[p], xv.at[p], x_sem.at[p]),
                pltpu.make_async_copy(branch.at[p], bv.at[p], b_sem.at[p]))

    def store(p):
        return pltpu.make_async_copy(xv.at[p], y.at[p], y_sem.at[p])

    for p in range(parts):
        for ld in loads(p):
            ld.start()

    def add(p, _):
        for ld in loads(p):
            ld.wait()
        for r in range(0, xv.shape[1], step):
            rr = pl.ds(r, step)
            xv[p, rr, :] = (xv[p, rr, :].astype(F32) + bv[p, rr, :].astype(F32)).astype(BF16)
        store(p).start()
        return 0

    lax.fori_loop(0, parts, add, 0)
    for p in range(parts):
        store(p).wait()


def neighbour_span(groups):
    short = 1
    while short * short * 4 <= groups:
        short *= 2
    return groups // short


def solution(mesh):
    tp, groups = mesh.shape["tp"], mesh.shape["dp"]
    span = neighbour_span(groups)
    assert tp == 8 and groups % (2 * span) == 0 and span % 2 == 0

    def local_layer(x_blk, ln_gain, ln_bias, w_qkv, w_out, w_up, w_down):
        n_seq, rows, d_model = x_blk.shape
        head = w_qkv.shape[3]
        ff = w_up.shape[1]
        ns, seq, blk = n_seq // 2, rows * tp, 2 * rows
        assert ns == 3 and w_qkv.shape[1:3] == (1, 3)
        chunk = min(512, d_model, ff)
        ln_rows, add_rows = min(64, rows // 2), min(16, rows // 2)
        dims = (span, rows, d_model, head, ff, chunk, ln_rows, add_rows)
        dma = pltpu.SemaphoreType.DMA
        anyspace = pl.BlockSpec(memory_space=pl.ANY)
        vmem = pl.BlockSpec(memory_space=pltpu.VMEM)

        def hbm(*shape):
            return jax.ShapeDtypeStruct(shape, BF16)

        outs = pl.pallas_call(
            functools.partial(layer_kernel, dims),
            name="layer",
            out_shape=(hbm(n_seq, rows, d_model), hbm(ns, seq, d_model), hbm(ns, rows, d_model), hbm(ns, seq, 2 * head),
                       hbm(ns, 4, rows, d_model), hbm(ns, 4, rows, d_model), hbm(ns, 2, rows, d_model)),
            in_specs=[anyspace, vmem, vmem, anyspace, anyspace, anyspace, anyspace],
            out_specs=(anyspace,) * 7,
            scratch_shapes=[
                pltpu.VMEM((3, d_model, 2 * head), BF16),
                pltpu.VMEM((d_model, 2 * ff), BF16),
                pltpu.VMEM((2 * ff + 2 * head, d_model), BF16),
                pltpu.VMEM((2, blk, d_model), BF16),
                pltpu.VMEM((2, blk, d_model), BF16),
                pltpu.VMEM((seq, 4 * head), BF16),
                pltpu.VMEM((2 * head, seq), BF16),
                pltpu.VMEM((2, blk, 2 * head), BF16),
                pltpu.VMEM((SLOTS, blk, 2 * ff + 2 * head), BF16),
                pltpu.VMEM((2, blk, d_model), BF16),
                pltpu.VMEM((3, rows, d_model), BF16),
                pltpu.VMEM((4, rows, d_model), BF16),
                pltpu.VMEM((2, head, blk), F32),
                pltpu.VMEM((2, 1, blk), F32),
                pltpu.VMEM((2, 1, blk), F32),
                dma((4,)), dma((PIECES,)), dma((PIECES,)), dma((PIECES, 4)), dma((PIECES, 4)),
                dma((ns, 2)), dma((ns, 2)), dma((ns, 2)), dma((ns, 2)), dma((ns, 2)), dma((ns, 2)),
                dma((ns, 6)), dma((ns, 6)),
                dma((ns, 4)), dma((ns, 4)), dma((2,)), dma((ns, 2)), dma((ns, 2)), dma((ns,)), dma((ns,)),
                dma((6,)), dma((2,)), dma((2,)), dma((2,)), dma((SLOTS,)), dma((3,)), dma,
            ],
            compiler_params=pltpu.CompilerParams(
                collective_id=0, has_side_effects=True, vmem_limit_bytes=VMEM_LIMIT),
        )(x_blk, ln_gain.reshape(1, d_model), ln_bias.reshape(1, d_model),
          jnp.transpose(w_qkv[:, 0], (1, 0, 2)), w_out, w_up, w_down)
        cut = (4 * n_seq, rows // 4, d_model)
        y = pl.pallas_call(
            residual_kernel, name="residual", in_specs=[anyspace, anyspace], out_specs=anyspace,
            out_shape=hbm(*cut),
            scratch_shapes=[pltpu.VMEM(cut, BF16), pltpu.VMEM(cut, BF16), dma(cut[:1]), dma(cut[:1]), dma(cut[:1])],
            compiler_params=pltpu.CompilerParams(vmem_limit_bytes=VMEM_LIMIT),
        )(x_blk.reshape(cut), outs[0].reshape(cut))
        return y.reshape(n_seq, rows, d_model)

    return jax.shard_map(
        local_layer, mesh=mesh,
        in_specs=(P("dp", "tp", None), P(), P(), P(None, "tp", None, None),
                  P("tp", None), P(None, "tp"), P("tp", None)),
        out_specs=P("dp", "tp", None), check_vma=False)
```

```python
import functools

import jax
import jax.numpy as jnp
from jax import lax
from jax.experimental import pallas as pl
from jax.experimental.pallas import tpu as pltpu
from jax.sharding import PartitionSpec as P

LN_EPS = 1e-5
MESH = pl.DeviceIdType.MESH
BF16 = jnp.bfloat16
F32 = jnp.float32
LOG2E = 1.4426950408889634
VMEM_LIMIT = 67_043_328

W_Q, W_K, W_V, UP0, UP1, DN0, DN1, DN2, DN3, OUT = range(10)
PIECES = 10
FAR, MATE, PART, OWN = range(4)
TILE, ATT, UP, DOWN = range(4)
INTER = ("Q2", "Q1", "Q0", "p01", "p00", "U0", "U1", "D2", "p11", "p10", "D0", "O", "D1", "D3", "p20", "p21")
ORDER = ("A00", "A01", "A02", "A03", "T00", "T01", "T02", "T03", "A10", "A11", "U0F", "U1M",
         "U0M", "A12", "A13", "T10", "T11", "T12", "T13", "A20", "D0F", "A21", "D1M", "U1F",
         "D0M", "A22", "U0P", "D1F", "A23", "T20", "D0P", "T21", "T22", "T23", "U2F", "D2F",
         "U1P", "D1P", "U2M", "D2M", "U2P", "U1O", "D2P", "D1O", "U0O", "D0O", "U2O", "D2O",
         )
START = ("pqQ2", "pqQ1", "phQ2", "pqQ0", "phQ1", "rm0", "nm10", "phQ0", "rp01")
BEFORE = {
    0: ("ld00", "ld01"),
    2: ("rp00", "ld02"),
    3: ("pqU0", "rf0", "nm11", "pqU1", "ld03", "ln0"),
    4: ("phU0", "pqD2"),
    5: ("nm20",),
    6: ("rm1",),
    7: ("phU1", "ld10"),
    8: ("rp11", "ld11"),
    10: ("phD2", "rp10", "ln1", "ow0", "lo0"),
    11: ("pqD0", "ln2"),
    12: ("pqO", "ld12", "lo2"),
    13: ("phD0", "pqD1", "rf1", "nm21"),
    14: ("ld13", "ln3"),
    15: ("pqD3", "phO"),
    18: ("phD1", "rm2", "rp20", "ld20"),
    19: ("phD3", "ow1", "lo1"),
    20: ("rp21", "ld21"),
    22: ("ad0F",),
    23: ("rf2", "ln4", "lo3"),
    24: ("ld22",),
    26: ("lo4",),
    27: ("ld23",),
    28: ("ln5",),
    34: ("ln6", "ow2", "lo5"),
    36: ("ln7", "lo6"),
    38: ("ln8", "lo7"),
    40: ("ln9", "lo8"),
    41: ("ln10", "lo9"),
    44: ("ln11", "lo10"),
    46: ("lo11",),
}
ADDS = { 24: "1M", 29: "1F", 32: "0P", 33: "0M", 37: "2F", 39: "1P", 41: "2M", 44: "2P", 45: "1O", 47: "0O" }
LAST_ADDS = ("2O",)

KINDS = "ATUD"
BLOCKS = "FMPO"
ITEMS = tuple((int(x[1]), BLOCKS.index(x[2])) for x in ORDER if x[0] == "U")
SLOTS = 4
PIECE = {"Q0": W_Q, "Q1": W_K, "Q2": W_V, "U0": UP0, "U1": UP1,
         "D0": DN0, "D1": DN1, "D2": DN2, "D3": DN3, "O": OUT}


def code_of(step):
    what, s = KINDS.index(step[0]), int(step[1])
    return 16 * what + (4 * s + int(step[2]) if what < UP else ITEMS.index((s, BLOCKS.index(step[2]))))


def pick(values, i, bits):
    per = 30 // bits
    words = [sum(v << bits * p for p, v in enumerate(values[w:w + per])) for w in range(0, len(values), per)]
    word, at = lax.div(i, per), lax.rem(i, per)
    packed = jnp.int32(words[0])
    for w in range(1, len(words)):
        packed = jnp.where(word == w, words[w], packed)
    out = packed
    for p in range(1, per):
        out = jnp.where(at == p, lax.div(packed, 1 << bits * p), out)
    return lax.rem(out, 1 << bits)


def sums():
    seq = []
    for t in range(len(ORDER)):
        seq += [(name[2:], t) for name in BEFORE.get(t, ()) if name[:2] == "ad"]
        if t in ADDS:
            seq.append((ADDS[t], t))
    seq += [(name, None) for name in LAST_ADDS]
    last, before = {}, {}
    for name, _ in seq:
        before[name] = last.get(name[1], -1)
        last[name[1]] = int(name[0])
    assert len(seq) == len(ITEMS)
    return before, last


BEFORE_SUM, LAST_SUM = sums()


def layer_kernel(dims, x, gain, bias, w_qkv, w_out, w_up, w_dn,
                 branch, ng, nout, obuf, ownp, sibin, mid,
                 wq, wu, wd, xt, nt, qk, vt, ot, ho, stage, cin, tbuf, acc, m_s, l_s,
                 w_l, wx_s, wx_r, wf_s, wf_r, nm_s, nm_r, np_s, np_r, nf_s, nf_r, nd_s, nd_r,
                 sp_s, sp_r, op_sem, t_s, t_r, p_s, p_r,
                 ln_sem, xt_sem, oo_sem, nl_sem, ol_sem, cl_sem, br_sem):
    span, rows, d_model, head, ff, chunk, ln_rows, add_rows = dims
    half = rows // 2
    blk = 2 * rows
    scale = LOG2E * head ** -0.5

    g, me = lax.axis_index("dp"), lax.axis_index("tp")
    c, j = lax.div(me, 2), lax.rem(me, 2)
    o = 1 - j
    pair = lax.div(c, 2)
    mate = c + 1 - 2 * lax.rem(c, 2)
    part = 3 - c
    far = 3 - mate
    zb, yb = lax.rem(g, 2), lax.rem(lax.div(g, span), 2)
    gz, gy = g + 1 - 2 * zb, g + span * (1 - 2 * yb)

    def dev(chip, core, group=g):
        return {"dp": group, "tp": 2 * chip + core}

    sib, mt, pt, zd, yd = dev(c, o), dev(mate, j), dev(part, j), dev(c, j, gz), dev(c, j, gy)

    def remote(src, dst, send, recv, to):
        return pltpu.make_async_remote_copy(src_ref=src, dst_ref=dst, send_sem=send, recv_sem=recv,
                                            device_id=to, device_id_type=MESH)

    def row(chip, core, extra=0):
        return pl.multiple_of((2 * chip + core) * rows + extra, half)

    def rowblock(chip):
        return pl.ds(pl.multiple_of(chip * blk, blk), blk)

    quarter = 2 * yb + zb
    q_z, q_y, q_zy = quarter + 1 - 2 * zb, quarter + 2 - 4 * yb, 3 - quarter

    def w_at(piece, q, side, hold):
        n = head // 4 if piece == OUT else ff // 16 if piece >= DN0 else d_model // 8 if piece >= UP0 else d_model // 4
        size = n if side is None else n // 2
        off = q * n + (0 if side is None else side * size)
        if UP0 <= piece <= DN3:
            off = off + (piece - (UP0 if piece <= UP1 else DN0)) * 4 * n
        if hold and DN0 <= piece <= DN3:
            off = off + ff
        if hold and piece == OUT:
            off = off + 2 * ff + head
        at = pl.ds(pl.multiple_of(off, n // 2), size)
        if piece <= W_V:
            return wq.at[piece, at, pl.ds(head, head)] if hold else w_qkv.at[piece, at, :]
        if piece <= UP1:
            return wu.at[at, pl.ds(ff, ff)] if hold else w_up.at[at, :]
        return wd.at[at, :] if hold else (w_out if piece == OUT else w_dn).at[at, :]

    def w_own(i):
        src, dst = ((w_qkv, wq.at[:, :, pl.ds(0, head)]), (w_up, wu.at[:, pl.ds(0, ff)]),
                    (w_dn, wd.at[pl.ds(0, ff), :]), (w_out, wd.at[pl.ds(2 * ff, head), :]))[i]
        return pltpu.make_async_copy(src, dst, w_l.at[i])

    def wx(k):
        return remote(w_at(k, quarter, None, False), w_at(k, quarter, None, True), wx_s.at[k], wx_r.at[k], pt)

    def wx_in(k):
        ref = w_at(k, quarter, None, True)
        return remote(ref, ref, wx_s.at[k], wx_r.at[k], pt)

    def wf(k, i):
        ref = (w_at(k, quarter, None, True) if i < 2 else w_at(k, q_y, 1, True) if i == 2 else w_at(k, q_z, 0, True))
        return remote(ref, ref, wf_s.at[k, i], wf_r.at[k, i], yd if i in (1, 3) else zd)

    def wf_in(k, i):
        ref = w_at(k, (q_z, q_y, q_zy, q_zy)[i], (None, None, 1, 0)[i], True)
        return remote(ref, ref, wf_s.at[k, i], wf_r.at[k, i], yd if i in (1, 3) else zd)

    def pass_quarter(k):
        wx_in(k).wait_recv()
        wf(k, 0).start()
        wf(k, 1).start()

    def pass_halves(k):
        wf_in(k, 0).wait_recv()
        wf_in(k, 1).wait_recv()
        wf(k, 2).start()
        wf(k, 3).start()

    def have(k):
        wf_in(k, 2).wait_recv()
        wf_in(k, 3).wait_recv()

    def own_seq(s):
        return 2 * s + pair

    def other_seq(s):
        return 2 * s + 1 - pair

    def n_own(s):
        return ng.at[s, pl.ds(row(c, j), rows)]

    def nm(s, h):
        ref = ng.at[s, pl.ds(row(c, j, h * half), half)]
        return remote(ref, ref, nm_s.at[s, h], nm_r.at[s, h], mt)

    def nm_in(s, h):
        ref = ng.at[s, pl.ds(row(mate, j, h * half), half)]
        return remote(ref, ref, nm_s.at[s, h], nm_r.at[s, h], mt)

    def np_(s, h):
        return remote(nout.at[s, pl.ds(h * half, half)], ng.at[s, pl.ds(row(c, j, h * half), half)],
                      np_s.at[s, h], np_r.at[s, h], pt)

    def np_in(s, h):
        ref = ng.at[s, pl.ds(row(part, j, h * half), half)]
        return remote(ref, ref, np_s.at[s, h], np_r.at[s, h], pt)

    def nf(s, h):
        ref = ng.at[s, pl.ds(row(part, j, h * half), half)]
        return remote(ref, ref, nf_s.at[s, h], nf_r.at[s, h], mt)

    def nf_in(s, h):
        ref = ng.at[s, pl.ds(row(far, j, h * half), half)]
        return remote(ref, ref, nf_s.at[s, h], nf_r.at[s, h], mt)

    def nd(s, i, core=j):
        ref = (ng.at[s, pl.ds(row(c if i == 0 else mate, core), rows)] if i < 2 else
               ng.at[s, pl.ds(row(part if i < 4 else far, core, (i % 2) * half), half)])
        return remote(ref, ref, nd_s.at[s, i], nd_r.at[s, i], sib)

    def nd_in(s, i):
        return nd(s, i, o)

    def relay_mate(s):
        for h in range(2):
            nm_in(s, h).wait_recv()
        nd(s, 1).start()

    def relay_part(s, h):
        np_in(s, h).wait_recv()
        nf(s, h).start()
        nd(s, 2 + h).start()

    def relay_far(s):
        for h in range(2):
            nf_in(s, h).wait_recv()
            nd(s, 4 + h).start()

    def ln_buf(b):
        return (xt if b < 4 else nt).at[(b // 2) % 2, pl.ds((b % 2) * rows, rows)]

    def ln_load(b):
        return pltpu.make_async_copy(x.at[own_seq(b // 2) if b % 2 else other_seq(b // 2)], ln_buf(b), ln_sem.at[b])

    def ln_store(b):
        return pltpu.make_async_copy(ln_buf(b), n_own(b // 2) if b % 2 else nout.at[b // 2], ln_sem.at[b])

    def normalise(b):
        ln_load(b).wait()
        buf = ln_buf(b)

        def norm(r, _):
            rr = pl.ds(pl.multiple_of(r * ln_rows, ln_rows), ln_rows)
            v = buf[rr, :].astype(F32)
            mean = jnp.mean(v, axis=-1, keepdims=True)
            cen = v - mean
            var = jnp.mean(cen * cen, axis=-1, keepdims=True)
            buf[rr, :] = (cen * lax.rsqrt(var + LN_EPS) * gain[...] + bias[...]).astype(BF16)
            return 0

        lax.fori_loop(0, rows // ln_rows, norm, 0)
        ln_store(b).start()

    barrier = pltpu.get_barrier_semaphore()
    for to in (sib, mt, pt, zd, yd):
        pl.semaphore_signal(barrier, inc=1, device_id=to, device_id_type=MESH)
    for b in range(6):
        ln_load(b).start()
    pl.semaphore_wait(barrier, 5)

    first = next(i for i, name in enumerate(INTER) if name[0] == "p")
    for name in INTER[:first]:
        wx(PIECE[name]).start()
    normalise(0)
    normalise(1)
    begun = set()
    for name in INTER[first:]:
        if name[0] != "p":
            wx(PIECE[name]).start()
            continue
        s, h = int(name[1]), int(name[2])
        if s not in begun:
            if s > 0:
                normalise(2 * s)
                normalise(2 * s + 1)
            ln_store(2 * s).wait()
        np_(s, h).start()
        if s == 0 and s not in begun:
            ln_store(1).wait()
            nm(0, 0).start()
            nm(0, 1).start()
            nd(0, 0).start()
        begun.add(s)
    for s in (1, 2):
        ln_store(2 * s + 1).wait()
        nd(s, 0).start()

    def tile_chip(i):
        return jnp.where(i == 0, c, jnp.where(i == 1, mate, jnp.where(i == 2, part, far)))

    def mlp_chip(kind):
        return jnp.where(kind == FAR, far, jnp.where(kind == MATE, mate, jnp.where(kind == PART, part, c)))

    def tile_copy(s, i):
        return pltpu.make_async_copy(ng.at[s, rowblock(tile_chip(i))], xt.at[lax.rem(i, 2)], xt_sem.at[lax.rem(i, 2)])

    def tile_start(s, i):
        for n in ((0,), (1,), (2, 3), (4, 5))[i]:
            nd_in(s, n).wait_recv()
        tile_copy(s, jnp.int32(i)).start()

    def tile(index):
        s, i = lax.div(index, 4), lax.rem(index, 4)
        tile_copy(s, i).wait()
        slot = lax.rem(i, 2)
        base = rowblock(tile_chip(i))
        for t in range(2):
            qk[base, pl.ds(t * 2 * head, 2 * head)] = jnp.dot(
                xt[slot], wq[t], preferred_element_type=F32).astype(BF16)
        vt[:, base] = jnp.transpose(jnp.dot(xt[slot], wq[2], preferred_element_type=F32)).astype(BF16)

    def dot_t(a, b):
        return lax.dot_general(a, b, (((1,), (1,)), ((), ())), preferred_element_type=F32)

    def o_out(s, i):
        return pltpu.make_async_copy(ot.at[lax.rem(i, 2)], obuf.at[s, rowblock(i)], oo_sem.at[lax.rem(i, 2)])

    def attend(index):
        s, i = lax.div(index, 4), lax.rem(index, 4)
        slot = lax.rem(i, 2)

        @pl.when(i >= 2)
        def _():
            o_out(s, i).wait()

        mine = rowblock(i)
        causal = (lax.broadcasted_iota(jnp.int32, (blk, blk), 0)
                  <= lax.broadcasted_iota(jnp.int32, (blk, blk), 1))
        for h in range(2):
            hd = pl.ds(h * head, head)
            sc = jnp.where(causal, dot_t(qk[mine, pl.ds((2 + h) * head, head)], qk[mine, hd]), -jnp.inf)
            top = jnp.max(sc, axis=0, keepdims=True)
            p = jnp.exp2((sc - top) * scale)
            m_s[h] = top
            l_s[h] = jnp.sum(p, axis=0, keepdims=True)
            acc[h] = jnp.dot(vt[hd, mine], p.astype(BF16), preferred_element_type=F32)

        def earlier(t, _):
            there = rowblock(t)
            for h in range(2):
                hd = pl.ds(h * head, head)
                sc = dot_t(qk[there, pl.ds((2 + h) * head, head)], qk[mine, hd])
                old = m_s[h]
                top = jnp.maximum(old, jnp.max(sc, axis=0, keepdims=True))
                p = jnp.exp2((sc - top) * scale)
                fade = jnp.exp2((old - top) * scale)
                m_s[h] = top
                l_s[h] = l_s[h] * fade + jnp.sum(p, axis=0, keepdims=True)
                acc[h] = acc[h] * fade + jnp.dot(vt[hd, there], p.astype(BF16), preferred_element_type=F32)
            return 0

        lax.fori_loop(0, i, earlier, 0)
        for h in range(2):
            ot[slot, :, pl.ds(h * head, head)] = jnp.transpose(acc[h] * (1.0 / l_s[h])).astype(BF16)
        o_out(s, i).start()

    def context_out(s):
        for i in (2, 3):
            o_out(jnp.int32(s), jnp.int32(i)).wait()

    def sp(s, kind, slot):
        return remote(stage.at[slot, pl.ds(pl.multiple_of(o * rows, rows), rows)], sibin.at[s, kind],
                      sp_s.at[s, kind], sp_r.at[s, kind], sib)

    def own_store(s, kind, slot):
        return pltpu.make_async_copy(stage.at[slot, pl.ds(pl.multiple_of(j * rows, rows), rows)], ownp.at[s, kind],
                                     op_sem.at[slot])

    def to_mate(s, kind):
        return remote(tbuf.at[kind], mid.at[s, kind], t_s.at[s, kind], t_r.at[s, kind], mt)

    def from_mate(s, kind):
        return remote(mid.at[s, kind], mid.at[s, kind], t_s.at[s, kind], t_r.at[s, kind], mt)

    def to_part(s):
        return remote(tbuf.at[PART], branch.at[own_seq(s)], p_s.at[s], p_r.at[s], pt)

    def from_part(s):
        return remote(branch.at[other_seq(s)], branch.at[other_seq(s)], p_s.at[s], p_r.at[s], pt)

    def keep(s):
        return pltpu.make_async_copy(tbuf.at[OWN], branch.at[own_seq(s)], br_sem)

    def sent(s, kind):
        if kind < PART:
            to_mate(s, kind).wait_send()
        elif kind == PART:
            to_part(s).wait_send()
        else:
            keep(s).wait()

    def add_now(name):
        s, kind = jnp.int32(int(name[0])), BLOCKS.index(name[1])
        add_start(s, kind, jnp.int32(BEFORE_SUM[name]))
        add_finish(s, kind)

    def add_loads(s, kind):
        srcs = [ownp.at[s, kind], sibin.at[s, kind]] + ([mid.at[s, kind - PART]] if kind >= PART else [])
        return [pltpu.make_async_copy(src, cin.at[n], cl_sem.at[n]) for n, src in enumerate(srcs)]

    def add_start(s, kind, before):
        remote(sibin.at[s, kind], sibin.at[s, kind], sp_s.at[s, kind], sp_r.at[s, kind], sib).wait_recv()
        if kind >= PART:
            from_mate(s, kind - PART).wait_recv()

        @pl.when(before >= 0)
        def _():
            sent(before, kind)

        for ld in add_loads(s, kind):
            ld.start()

    def add_finish(s, kind):
        for ld in add_loads(s, kind):
            ld.wait()

        def add(r, _):
            rr = pl.ds(pl.multiple_of(r * add_rows, add_rows), add_rows)
            if kind < PART:
                tbuf[kind, rr, :] = cin[0, rr, :] + cin[1, rr, :]
            else:
                tbuf[kind, rr, :] = (cin[0, rr, :].astype(F32) + cin[1, rr, :].astype(F32)
                                     + cin[2, rr, :].astype(F32)).astype(BF16)
            return 0

        lax.fori_loop(0, rows // add_rows, add, 0)
        if kind < PART:
            to_mate(s, kind).start()
        elif kind == PART:
            to_part(s).start()
        else:
            keep(s).start()

    def item(k):
        both = pick([4 * s + b for s, b in ITEMS], k, 4)
        return lax.div(both, 4), lax.rem(both, 4)

    def n_load(k):
        s, kind = item(k)
        return pltpu.make_async_copy(ng.at[s, rowblock(mlp_chip(kind))], nt.at[lax.rem(k, 2)], nl_sem.at[lax.rem(k, 2)])

    def o_load(k):
        s, kind = item(k)
        return pltpu.make_async_copy(obuf.at[s, rowblock(mlp_chip(kind))],
                                     ho.at[lax.rem(k, SLOTS), :, pl.ds(2 * ff, 2 * head)], ol_sem.at[lax.rem(k, SLOTS)])

    def mlp_up(k):
        n_load(k).wait()

        @pl.when(k == 0)
        def _():
            have(UP0)
            have(UP1)
            w_own(1).wait()

        src, dst = lax.rem(k, 2), lax.rem(k, SLOTS)

        def up(t, _):
            cols = pl.ds(pl.multiple_of(t * chunk, chunk), chunk)
            hid = jnp.dot(nt[src], wu[:, cols], preferred_element_type=F32)
            ho[dst, :, cols] = (0.5 * hid * (1.0 + lax.erf(hid * 0.7071067811865476))).astype(BF16)
            return 0

        lax.fori_loop(0, 2 * ff // chunk, up, 0, unroll=True)

    def stage_free(k):
        s, kind = item(k)
        sp(s, kind, lax.rem(k, 2)).wait_send()

    def own_stored(k):
        s, kind = item(k)
        own_store(s, kind, lax.rem(k, 2)).wait()

    def mlp_down(k):
        s, kind = item(k)
        slot, src = lax.rem(k, 2), lax.rem(k, SLOTS)
        o_load(k).wait()

        @pl.when(k == 0)
        def _():
            for p in range(DN0, OUT + 1):
                have(p)
            w_own(2).wait()
            w_own(3).wait()

        @pl.when(k >= 2)
        def _():
            stage_free(k - 2)

        def down(r, size):
            def one(t, _):
                cols = pl.ds(pl.multiple_of(t * chunk, chunk), chunk)
                stage[slot, pl.ds(r, size), cols] = jnp.dot(
                    ho[src, pl.ds(r, size), :], wd[:, cols], preferred_element_type=F32).astype(BF16)
                return 0

            lax.fori_loop(0, d_model // chunk, one, 0, unroll=True)

        split = (k == 0) | (k == len(ITEMS) - 1)

        @pl.when(jnp.logical_not(split))
        def _():
            down(0, blk)
            sp(s, kind, slot).start()

        @pl.when(split)
        def _():
            def part_of(p, _):
                down(pl.multiple_of(jnp.where(p == 0, o, j) * rows, rows), rows)

                @pl.when(p == 0)
                def _():
                    sp(s, kind, slot).start()

                return 0

            lax.fori_loop(0, 2, part_of, 0)

        own_store(s, kind, slot).start()

    def act(name):
        what, arg = name[:2], name[2:]
        if what == "pq":
            pass_quarter(PIECE[arg])
        elif what == "ph":
            pass_halves(PIECE[arg])
        elif what == "rm":
            relay_mate(int(arg))
        elif what == "rp":
            relay_part(int(arg[0]), int(arg[1]))
        elif what == "rf":
            relay_far(int(arg))
        elif what == "ld":
            tile_start(int(arg[0]), int(arg[1]))
        elif what == "nm":
            nm(int(arg[0]), int(arg[1])).start()
        elif what == "ad":
            add_now(arg)
        elif what == "ow":
            context_out(int(arg))
        elif what == "ln":
            n_load(jnp.int32(int(arg))).start()
        else:
            o_load(jnp.int32(int(arg))).start()

    for i in range(4):
        w_own(i).start()
    for name in START:
        act(name)
    w_own(0).wait()
    for k in (W_Q, W_K, W_V):
        have(k)

    codes = [code_of(step) for step in ORDER]

    def add_code(name):
        return 1 + 4 * int(name[0]) + BLOCKS.index(name[1]) + 12 * (1 + BEFORE_SUM[name])

    adds = [add_code(ADDS[t]) if t in ADDS else 0 for t in range(len(ORDER))]

    def adding(code, do):
        @pl.when(code > 0)
        def _():
            which = lax.rem(code - 1, 12)
            for kind in range(4):
                @pl.when(lax.rem(which, 4) == kind)
                def _(kind=kind):
                    do(lax.div(which, 4), kind, lax.div(code - 1, 12) - 1)

    def events(t, lo, size):
        if not any(p in BEFORE for p in range(lo, lo + size)):
            return
        if size == 1:
            for name in BEFORE[lo]:
                act(name)
            return
        size //= 4
        for q in range(lo, lo + 4 * size, size):
            @pl.when(lax.div(t, size) == q // size)
            def _(q=q):
                events(t, q, size)

    def run(t, before):
        events(t, 0, 64)
        code, add = pick(codes, t, 6), pick(adds, t, 6)
        adding(add, add_start)
        what, index = lax.div(code, 16), lax.rem(code, 16)
        for kind, body in ((TILE, tile), (ATT, attend), (UP, mlp_up), (DOWN, mlp_down)):
            @pl.when(what == kind)
            def _(body=body):
                body(index)

        adding(add, lambda s, kind, _: add_finish(s, kind))

        @pl.when(lax.div(before, 16) == DOWN)
        def _():
            own_stored(lax.rem(before, 16))

        return code

    lax.fori_loop(0, len(ORDER), run, jnp.int32(0))
    own_stored(jnp.int32(len(ITEMS) - 1))
    for name in LAST_ADDS:
        add_now(name)
    for k in range(len(ITEMS) - 2, len(ITEMS)):
        stage_free(jnp.int32(k))
    for s in range(3):
        for h in range(2):
            nm(s, h).wait_send()
            np_(s, h).wait_send()
            nf(s, h).wait_send()
        for i in range(6):
            nd(s, i).wait_send()
    for k in range(PIECES):
        wx(k).wait_send()
        for i in range(4):
            wf(k, i).wait_send()
    for s in range(3):
        from_part(s).wait_recv()
    for name, s in LAST_SUM.items():
        sent(s, BLOCKS.index(name))


def residual_kernel(x, branch, y, xv, bv, x_sem, b_sem, y_sem):
    parts, step = xv.shape[0], min(64, xv.shape[1])

    def loads(p):
        return (pltpu.make_async_copy(x.at[p], xv.at[p], x_sem.at[p]),
                pltpu.make_async_copy(branch.at[p], bv.at[p], b_sem.at[p]))

    def store(p):
        return pltpu.make_async_copy(xv.at[p], y.at[p], y_sem.at[p])

    for p in range(parts):
        for ld in loads(p):
            ld.start()

    def add(p, _):
        for ld in loads(p):
            ld.wait()
        for r in range(0, xv.shape[1], step):
            rr = pl.ds(r, step)
            xv[p, rr, :] = (xv[p, rr, :].astype(F32) + bv[p, rr, :].astype(F32)).astype(BF16)
        store(p).start()
        return 0

    lax.fori_loop(0, parts, add, 0)
    for p in range(parts):
        store(p).wait()


def neighbour_span(groups):
    short = 1
    while short * short * 4 <= groups:
        short *= 2
    return groups // short


def solution(mesh):
    tp, groups = mesh.shape["tp"], mesh.shape["dp"]
    span = neighbour_span(groups)
    assert tp == 8 and groups % (2 * span) == 0 and span % 2 == 0

    def local_layer(x_blk, ln_gain, ln_bias, w_qkv, w_out, w_up, w_down):
        n_seq, rows, d_model = x_blk.shape
        head = w_qkv.shape[3]
        ff = w_up.shape[1]
        ns, seq, blk = n_seq // 2, rows * tp, 2 * rows
        assert ns == 3 and w_qkv.shape[1:3] == (1, 3)
        chunk = min(512, d_model, ff)
        ln_rows, add_rows = min(64, rows // 2), min(16, rows // 2)
        dims = (span, rows, d_model, head, ff, chunk, ln_rows, add_rows)
        dma = pltpu.SemaphoreType.DMA
        anyspace = pl.BlockSpec(memory_space=pl.ANY)
        vmem = pl.BlockSpec(memory_space=pltpu.VMEM)

        def hbm(*shape):
            return jax.ShapeDtypeStruct(shape, BF16)

        outs = pl.pallas_call(
            functools.partial(layer_kernel, dims),
            name="layer",
            out_shape=(hbm(n_seq, rows, d_model), hbm(ns, seq, d_model), hbm(ns, rows, d_model), hbm(ns, seq, 2 * head),
                       hbm(ns, 4, rows, d_model), hbm(ns, 4, rows, d_model), hbm(ns, 2, rows, d_model)),
            in_specs=[anyspace, vmem, vmem, anyspace, anyspace, anyspace, anyspace],
            out_specs=(anyspace,) * 7,
            scratch_shapes=[
                pltpu.VMEM((3, d_model, 2 * head), BF16),
                pltpu.VMEM((d_model, 2 * ff), BF16),
                pltpu.VMEM((2 * ff + 2 * head, d_model), BF16),
                pltpu.VMEM((2, blk, d_model), BF16),
                pltpu.VMEM((2, blk, d_model), BF16),
                pltpu.VMEM((seq, 4 * head), BF16),
                pltpu.VMEM((2 * head, seq), BF16),
                pltpu.VMEM((2, blk, 2 * head), BF16),
                pltpu.VMEM((SLOTS, blk, 2 * ff + 2 * head), BF16),
                pltpu.VMEM((2, blk, d_model), BF16),
                pltpu.VMEM((3, rows, d_model), BF16),
                pltpu.VMEM((4, rows, d_model), BF16),
                pltpu.VMEM((2, head, blk), F32),
                pltpu.VMEM((2, 1, blk), F32),
                pltpu.VMEM((2, 1, blk), F32),
                dma((4,)), dma((PIECES,)), dma((PIECES,)), dma((PIECES, 4)), dma((PIECES, 4)),
                dma((ns, 2)), dma((ns, 2)), dma((ns, 2)), dma((ns, 2)), dma((ns, 2)), dma((ns, 2)),
                dma((ns, 6)), dma((ns, 6)),
                dma((ns, 4)), dma((ns, 4)), dma((2,)), dma((ns, 2)), dma((ns, 2)), dma((ns,)), dma((ns,)),
                dma((6,)), dma((2,)), dma((2,)), dma((2,)), dma((SLOTS,)), dma((3,)), dma,
            ],
            compiler_params=pltpu.CompilerParams(
                collective_id=0, has_side_effects=True, vmem_limit_bytes=VMEM_LIMIT),
        )(x_blk, ln_gain.reshape(1, d_model), ln_bias.reshape(1, d_model),
          jnp.transpose(w_qkv[:, 0], (1, 0, 2)), w_out, w_up, w_down)
        cut = (4 * n_seq, rows // 4, d_model)
        y = pl.pallas_call(
            residual_kernel, name="residual", in_specs=[anyspace, anyspace], out_specs=anyspace,
            out_shape=hbm(*cut),
            scratch_shapes=[pltpu.VMEM(cut, BF16), pltpu.VMEM(cut, BF16), dma(cut[:1]), dma(cut[:1]), dma(cut[:1])],
            compiler_params=pltpu.CompilerParams(vmem_limit_bytes=VMEM_LIMIT),
        )(x_blk.reshape(cut), outs[0].reshape(cut))
        return y.reshape(n_seq, rows, d_model)

    return jax.shard_map(
        local_layer, mesh=mesh,
        in_specs=(P("dp", "tp", None), P(), P(), P(None, "tp", None, None),
                  P("tp", None), P(None, "tp"), P("tp", None)),
        out_specs=P("dp", "tp", None), check_vma=False)
```

```python
import functools

import jax
import jax.numpy as jnp
from jax import lax
from jax.experimental import pallas as pl
from jax.experimental.pallas import tpu as pltpu
from jax.sharding import PartitionSpec as P

LN_EPS = 1e-5
MESH = pl.DeviceIdType.MESH
BF16 = jnp.bfloat16
F32 = jnp.float32
LOG2E = 1.4426950408889634
VMEM_LIMIT = 67_043_328

W_Q, W_K, W_V, UP0, UP1, DN0, DN1, DN2, DN3, OUT = range(10)
PIECES = 10
FAR, MATE, PART, OWN = range(4)
TILE, ATT, UP, DOWN = range(4)
INTER = ("Q2", "Q1", "Q0", "p01", "p00", "U0", "U1", "D2", "p11", "p10", "D0", "O", "D1", "D3", "p20", "p21")
ORDER = ("A00", "A01", "A02", "A03", "T00", "T01", "T02", "T03", "A10", "A11", "U0F", "U1M",
         "U0M", "A12", "A13", "T10", "T11", "T12", "T13", "A20", "D0F", "A21", "D1M", "U1F",
         "D0M", "A22", "U0P", "D1F", "A23", "T20", "D0P", "T21", "T22", "T23", "U2F", "D2F",
         "U1P", "D1P", "U2M", "D2M", "U2P", "U1O", "D2P", "D1O", "U0O", "D0O", "U2O", "D2O",
         )
START = ("pqQ2", "pqQ1", "phQ2", "pqQ0", "phQ1", "rm0", "nm10", "phQ0", "rp01")
BEFORE = {
    0: ("ld00", "ld01"),
    2: ("rp00", "ld02"),
    3: ("pqU0", "rf0", "nm11", "pqU1", "ld03", "ln0"),
    4: ("phU0", "pqD2"),
    5: ("nm20",),
    6: ("rm1",),
    7: ("phU1", "ld10"),
    8: ("rp11", "ld11"),
    10: ("phD2", "rp10", "ln1", "ow0", "lo0"),
    11: ("pqD0", "ln2"),
    12: ("pqO", "ld12", "lo2"),
    13: ("phD0", "pqD1", "rf1", "nm21"),
    14: ("ld13", "ln3"),
    15: ("pqD3", "phO"),
    18: ("phD1", "rm2", "rp20", "ld20"),
    19: ("phD3", "ow1", "lo1"),
    20: ("rp21", "ld21"),
    22: ("ad0F",),
    23: ("rf2", "ln4", "lo3"),
    24: ("ld22",),
    26: ("lo4",),
    27: ("ld23",),
    28: ("ln5",),
    34: ("ln6", "ow2", "lo5"),
    36: ("ln7", "lo6"),
    38: ("ln8", "lo7"),
    40: ("ln9", "lo8"),
    41: ("ln10", "lo9"),
    44: ("ln11", "lo10"),
    46: ("lo11",),
}
ADDS = { 24: "1M", 29: "1F", 32: "0P", 33: "0M", 37: "2F", 39: "1P", 41: "2M", 44: "2P", 45: "1O", 47: "0O" }
LAST_ADDS = ("2O",)

KINDS = "ATUD"
BLOCKS = "FMPO"
ITEMS = tuple((int(x[1]), BLOCKS.index(x[2])) for x in ORDER if x[0] == "U")
SLOTS = 4
PIECE = {"Q0": W_Q, "Q1": W_K, "Q2": W_V, "U0": UP0, "U1": UP1,
         "D0": DN0, "D1": DN1, "D2": DN2, "D3": DN3, "O": OUT}


def code_of(step):
    what, s = KINDS.index(step[0]), int(step[1])
    return 16 * what + (4 * s + int(step[2]) if what < UP else ITEMS.index((s, BLOCKS.index(step[2]))))


def pick(values, i, bits):
    per = 30 // bits
    words = [sum(v << bits * p for p, v in enumerate(values[w:w + per])) for w in range(0, len(values), per)]
    word, at = lax.div(i, per), lax.rem(i, per)
    packed = jnp.int32(words[0])
    for w in range(1, len(words)):
        packed = jnp.where(word == w, words[w], packed)
    out = packed
    for p in range(1, per):
        out = jnp.where(at == p, lax.div(packed, 1 << bits * p), out)
    return lax.rem(out, 1 << bits)


def sums():
    seq = []
    for t in range(len(ORDER)):
        seq += [(name[2:], t) for name in BEFORE.get(t, ()) if name[:2] == "ad"]
        if t in ADDS:
            seq.append((ADDS[t], t))
    last, before = {}, {}
    for name, _ in seq:
        before[name] = last.get(name[1], -1)
        last[name[1]] = int(name[0])
    assert len(seq) == len(ITEMS) - 1 and LAST_ADDS == ("2O",)
    return before, last


BEFORE_SUM, LAST_SUM = sums()


def layer_kernel(dims, x, gain, bias, w_qkv, w_out, w_up, w_dn,
                 branch, ng, nout, obuf, ownp, sibin, mid,
                 wq, wu, wd, xt, nt, qk, vt, ot, ho, stage, cin, tbuf, acc, m_s, l_s,
                 w_l, wx_s, wx_r, wf_s, wf_r, nm_s, nm_r, np_s, np_r, nf_s, nf_r, nd_s, nd_r,
                 sp_s, sp_r, op_sem, t_s, t_r, p_s, p_r,
                 ln_sem, xt_sem, oo_sem, nl_sem, ol_sem, cl_sem, br_sem):
    span, rows, d_model, head, ff, chunk, ln_rows, add_rows = dims
    half = rows // 2
    blk = 2 * rows
    scale = LOG2E * head ** -0.5

    g, me = lax.axis_index("dp"), lax.axis_index("tp")
    c, j = lax.div(me, 2), lax.rem(me, 2)
    o = 1 - j
    pair = lax.div(c, 2)
    mate = c + 1 - 2 * lax.rem(c, 2)
    part = 3 - c
    far = 3 - mate
    zb, yb = lax.rem(g, 2), lax.rem(lax.div(g, span), 2)
    gz, gy = g + 1 - 2 * zb, g + span * (1 - 2 * yb)

    def dev(chip, core, group=g):
        return {"dp": group, "tp": 2 * chip + core}

    sib, mt, pt, zd, yd = dev(c, o), dev(mate, j), dev(part, j), dev(c, j, gz), dev(c, j, gy)

    def remote(src, dst, send, recv, to):
        return pltpu.make_async_remote_copy(src_ref=src, dst_ref=dst, send_sem=send, recv_sem=recv,
                                            device_id=to, device_id_type=MESH)

    def row(chip, core, extra=0):
        return pl.multiple_of((2 * chip + core) * rows + extra, half)

    def rowblock(chip):
        return pl.ds(pl.multiple_of(chip * blk, blk), blk)

    quarter = 2 * yb + zb
    q_z, q_y, q_zy = quarter + 1 - 2 * zb, quarter + 2 - 4 * yb, 3 - quarter

    def w_at(piece, q, side, hold):
        n = head // 4 if piece == OUT else ff // 16 if piece >= DN0 else d_model // 8 if piece >= UP0 else d_model // 4
        size = n if side is None else n // 2
        off = q * n + (0 if side is None else side * size)
        if UP0 <= piece <= DN3:
            off = off + (piece - (UP0 if piece <= UP1 else DN0)) * 4 * n
        if hold and DN0 <= piece <= DN3:
            off = off + ff
        if hold and piece == OUT:
            off = off + 2 * ff + head
        at = pl.ds(pl.multiple_of(off, n // 2), size)
        if piece <= W_V:
            return wq.at[piece, at, pl.ds(head, head)] if hold else w_qkv.at[piece, at, :]
        if piece <= UP1:
            return wu.at[at, pl.ds(ff, ff)] if hold else w_up.at[at, :]
        return wd.at[at, :] if hold else (w_out if piece == OUT else w_dn).at[at, :]

    def w_own(i):
        src, dst = ((w_qkv, wq.at[:, :, pl.ds(0, head)]), (w_up, wu.at[:, pl.ds(0, ff)]),
                    (w_dn, wd.at[pl.ds(0, ff), :]), (w_out, wd.at[pl.ds(2 * ff, head), :]))[i]
        return pltpu.make_async_copy(src, dst, w_l.at[i])

    def wx(k):
        return remote(w_at(k, quarter, None, False), w_at(k, quarter, None, True), wx_s.at[k], wx_r.at[k], pt)

    def wx_in(k):
        ref = w_at(k, quarter, None, True)
        return remote(ref, ref, wx_s.at[k], wx_r.at[k], pt)

    def wf(k, i):
        ref = (w_at(k, quarter, None, True) if i < 2 else w_at(k, q_y, 1, True) if i == 2 else w_at(k, q_z, 0, True))
        return remote(ref, ref, wf_s.at[k, i], wf_r.at[k, i], yd if i in (1, 3) else zd)

    def wf_in(k, i):
        ref = w_at(k, (q_z, q_y, q_zy, q_zy)[i], (None, None, 1, 0)[i], True)
        return remote(ref, ref, wf_s.at[k, i], wf_r.at[k, i], yd if i in (1, 3) else zd)

    def pass_quarter(k):
        wx_in(k).wait_recv()
        wf(k, 0).start()
        wf(k, 1).start()

    def pass_halves(k):
        wf_in(k, 0).wait_recv()
        wf_in(k, 1).wait_recv()
        wf(k, 2).start()
        wf(k, 3).start()

    def have(k):
        wf_in(k, 2).wait_recv()
        wf_in(k, 3).wait_recv()

    def own_seq(s):
        return 2 * s + pair

    def other_seq(s):
        return 2 * s + 1 - pair

    def n_own(s):
        return ng.at[s, pl.ds(row(c, j), rows)]

    def nm(s, h):
        ref = ng.at[s, pl.ds(row(c, j, h * half), half)]
        return remote(ref, ref, nm_s.at[s, h], nm_r.at[s, h], mt)

    def nm_in(s, h):
        ref = ng.at[s, pl.ds(row(mate, j, h * half), half)]
        return remote(ref, ref, nm_s.at[s, h], nm_r.at[s, h], mt)

    def np_(s, h):
        return remote(nout.at[s, pl.ds(h * half, half)], ng.at[s, pl.ds(row(c, j, h * half), half)],
                      np_s.at[s, h], np_r.at[s, h], pt)

    def np_in(s, h):
        ref = ng.at[s, pl.ds(row(part, j, h * half), half)]
        return remote(ref, ref, np_s.at[s, h], np_r.at[s, h], pt)

    def nf(s, h):
        ref = ng.at[s, pl.ds(row(part, j, h * half), half)]
        return remote(ref, ref, nf_s.at[s, h], nf_r.at[s, h], mt)

    def nf_in(s, h):
        ref = ng.at[s, pl.ds(row(far, j, h * half), half)]
        return remote(ref, ref, nf_s.at[s, h], nf_r.at[s, h], mt)

    def nd(s, i, core=j):
        ref = (ng.at[s, pl.ds(row(c if i == 0 else mate, core), rows)] if i < 2 else
               ng.at[s, pl.ds(row(part if i < 4 else far, core, (i % 2) * half), half)])
        return remote(ref, ref, nd_s.at[s, i], nd_r.at[s, i], sib)

    def nd_in(s, i):
        return nd(s, i, o)

    def relay_mate(s):
        for h in range(2):
            nm_in(s, h).wait_recv()
        nd(s, 1).start()

    def relay_part(s, h):
        np_in(s, h).wait_recv()
        nf(s, h).start()
        nd(s, 2 + h).start()

    def relay_far(s):
        for h in range(2):
            nf_in(s, h).wait_recv()
            nd(s, 4 + h).start()

    def ln_buf(b):
        return (xt if b < 4 else nt).at[(b // 2) % 2, pl.ds((b % 2) * rows, rows)]

    def ln_load(b):
        return pltpu.make_async_copy(x.at[own_seq(b // 2) if b % 2 else other_seq(b // 2)], ln_buf(b), ln_sem.at[b])

    def ln_store(b):
        return pltpu.make_async_copy(ln_buf(b), n_own(b // 2) if b % 2 else nout.at[b // 2], ln_sem.at[b])

    def normalise(b):
        ln_load(b).wait()
        buf = ln_buf(b)

        def norm(r, _):
            rr = pl.ds(pl.multiple_of(r * ln_rows, ln_rows), ln_rows)
            v = buf[rr, :].astype(F32)
            mean = jnp.mean(v, axis=-1, keepdims=True)
            cen = v - mean
            var = jnp.mean(cen * cen, axis=-1, keepdims=True)
            buf[rr, :] = (cen * lax.rsqrt(var + LN_EPS) * gain[...] + bias[...]).astype(BF16)
            return 0

        lax.fori_loop(0, rows // ln_rows, norm, 0)
        ln_store(b).start()

    barrier = pltpu.get_barrier_semaphore()
    for to in (sib, mt, pt, zd, yd):
        pl.semaphore_signal(barrier, inc=1, device_id=to, device_id_type=MESH)
    for b in range(6):
        ln_load(b).start()
    pl.semaphore_wait(barrier, 5)

    first = next(i for i, name in enumerate(INTER) if name[0] == "p")
    for name in INTER[:first]:
        wx(PIECE[name]).start()
    normalise(0)
    normalise(1)
    begun = set()
    for name in INTER[first:]:
        if name[0] != "p":
            wx(PIECE[name]).start()
            continue
        s, h = int(name[1]), int(name[2])
        if s not in begun:
            if s > 0:
                normalise(2 * s)
                normalise(2 * s + 1)
            ln_store(2 * s).wait()
        np_(s, h).start()
        if s == 0 and s not in begun:
            ln_store(1).wait()
            nm(0, 0).start()
            nm(0, 1).start()
            nd(0, 0).start()
        begun.add(s)
    for s in (1, 2):
        ln_store(2 * s + 1).wait()
        nd(s, 0).start()

    def tile_chip(i):
        return jnp.where(i == 0, c, jnp.where(i == 1, mate, jnp.where(i == 2, part, far)))

    def mlp_chip(kind):
        return jnp.where(kind == FAR, far, jnp.where(kind == MATE, mate, jnp.where(kind == PART, part, c)))

    def tile_copy(s, i):
        return pltpu.make_async_copy(ng.at[s, rowblock(tile_chip(i))], xt.at[lax.rem(i, 2)], xt_sem.at[lax.rem(i, 2)])

    def tile_start(s, i):
        for n in ((0,), (1,), (2, 3), (4, 5))[i]:
            nd_in(s, n).wait_recv()
        tile_copy(s, jnp.int32(i)).start()

    def tile(index):
        s, i = lax.div(index, 4), lax.rem(index, 4)
        tile_copy(s, i).wait()
        slot = lax.rem(i, 2)
        base = rowblock(tile_chip(i))
        for t in range(2):
            qk[base, pl.ds(t * 2 * head, 2 * head)] = jnp.dot(
                xt[slot], wq[t], preferred_element_type=F32).astype(BF16)
        vt[:, base] = jnp.transpose(jnp.dot(xt[slot], wq[2], preferred_element_type=F32)).astype(BF16)

    def dot_t(a, b):
        return lax.dot_general(a, b, (((1,), (1,)), ((), ())), preferred_element_type=F32)

    def o_out(s, i):
        return pltpu.make_async_copy(ot.at[lax.rem(i, 2)], obuf.at[s, rowblock(i)], oo_sem.at[lax.rem(i, 2)])

    def attend(index):
        s, i = lax.div(index, 4), lax.rem(index, 4)
        slot = lax.rem(i, 2)

        @pl.when(i >= 2)
        def _():
            o_out(s, i).wait()

        mine = rowblock(i)
        causal = (lax.broadcasted_iota(jnp.int32, (blk, blk), 0)
                  <= lax.broadcasted_iota(jnp.int32, (blk, blk), 1))
        for h in range(2):
            hd = pl.ds(h * head, head)
            sc = jnp.where(causal, dot_t(qk[mine, pl.ds((2 + h) * head, head)], qk[mine, hd]), -jnp.inf)
            top = jnp.max(sc, axis=0, keepdims=True)
            p = jnp.exp2((sc - top) * scale)
            m_s[h] = top
            l_s[h] = jnp.sum(p, axis=0, keepdims=True)
            acc[h] = jnp.dot(vt[hd, mine], p.astype(BF16), preferred_element_type=F32)

        def earlier(t, _):
            there = rowblock(t)
            for h in range(2):
                hd = pl.ds(h * head, head)
                sc = dot_t(qk[there, pl.ds((2 + h) * head, head)], qk[mine, hd])
                old = m_s[h]
                top = jnp.maximum(old, jnp.max(sc, axis=0, keepdims=True))
                p = jnp.exp2((sc - top) * scale)
                fade = jnp.exp2((old - top) * scale)
                m_s[h] = top
                l_s[h] = l_s[h] * fade + jnp.sum(p, axis=0, keepdims=True)
                acc[h] = acc[h] * fade + jnp.dot(vt[hd, there], p.astype(BF16), preferred_element_type=F32)
            return 0

        lax.fori_loop(0, i, earlier, 0)
        for h in range(2):
            ot[slot, :, pl.ds(h * head, head)] = jnp.transpose(acc[h] * (1.0 / l_s[h])).astype(BF16)
        o_out(s, i).start()

    def context_out(s):
        for i in (2, 3):
            o_out(jnp.int32(s), jnp.int32(i)).wait()

    def sp(s, kind, slot):
        return remote(stage.at[slot, pl.ds(pl.multiple_of(o * rows, rows), rows)], sibin.at[s, kind],
                      sp_s.at[s, kind], sp_r.at[s, kind], sib)

    def own_store(s, kind, slot):
        return pltpu.make_async_copy(stage.at[slot, pl.ds(pl.multiple_of(j * rows, rows), rows)], ownp.at[s, kind],
                                     op_sem.at[slot])

    def to_mate(s, kind):
        return remote(tbuf.at[kind], mid.at[s, kind], t_s.at[s, kind], t_r.at[s, kind], mt)

    def from_mate(s, kind):
        return remote(mid.at[s, kind], mid.at[s, kind], t_s.at[s, kind], t_r.at[s, kind], mt)

    def to_part(s):
        return remote(tbuf.at[PART], branch.at[own_seq(s)], p_s.at[s], p_r.at[s], pt)

    def from_part(s):
        return remote(branch.at[other_seq(s)], branch.at[other_seq(s)], p_s.at[s], p_r.at[s], pt)

    def keep(s):
        return pltpu.make_async_copy(tbuf.at[OWN], branch.at[own_seq(s)], br_sem)

    def sent(s, kind):
        if kind < PART:
            to_mate(s, kind).wait_send()
        elif kind == PART:
            to_part(s).wait_send()
        else:
            keep(s).wait()

    def add_now(name):
        s, kind = jnp.int32(int(name[0])), BLOCKS.index(name[1])
        add_start(s, kind, jnp.int32(BEFORE_SUM[name]))
        add_finish(s, kind)

    def add_loads(s, kind):
        srcs = [ownp.at[s, kind], sibin.at[s, kind]] + ([mid.at[s, kind - PART]] if kind >= PART else [])
        return [pltpu.make_async_copy(src, cin.at[n], cl_sem.at[n]) for n, src in enumerate(srcs)]

    def add_start(s, kind, before):
        remote(sibin.at[s, kind], sibin.at[s, kind], sp_s.at[s, kind], sp_r.at[s, kind], sib).wait_recv()
        if kind >= PART:
            from_mate(s, kind - PART).wait_recv()

        @pl.when(before >= 0)
        def _():
            sent(before, kind)

        for ld in add_loads(s, kind):
            ld.start()

    def add_finish(s, kind):
        for ld in add_loads(s, kind):
            ld.wait()

        def add(r, _):
            rr = pl.ds(pl.multiple_of(r * add_rows, add_rows), add_rows)
            if kind < PART:
                tbuf[kind, rr, :] = cin[0, rr, :] + cin[1, rr, :]
            else:
                tbuf[kind, rr, :] = (cin[0, rr, :].astype(F32) + cin[1, rr, :].astype(F32)
                                     + cin[2, rr, :].astype(F32)).astype(BF16)
            return 0

        lax.fori_loop(0, rows // add_rows, add, 0)
        if kind < PART:
            to_mate(s, kind).start()
        elif kind == PART:
            to_part(s).start()
        else:
            keep(s).start()

    def item(k):
        both = pick([4 * s + b for s, b in ITEMS], k, 4)
        return lax.div(both, 4), lax.rem(both, 4)

    def n_load(k):
        s, kind = item(k)
        return pltpu.make_async_copy(ng.at[s, rowblock(mlp_chip(kind))], nt.at[lax.rem(k, 2)], nl_sem.at[lax.rem(k, 2)])

    def o_load(k):
        s, kind = item(k)
        return pltpu.make_async_copy(obuf.at[s, rowblock(mlp_chip(kind))],
                                     ho.at[lax.rem(k, SLOTS), :, pl.ds(2 * ff, 2 * head)], ol_sem.at[lax.rem(k, SLOTS)])

    def mlp_up(k):
        n_load(k).wait()

        @pl.when(k == 0)
        def _():
            have(UP0)
            have(UP1)
            w_own(1).wait()

        src, dst = lax.rem(k, 2), lax.rem(k, SLOTS)

        def up(t, _):
            cols = pl.ds(pl.multiple_of(t * chunk, chunk), chunk)
            hid = jnp.dot(nt[src], wu[:, cols], preferred_element_type=F32)
            ho[dst, :, cols] = (0.5 * hid * (1.0 + lax.erf(hid * 0.7071067811865476))).astype(BF16)
            return 0

        lax.fori_loop(0, 2 * ff // chunk, up, 0, unroll=True)

    def stage_free(k):
        s, kind = item(k)
        sp(s, kind, lax.rem(k, 2)).wait_send()

    def own_stored(k):
        s, kind = item(k)
        own_store(s, kind, lax.rem(k, 2)).wait()

    def mlp_down(k):
        s, kind = item(k)
        slot, src = lax.rem(k, 2), lax.rem(k, SLOTS)
        o_load(k).wait()

        @pl.when(k == 0)
        def _():
            for p in range(DN0, OUT + 1):
                have(p)
            w_own(2).wait()
            w_own(3).wait()

        @pl.when(k >= 2)
        def _():
            stage_free(k - 2)

        def down(r, size):
            def one(t, _):
                cols = pl.ds(pl.multiple_of(t * chunk, chunk), chunk)
                stage[slot, pl.ds(r, size), cols] = jnp.dot(
                    ho[src, pl.ds(r, size), :], wd[:, cols], preferred_element_type=F32).astype(BF16)
                return 0

            lax.fori_loop(0, d_model // chunk, one, 0, unroll=True)

        split = (k == 0) | (k == len(ITEMS) - 1)

        @pl.when(jnp.logical_not(split))
        def _():
            down(0, blk)
            sp(s, kind, slot).start()

        @pl.when(split)
        def _():
            def part_of(p, _):
                down(pl.multiple_of(jnp.where(p == 0, o, j) * rows, rows), rows)

                @pl.when(p == 0)
                def _():
                    sp(s, kind, slot).start()

                return 0

            lax.fori_loop(0, 2, part_of, 0)

        own_store(s, kind, slot).start()

    def act(name):
        what, arg = name[:2], name[2:]
        if what == "pq":
            pass_quarter(PIECE[arg])
        elif what == "ph":
            pass_halves(PIECE[arg])
        elif what == "rm":
            relay_mate(int(arg))
        elif what == "rp":
            relay_part(int(arg[0]), int(arg[1]))
        elif what == "rf":
            relay_far(int(arg))
        elif what == "ld":
            tile_start(int(arg[0]), int(arg[1]))
        elif what == "nm":
            nm(int(arg[0]), int(arg[1])).start()
        elif what == "ad":
            add_now(arg)
        elif what == "ow":
            context_out(int(arg))
        elif what == "ln":
            n_load(jnp.int32(int(arg))).start()
        else:
            o_load(jnp.int32(int(arg))).start()

    for i in range(4):
        w_own(i).start()
    for name in START:
        act(name)
    w_own(0).wait()
    for k in (W_Q, W_K, W_V):
        have(k)

    codes = [code_of(step) for step in ORDER]

    def add_code(name):
        return 1 + 4 * int(name[0]) + BLOCKS.index(name[1]) + 12 * (1 + BEFORE_SUM[name])

    adds = [add_code(ADDS[t]) if t in ADDS else 0 for t in range(len(ORDER))]

    def adding(code, do):
        @pl.when(code > 0)
        def _():
            which = lax.rem(code - 1, 12)
            for kind in range(4):
                @pl.when(lax.rem(which, 4) == kind)
                def _(kind=kind):
                    do(lax.div(which, 4), kind, lax.div(code - 1, 12) - 1)

    def events(t, lo, size):
        if not any(p in BEFORE for p in range(lo, lo + size)):
            return
        if size == 1:
            for name in BEFORE[lo]:
                act(name)
            return
        size //= 4
        for q in range(lo, lo + 4 * size, size):
            @pl.when(lax.div(t, size) == q // size)
            def _(q=q):
                events(t, q, size)

    def run(t, before):
        events(t, 0, 64)
        code, add = pick(codes, t, 6), pick(adds, t, 6)
        adding(add, add_start)
        what, index = lax.div(code, 16), lax.rem(code, 16)
        for kind, body in ((TILE, tile), (ATT, attend), (UP, mlp_up), (DOWN, mlp_down)):
            @pl.when(what == kind)
            def _(body=body):
                body(index)

        adding(add, lambda s, kind, _: add_finish(s, kind))

        @pl.when(lax.div(before, 16) == DOWN)
        def _():
            own_stored(lax.rem(before, 16))

        return code

    lax.fori_loop(0, len(ORDER), run, jnp.int32(0))
    own_stored(jnp.int32(len(ITEMS) - 1))
    remote(sibin.at[2, OWN], sibin.at[2, OWN], sp_s.at[2, OWN], sp_r.at[2, OWN], sib).wait_recv()
    from_mate(2, MATE).wait_recv()
    for k in range(len(ITEMS) - 2, len(ITEMS)):
        stage_free(jnp.int32(k))
    for s in range(3):
        for h in range(2):
            nm(s, h).wait_send()
            np_(s, h).wait_send()
            nf(s, h).wait_send()
        for i in range(6):
            nd(s, i).wait_send()
    for k in range(PIECES):
        wx(k).wait_send()
        for i in range(4):
            wf(k, i).wait_send()
    for s in range(3):
        from_part(s).wait_recv()
    for name, s in LAST_SUM.items():
        sent(s, BLOCKS.index(name))


def residual_kernel(x, branch, own, other, mate, y, xv, bv, ov, mv, x_sem, b_sem, o_sem, m_sem, y_sem):
    n_seq, cuts, rows, _ = xv.shape
    late = n_seq - 2 + lax.div(lax.axis_index("tp"), 4)

    def at(ref, i):
        return ref.at[pl.ds(pl.multiple_of(i * rows, rows), rows)]

    def load_x(q, i):
        return pltpu.make_async_copy(at(x.at[q], i), xv.at[q, i], x_sem.at[q, i])

    def load_b(q, i):
        return pltpu.make_async_copy(at(branch.at[q], i), bv.at[q, i], b_sem.at[q, i])

    def load_late(i):
        return (pltpu.make_async_copy(at(own.at[2, OWN], i), bv.at[late, i], b_sem.at[late, i]),
                pltpu.make_async_copy(at(other.at[2, OWN], i), ov.at[i], o_sem.at[i]),
                pltpu.make_async_copy(at(mate.at[2, MATE], i), mv.at[i], m_sem.at[i]))

    def store(q, i):
        return pltpu.make_async_copy(xv.at[q, i], at(y.at[q], i), y_sem.at[q, i])

    def start(p, _):
        q, i = lax.div(p, cuts), lax.rem(p, cuts)
        load_x(q, i).start()

        @pl.when(q == late)
        def _():
            for ld in load_late(i):
                ld.start()

        @pl.when(q != late)
        def _():
            load_b(q, i).start()

        return 0

    def add(p, _):
        q, i = lax.div(p, cuts), lax.rem(p, cuts)
        load_x(q, i).wait()

        @pl.when(q == late)
        def _():
            for ld in load_late(i):
                ld.wait()
            total = bv[q, i].astype(F32) + ov[i].astype(F32) + mv[i].astype(F32)
            xv[q, i] = (xv[q, i].astype(F32) + total.astype(BF16).astype(F32)).astype(BF16)

        @pl.when(q != late)
        def _():
            load_b(q, i).wait()
            xv[q, i] = (xv[q, i].astype(F32) + bv[q, i].astype(F32)).astype(BF16)

        store(q, i).start()
        return 0

    def done(p, _):
        store(lax.div(p, cuts), lax.rem(p, cuts)).wait()
        return 0

    for step in (start, add, done):
        lax.fori_loop(0, n_seq * cuts, step, 0)


def neighbour_span(groups):
    short = 1
    while short * short * 4 <= groups:
        short *= 2
    return groups // short


def solution(mesh):
    tp, groups = mesh.shape["tp"], mesh.shape["dp"]
    span = neighbour_span(groups)
    assert tp == 8 and groups % (2 * span) == 0 and span % 2 == 0

    def local_layer(x_blk, ln_gain, ln_bias, w_qkv, w_out, w_up, w_down):
        n_seq, rows, d_model = x_blk.shape
        head = w_qkv.shape[3]
        ff = w_up.shape[1]
        ns, seq, blk = n_seq // 2, rows * tp, 2 * rows
        assert ns == 3 and w_qkv.shape[1:3] == (1, 3)
        chunk = min(512, d_model, ff)
        ln_rows, add_rows = min(64, rows // 2), min(16, rows // 2)
        dims = (span, rows, d_model, head, ff, chunk, ln_rows, add_rows)
        dma = pltpu.SemaphoreType.DMA
        anyspace = pl.BlockSpec(memory_space=pl.ANY)
        vmem = pl.BlockSpec(memory_space=pltpu.VMEM)

        def hbm(*shape):
            return jax.ShapeDtypeStruct(shape, BF16)

        outs = pl.pallas_call(
            functools.partial(layer_kernel, dims),
            name="layer",
            out_shape=(hbm(n_seq, rows, d_model), hbm(ns, seq, d_model), hbm(ns, rows, d_model), hbm(ns, seq, 2 * head),
                       hbm(ns, 4, rows, d_model), hbm(ns, 4, rows, d_model), hbm(ns, 2, rows, d_model)),
            in_specs=[anyspace, vmem, vmem, anyspace, anyspace, anyspace, anyspace],
            out_specs=(anyspace,) * 7,
            scratch_shapes=[
                pltpu.VMEM((3, d_model, 2 * head), BF16),
                pltpu.VMEM((d_model, 2 * ff), BF16),
                pltpu.VMEM((2 * ff + 2 * head, d_model), BF16),
                pltpu.VMEM((2, blk, d_model), BF16),
                pltpu.VMEM((2, blk, d_model), BF16),
                pltpu.VMEM((seq, 4 * head), BF16),
                pltpu.VMEM((2 * head, seq), BF16),
                pltpu.VMEM((2, blk, 2 * head), BF16),
                pltpu.VMEM((SLOTS, blk, 2 * ff + 2 * head), BF16),
                pltpu.VMEM((2, blk, d_model), BF16),
                pltpu.VMEM((3, rows, d_model), BF16),
                pltpu.VMEM((4, rows, d_model), BF16),
                pltpu.VMEM((2, head, blk), F32),
                pltpu.VMEM((2, 1, blk), F32),
                pltpu.VMEM((2, 1, blk), F32),
                dma((4,)), dma((PIECES,)), dma((PIECES,)), dma((PIECES, 4)), dma((PIECES, 4)),
                dma((ns, 2)), dma((ns, 2)), dma((ns, 2)), dma((ns, 2)), dma((ns, 2)), dma((ns, 2)),
                dma((ns, 6)), dma((ns, 6)),
                dma((ns, 4)), dma((ns, 4)), dma((2,)), dma((ns, 2)), dma((ns, 2)), dma((ns,)), dma((ns,)),
                dma((6,)), dma((2,)), dma((2,)), dma((2,)), dma((SLOTS,)), dma((3,)), dma,
            ],
            compiler_params=pltpu.CompilerParams(
                collective_id=0, has_side_effects=True, vmem_limit_bytes=VMEM_LIMIT),
        )(x_blk, ln_gain.reshape(1, d_model), ln_bias.reshape(1, d_model),
          jnp.transpose(w_qkv[:, 0], (1, 0, 2)), w_out, w_up, w_down)
        cut = (n_seq, 4, rows // 4, d_model)
        return pl.pallas_call(
            residual_kernel, name="residual", in_specs=[anyspace] * 5, out_specs=anyspace,
            out_shape=hbm(n_seq, rows, d_model),
            scratch_shapes=[pltpu.VMEM(cut, BF16), pltpu.VMEM(cut, BF16), pltpu.VMEM(cut[1:], BF16),
                            pltpu.VMEM(cut[1:], BF16), dma(cut[:2]), dma(cut[:2]), dma(cut[1:2]), dma(cut[1:2]),
                            dma(cut[:2])],
            compiler_params=pltpu.CompilerParams(vmem_limit_bytes=VMEM_LIMIT),
        )(x_blk, outs[0], outs[4], outs[5], outs[6])

    return jax.shard_map(
        local_layer, mesh=mesh,
        in_specs=(P("dp", "tp", None), P(), P(), P(None, "tp", None, None),
                  P("tp", None), P(None, "tp"), P("tp", None)),
        out_specs=P("dp", "tp", None), check_vma=False)
```

```python
import functools

import jax
import jax.numpy as jnp
from jax import lax
from jax.experimental import pallas as pl
from jax.experimental.pallas import tpu as pltpu
from jax.sharding import PartitionSpec as P

LN_EPS = 1e-5
MESH = pl.DeviceIdType.MESH
BF16 = jnp.bfloat16
F32 = jnp.float32
LOG2E = 1.4426950408889634
VMEM_LIMIT = 67_043_328

W_Q, W_K, W_V, UP0, UP1, DN0, DN1, DN2, DN3, OUT = range(10)
PIECES = 10
FAR, MATE, PART, OWN = range(4)
TILE, ATT, UP, DOWN = range(4)
INTER = ("Q2", "Q1", "Q0", "p00", "p01", "D0", "U1", "U0", "p11", "p10", "D3", "D1", "O", "D2", "p20", "p21")
ORDER = ("A00", "A01", "A02", "A03", "T00", "T01", "T02", "T03", "A10", "A11", "U0F", "A12",
         "U0M", "U1M", "A13", "T10", "T11", "T12", "T13", "U0P", "D0F", "U1F", "D0M", "D1M",
         "A20", "A21", "A22", "U1P", "D0P", "D1F", "A23", "T20", "T21", "T22", "T23", "D1P",
         "U2F", "D2F", "U2M", "U2P", "D2M", "U1O", "D2P", "D1O", "U0O", "D0O", "U2O", "D2O",
         )
START = ("pqQ2", "pqQ1", "phQ2", "pqQ0", "phQ1", "rm0", "nm10", "phQ0", "rp00")
BEFORE = {
    0: ("ld00", "ld01"),
    2: ("rp01", "pqD0", "ld02"),
    3: ("phD0", "pqU1", "nm11", "rf0", "ld03", "ln0"),
    4: ("pqU0", "nm20"),
    6: ("phU1", "rm1"),
    7: ("ld10",),
    8: ("phU0", "rp11", "ld11"),
    10: ("rp10", "ln1", "ow0", "lo0"),
    11: ("pqD3", "ld12"),
    12: ("pqD1", "ln2", "lo1"),
    13: ("phD3", "pqO", "rf1", "nm21", "ln3"),
    14: ("ld13",),
    15: ("phD1", "pqD2"),
    17: ("rm2",),
    18: ("phO", "rp20"),
    19: ("phD2", "ln4", "ow1", "lo2", "lo3"),
    20: ("rp21",),
    21: ("ln5", "lo4"),
    22: ("ad0F",),
    23: ("rf2", "ld20"),
    24: ("ld21",),
    25: ("ld22",),
    27: ("lo5",),
    29: ("ld23",),
    30: ("ln6",),
    36: ("ln7", "ow2", "lo6"),
    38: ("ln8", "lo7"),
    39: ("ln9", "lo8"),
    41: ("ln10", "lo9"),
    44: ("ln11", "lo10"),
    45: ("ad2P",),
    46: ("lo11",),
}
ADDS = { 24: "0M", 30: "0P", 31: "1F", 32: "1M", 37: "1P", 39: "2F", 42: "2M", 45: "1O", 47: "0O" }
LAST_ADDS = ("2O",)

KINDS = "ATUD"
BLOCKS = "FMPO"
ITEMS = tuple((int(x[1]), BLOCKS.index(x[2])) for x in ORDER if x[0] == "U")
SLOTS = 4
PIECE = {"Q0": W_Q, "Q1": W_K, "Q2": W_V, "U0": UP0, "U1": UP1,
         "D0": DN0, "D1": DN1, "D2": DN2, "D3": DN3, "O": OUT}


def code_of(step):
    what, s = KINDS.index(step[0]), int(step[1])
    return 16 * what + (4 * s + int(step[2]) if what < UP else ITEMS.index((s, BLOCKS.index(step[2]))))


def pick(values, i, bits):
    per = 30 // bits
    words = [sum(v << bits * p for p, v in enumerate(values[w:w + per])) for w in range(0, len(values), per)]
    word, at = lax.div(i, per), lax.rem(i, per)
    packed = jnp.int32(words[0])
    for w in range(1, len(words)):
        packed = jnp.where(word == w, words[w], packed)
    out = packed
    for p in range(1, per):
        out = jnp.where(at == p, lax.div(packed, 1 << bits * p), out)
    return lax.rem(out, 1 << bits)


def sums():
    seq = []
    for t in range(len(ORDER)):
        seq += [(name[2:], t) for name in BEFORE.get(t, ()) if name[:2] == "ad"]
        if t in ADDS:
            seq.append((ADDS[t], t))
    seq += [(name, None) for name in LAST_ADDS]
    last, before = {}, {}
    for name, _ in seq:
        before[name] = last.get(name[1], -1)
        last[name[1]] = int(name[0])
    assert len(seq) == len(ITEMS)
    return before, last


BEFORE_SUM, LAST_SUM = sums()


def layer_kernel(dims, x, gain, bias, w_qkv, w_out, w_up, w_dn,
                 branch, ng, nout, obuf, ownp, sibin, mid,
                 wq, wu, wd, xt, nt, qk, vt, ot, ho, stage, cin, tbuf, acc, m_s, l_s,
                 w_l, wx_s, wx_r, wf_s, wf_r, nm_s, nm_r, np_s, np_r, nf_s, nf_r, nd_s, nd_r,
                 sp_s, sp_r, op_sem, t_s, t_r, p_s, p_r,
                 ln_sem, xt_sem, oo_sem, nl_sem, ol_sem, cl_sem, br_sem):
    span, rows, d_model, head, ff, chunk, ln_rows, add_rows = dims
    half = rows // 2
    blk = 2 * rows
    scale = LOG2E * head ** -0.5

    g, me = lax.axis_index("dp"), lax.axis_index("tp")
    c, j = lax.div(me, 2), lax.rem(me, 2)
    o = 1 - j
    pair = lax.div(c, 2)
    mate = c + 1 - 2 * lax.rem(c, 2)
    part = 3 - c
    far = 3 - mate
    zb, yb = lax.rem(g, 2), lax.rem(lax.div(g, span), 2)
    gz, gy = g + 1 - 2 * zb, g + span * (1 - 2 * yb)

    def dev(chip, core, group=g):
        return {"dp": group, "tp": 2 * chip + core}

    sib, mt, pt, zd, yd = dev(c, o), dev(mate, j), dev(part, j), dev(c, j, gz), dev(c, j, gy)

    def remote(src, dst, send, recv, to):
        return pltpu.make_async_remote_copy(src_ref=src, dst_ref=dst, send_sem=send, recv_sem=recv,
                                            device_id=to, device_id_type=MESH)

    def row(chip, core, extra=0):
        return pl.multiple_of((2 * chip + core) * rows + extra, half)

    def rowblock(chip):
        return pl.ds(pl.multiple_of(chip * blk, blk), blk)

    quarter = 2 * yb + zb
    q_z, q_y, q_zy = quarter + 1 - 2 * zb, quarter + 2 - 4 * yb, 3 - quarter

    def w_at(piece, q, side, hold):
        n = head // 4 if piece == OUT else ff // 16 if piece >= DN0 else d_model // 8 if piece >= UP0 else d_model // 4
        size = n if side is None else n // 2
        off = q * n + (0 if side is None else side * size)
        if UP0 <= piece <= DN3:
            off = off + (piece - (UP0 if piece <= UP1 else DN0)) * 4 * n
        if hold and DN0 <= piece <= DN3:
            off = off + ff
        if hold and piece == OUT:
            off = off + 2 * ff + head
        at = pl.ds(pl.multiple_of(off, n // 2), size)
        if piece <= W_V:
            return wq.at[piece, at, pl.ds(head, head)] if hold else w_qkv.at[piece, at, :]
        if piece <= UP1:
            return wu.at[at, pl.ds(ff, ff)] if hold else w_up.at[at, :]
        return wd.at[at, :] if hold else (w_out if piece == OUT else w_dn).at[at, :]

    def w_own(i):
        src, dst = ((w_qkv, wq.at[:, :, pl.ds(0, head)]), (w_up, wu.at[:, pl.ds(0, ff)]),
                    (w_dn, wd.at[pl.ds(0, ff), :]), (w_out, wd.at[pl.ds(2 * ff, head), :]))[i]
        return pltpu.make_async_copy(src, dst, w_l.at[i])

    def wx(k):
        return remote(w_at(k, quarter, None, False), w_at(k, quarter, None, True), wx_s.at[k], wx_r.at[k], pt)

    def wx_in(k):
        ref = w_at(k, quarter, None, True)
        return remote(ref, ref, wx_s.at[k], wx_r.at[k], pt)

    def wf(k, i):
        ref = (w_at(k, quarter, None, True) if i < 2 else w_at(k, q_y, 1, True) if i == 2 else w_at(k, q_z, 0, True))
        return remote(ref, ref, wf_s.at[k, i], wf_r.at[k, i], yd if i in (1, 3) else zd)

    def wf_in(k, i):
        ref = w_at(k, (q_z, q_y, q_zy, q_zy)[i], (None, None, 1, 0)[i], True)
        return remote(ref, ref, wf_s.at[k, i], wf_r.at[k, i], yd if i in (1, 3) else zd)

    def pass_quarter(k):
        wx_in(k).wait_recv()
        wf(k, 0).start()
        wf(k, 1).start()

    def pass_halves(k):
        wf_in(k, 0).wait_recv()
        wf_in(k, 1).wait_recv()
        wf(k, 2).start()
        wf(k, 3).start()

    def have(k):
        wf_in(k, 2).wait_recv()
        wf_in(k, 3).wait_recv()

    def own_seq(s):
        return 2 * s + pair

    def other_seq(s):
        return 2 * s + 1 - pair

    def n_own(s):
        return ng.at[s, pl.ds(row(c, j), rows)]

    def nm(s, h):
        ref = ng.at[s, pl.ds(row(c, j, h * half), half)]
        return remote(ref, ref, nm_s.at[s, h], nm_r.at[s, h], mt)

    def nm_in(s, h):
        ref = ng.at[s, pl.ds(row(mate, j, h * half), half)]
        return remote(ref, ref, nm_s.at[s, h], nm_r.at[s, h], mt)

    def np_(s, h):
        return remote(nout.at[s, pl.ds(h * half, half)], ng.at[s, pl.ds(row(c, j, h * half), half)],
                      np_s.at[s, h], np_r.at[s, h], pt)

    def np_in(s, h):
        ref = ng.at[s, pl.ds(row(part, j, h * half), half)]
        return remote(ref, ref, np_s.at[s, h], np_r.at[s, h], pt)

    def nf(s, h):
        ref = ng.at[s, pl.ds(row(part, j, h * half), half)]
        return remote(ref, ref, nf_s.at[s, h], nf_r.at[s, h], mt)

    def nf_in(s, h):
        ref = ng.at[s, pl.ds(row(far, j, h * half), half)]
        return remote(ref, ref, nf_s.at[s, h], nf_r.at[s, h], mt)

    def nd(s, i, core=j):
        ref = (ng.at[s, pl.ds(row(c if i == 0 else mate, core), rows)] if i < 2 else
               ng.at[s, pl.ds(row(part if i < 4 else far, core, (i % 2) * half), half)])
        return remote(ref, ref, nd_s.at[s, i], nd_r.at[s, i], sib)

    def nd_in(s, i):
        return nd(s, i, o)

    def relay_mate(s):
        for h in range(2):
            nm_in(s, h).wait_recv()
        nd(s, 1).start()

    def relay_part(s, h):
        np_in(s, h).wait_recv()
        nf(s, h).start()
        nd(s, 2 + h).start()

    def relay_far(s):
        for h in range(2):
            nf_in(s, h).wait_recv()
            nd(s, 4 + h).start()

    def ln_buf(b):
        return (xt if b < 4 else nt).at[(b // 2) % 2, pl.ds((b % 2) * rows, rows)]

    def ln_load(b):
        return pltpu.make_async_copy(x.at[own_seq(b // 2) if b % 2 else other_seq(b // 2)], ln_buf(b), ln_sem.at[b])

    def ln_store(b):
        return pltpu.make_async_copy(ln_buf(b), n_own(b // 2) if b % 2 else nout.at[b // 2], ln_sem.at[b])

    def normalise(b):
        ln_load(b).wait()
        buf = ln_buf(b)

        def norm(r, _):
            rr = pl.ds(pl.multiple_of(r * ln_rows, ln_rows), ln_rows)
            v = buf[rr, :].astype(F32)
            mean = jnp.mean(v, axis=-1, keepdims=True)
            cen = v - mean
            var = jnp.mean(cen * cen, axis=-1, keepdims=True)
            buf[rr, :] = (cen * lax.rsqrt(var + LN_EPS) * gain[...] + bias[...]).astype(BF16)
            return 0

        lax.fori_loop(0, rows // ln_rows, norm, 0)
        ln_store(b).start()

    barrier = pltpu.get_barrier_semaphore()
    for to in (sib, mt, pt, zd, yd):
        pl.semaphore_signal(barrier, inc=1, device_id=to, device_id_type=MESH)
    for b in range(6):
        ln_load(b).start()
    pl.semaphore_wait(barrier, 5)

    first = next(i for i, name in enumerate(INTER) if name[0] == "p")
    for name in INTER[:first]:
        wx(PIECE[name]).start()
    normalise(0)
    normalise(1)
    begun = set()
    for name in INTER[first:]:
        if name[0] != "p":
            wx(PIECE[name]).start()
            continue
        s, h = int(name[1]), int(name[2])
        if s not in begun:
            if s > 0:
                normalise(2 * s)
                normalise(2 * s + 1)
            ln_store(2 * s).wait()
        np_(s, h).start()
        if s == 0 and s not in begun:
            ln_store(1).wait()
            nm(0, 0).start()
            nm(0, 1).start()
            nd(0, 0).start()
        begun.add(s)
    for s in (1, 2):
        ln_store(2 * s + 1).wait()
        nd(s, 0).start()

    def tile_chip(i):
        return jnp.where(i == 0, c, jnp.where(i == 1, mate, jnp.where(i == 2, part, far)))

    def mlp_chip(kind):
        return jnp.where(kind == FAR, far, jnp.where(kind == MATE, mate, jnp.where(kind == PART, part, c)))

    def tile_copy(s, i):
        return pltpu.make_async_copy(ng.at[s, rowblock(tile_chip(i))], xt.at[lax.rem(i, 2)], xt_sem.at[lax.rem(i, 2)])

    def tile_start(s, i):
        for n in ((0,), (1,), (2, 3), (4, 5))[i]:
            nd_in(s, n).wait_recv()
        tile_copy(s, jnp.int32(i)).start()

    def tile(index):
        s, i = lax.div(index, 4), lax.rem(index, 4)
        tile_copy(s, i).wait()
        slot = lax.rem(i, 2)
        base = rowblock(tile_chip(i))
        for t in range(2):
            qk[base, pl.ds(t * 2 * head, 2 * head)] = jnp.dot(
                xt[slot], wq[t], preferred_element_type=F32).astype(BF16)
        vt[:, base] = jnp.transpose(jnp.dot(xt[slot], wq[2], preferred_element_type=F32)).astype(BF16)

    def dot_t(a, b):
        return lax.dot_general(a, b, (((1,), (1,)), ((), ())), preferred_element_type=F32)

    def o_out(s, i):
        return pltpu.make_async_copy(ot.at[lax.rem(i, 2)], obuf.at[s, rowblock(i)], oo_sem.at[lax.rem(i, 2)])

    def attend(index):
        s, i = lax.div(index, 4), lax.rem(index, 4)
        slot = lax.rem(i, 2)

        @pl.when(i >= 2)
        def _():
            o_out(s, i).wait()

        mine = rowblock(i)
        causal = (lax.broadcasted_iota(jnp.int32, (blk, blk), 0)
                  <= lax.broadcasted_iota(jnp.int32, (blk, blk), 1))
        for h in range(2):
            hd = pl.ds(h * head, head)
            sc = jnp.where(causal, dot_t(qk[mine, pl.ds((2 + h) * head, head)], qk[mine, hd]), -jnp.inf)
            top = jnp.max(sc, axis=0, keepdims=True)
            p = jnp.exp2((sc - top) * scale)
            m_s[h] = top
            l_s[h] = jnp.sum(p, axis=0, keepdims=True)
            acc[h] = jnp.dot(vt[hd, mine], p.astype(BF16), preferred_element_type=F32)

        def earlier(t, _):
            there = rowblock(t)
            for h in range(2):
                hd = pl.ds(h * head, head)
                sc = dot_t(qk[there, pl.ds((2 + h) * head, head)], qk[mine, hd])
                old = m_s[h]
                top = jnp.maximum(old, jnp.max(sc, axis=0, keepdims=True))
                p = jnp.exp2((sc - top) * scale)
                fade = jnp.exp2((old - top) * scale)
                m_s[h] = top
                l_s[h] = l_s[h] * fade + jnp.sum(p, axis=0, keepdims=True)
                acc[h] = acc[h] * fade + jnp.dot(vt[hd, there], p.astype(BF16), preferred_element_type=F32)
            return 0

        lax.fori_loop(0, i, earlier, 0)
        for h in range(2):
            ot[slot, :, pl.ds(h * head, head)] = jnp.transpose(acc[h] * (1.0 / l_s[h])).astype(BF16)
        o_out(s, i).start()

    def context_out(s):
        for i in (2, 3):
            o_out(jnp.int32(s), jnp.int32(i)).wait()

    def sp(s, kind, slot):
        return remote(stage.at[slot, pl.ds(pl.multiple_of(o * rows, rows), rows)], sibin.at[s, kind],
                      sp_s.at[s, kind], sp_r.at[s, kind], sib)

    def own_store(s, kind, slot):
        return pltpu.make_async_copy(stage.at[slot, pl.ds(pl.multiple_of(j * rows, rows), rows)], ownp.at[s, kind],
                                     op_sem.at[slot])

    def to_mate(s, kind):
        return remote(tbuf.at[kind], mid.at[s, kind], t_s.at[s, kind], t_r.at[s, kind], mt)

    def from_mate(s, kind):
        return remote(mid.at[s, kind], mid.at[s, kind], t_s.at[s, kind], t_r.at[s, kind], mt)

    def to_part(s):
        return remote(tbuf.at[PART], branch.at[own_seq(s)], p_s.at[s], p_r.at[s], pt)

    def from_part(s):
        return remote(branch.at[other_seq(s)], branch.at[other_seq(s)], p_s.at[s], p_r.at[s], pt)

    def keep(s):
        return pltpu.make_async_copy(tbuf.at[OWN], branch.at[own_seq(s)], br_sem)

    def sent(s, kind):
        if kind < PART:
            to_mate(s, kind).wait_send()
        elif kind == PART:
            to_part(s).wait_send()
        else:
            keep(s).wait()

    def add_now(name):
        s, kind = jnp.int32(int(name[0])), BLOCKS.index(name[1])
        add_start(s, kind, jnp.int32(BEFORE_SUM[name]))
        add_finish(s, kind)

    def add_loads(s, kind):
        srcs = [ownp.at[s, kind], sibin.at[s, kind]] + ([mid.at[s, kind - PART]] if kind >= PART else [])
        return [pltpu.make_async_copy(src, cin.at[n], cl_sem.at[n]) for n, src in enumerate(srcs)]

    def add_start(s, kind, before):
        remote(sibin.at[s, kind], sibin.at[s, kind], sp_s.at[s, kind], sp_r.at[s, kind], sib).wait_recv()
        if kind >= PART:
            from_mate(s, kind - PART).wait_recv()

        @pl.when(before >= 0)
        def _():
            sent(before, kind)

        for ld in add_loads(s, kind):
            ld.start()

    def add_finish(s, kind):
        for ld in add_loads(s, kind):
            ld.wait()

        def add(r, _):
            rr = pl.ds(pl.multiple_of(r * add_rows, add_rows), add_rows)
            if kind < PART:
                tbuf[kind, rr, :] = cin[0, rr, :] + cin[1, rr, :]
            else:
                tbuf[kind, rr, :] = (cin[0, rr, :].astype(F32) + cin[1, rr, :].astype(F32)
                                     + cin[2, rr, :].astype(F32)).astype(BF16)
            return 0

        lax.fori_loop(0, rows // add_rows, add, 0)
        if kind < PART:
            to_mate(s, kind).start()
        elif kind == PART:
            to_part(s).start()
        else:
            keep(s).start()

    def item(k):
        both = pick([4 * s + b for s, b in ITEMS], k, 4)
        return lax.div(both, 4), lax.rem(both, 4)

    def n_load(k):
        s, kind = item(k)
        return pltpu.make_async_copy(ng.at[s, rowblock(mlp_chip(kind))], nt.at[lax.rem(k, 2)], nl_sem.at[lax.rem(k, 2)])

    def o_load(k):
        s, kind = item(k)
        return pltpu.make_async_copy(obuf.at[s, rowblock(mlp_chip(kind))],
                                     ho.at[lax.rem(k, SLOTS), :, pl.ds(2 * ff, 2 * head)], ol_sem.at[lax.rem(k, SLOTS)])

    def mlp_up(k):
        n_load(k).wait()

        @pl.when(k == 0)
        def _():
            have(UP0)
            have(UP1)
            w_own(1).wait()

        src, dst = lax.rem(k, 2), lax.rem(k, SLOTS)

        def up(t, _):
            cols = pl.ds(pl.multiple_of(t * chunk, chunk), chunk)
            hid = jnp.dot(nt[src], wu[:, cols], preferred_element_type=F32)
            ho[dst, :, cols] = (0.5 * hid * (1.0 + lax.erf(hid * 0.7071067811865476))).astype(BF16)
            return 0

        lax.fori_loop(0, 2 * ff // chunk, up, 0, unroll=True)

    def stage_free(k):
        s, kind = item(k)
        sp(s, kind, lax.rem(k, 2)).wait_send()

    def own_stored(k):
        s, kind = item(k)
        own_store(s, kind, lax.rem(k, 2)).wait()

    def mlp_down(k):
        s, kind = item(k)
        slot, src = lax.rem(k, 2), lax.rem(k, SLOTS)
        o_load(k).wait()

        @pl.when(k == 0)
        def _():
            for p in range(DN0, OUT + 1):
                have(p)
            w_own(2).wait()
            w_own(3).wait()

        @pl.when(k >= 2)
        def _():
            stage_free(k - 2)

        def down(r, size):
            def one(t, _):
                cols = pl.ds(pl.multiple_of(t * chunk, chunk), chunk)
                stage[slot, pl.ds(r, size), cols] = jnp.dot(
                    ho[src, pl.ds(r, size), :], wd[:, cols], preferred_element_type=F32).astype(BF16)
                return 0

            lax.fori_loop(0, d_model // chunk, one, 0, unroll=True)

        split = (k == 0) | (k == len(ITEMS) - 1)

        @pl.when(jnp.logical_not(split))
        def _():
            down(0, blk)
            sp(s, kind, slot).start()

        @pl.when(split)
        def _():
            def part_of(p, _):
                down(pl.multiple_of(jnp.where(p == 0, o, j) * rows, rows), rows)

                @pl.when(p == 0)
                def _():
                    sp(s, kind, slot).start()

                return 0

            lax.fori_loop(0, 2, part_of, 0)

        own_store(s, kind, slot).start()

    def act(name):
        what, arg = name[:2], name[2:]
        if what == "pq":
            pass_quarter(PIECE[arg])
        elif what == "ph":
            pass_halves(PIECE[arg])
        elif what == "rm":
            relay_mate(int(arg))
        elif what == "rp":
            relay_part(int(arg[0]), int(arg[1]))
        elif what == "rf":
            relay_far(int(arg))
        elif what == "ld":
            tile_start(int(arg[0]), int(arg[1]))
        elif what == "nm":
            nm(int(arg[0]), int(arg[1])).start()
        elif what == "ad":
            add_now(arg)
        elif what == "ow":
            context_out(int(arg))
        elif what == "ln":
            n_load(jnp.int32(int(arg))).start()
        else:
            o_load(jnp.int32(int(arg))).start()

    for i in range(4):
        w_own(i).start()
    for name in START:
        act(name)
    w_own(0).wait()
    for k in (W_Q, W_K, W_V):
        have(k)

    codes = [code_of(step) for step in ORDER]

    def add_code(name):
        return 1 + 4 * int(name[0]) + BLOCKS.index(name[1]) + 12 * (1 + BEFORE_SUM[name])

    adds = [add_code(ADDS[t]) if t in ADDS else 0 for t in range(len(ORDER))]

    def adding(code, do):
        @pl.when(code > 0)
        def _():
            which = lax.rem(code - 1, 12)
            for kind in range(4):
                @pl.when(lax.rem(which, 4) == kind)
                def _(kind=kind):
                    do(lax.div(which, 4), kind, lax.div(code - 1, 12) - 1)

    def events(t, lo, hi):
        if not any(p in BEFORE for p in range(lo, hi)):
            return
        if hi - lo == 1:
            for name in BEFORE[lo]:
                act(name)
            return
        half_way = (lo + hi) // 2
        lax.cond(t < half_way, lambda: events(t, lo, half_way), lambda: events(t, half_way, hi))

    def run(t, before):
        events(t, 0, len(ORDER))
        code, add = pick(codes, t, 6), pick(adds, t, 6)
        adding(add, add_start)
        what, index = lax.div(code, 16), lax.rem(code, 16)
        lax.cond(
            what < UP,
            lambda: lax.cond(what == TILE, lambda: tile(index), lambda: attend(index)),
            lambda: lax.cond(what == UP, lambda: mlp_up(index), lambda: mlp_down(index)))
        adding(add, lambda s, kind, _: add_finish(s, kind))

        @pl.when(lax.div(before, 16) == DOWN)
        def _():
            own_stored(lax.rem(before, 16))

        return code

    lax.fori_loop(0, len(ORDER), run, jnp.int32(0))
    own_stored(jnp.int32(len(ITEMS) - 1))
    for name in LAST_ADDS:
        add_now(name)
    for k in range(len(ITEMS) - 2, len(ITEMS)):
        stage_free(jnp.int32(k))
    for s in range(3):
        for h in range(2):
            nm(s, h).wait_send()
            np_(s, h).wait_send()
            nf(s, h).wait_send()
        for i in range(6):
            nd(s, i).wait_send()
    for k in range(PIECES):
        wx(k).wait_send()
        for i in range(4):
            wf(k, i).wait_send()
    for s in range(3):
        from_part(s).wait_recv()
    for name, s in LAST_SUM.items():
        sent(s, BLOCKS.index(name))


def residual_kernel(x, branch, y, xv, bv, x_sem, b_sem, y_sem):
    parts, step = xv.shape[0], min(64, xv.shape[1])

    def loads(p):
        return (pltpu.make_async_copy(x.at[p], xv.at[p], x_sem.at[p]),
                pltpu.make_async_copy(branch.at[p], bv.at[p], b_sem.at[p]))

    def store(p):
        return pltpu.make_async_copy(xv.at[p], y.at[p], y_sem.at[p])

    for p in range(parts):
        for ld in loads(p):
            ld.start()

    def add(p, _):
        for ld in loads(p):
            ld.wait()
        for r in range(0, xv.shape[1], step):
            rr = pl.ds(r, step)
            xv[p, rr, :] = (xv[p, rr, :].astype(F32) + bv[p, rr, :].astype(F32)).astype(BF16)
        store(p).start()
        return 0

    lax.fori_loop(0, parts, add, 0)
    for p in range(parts):
        store(p).wait()


def neighbour_span(groups):
    short = 1
    while short * short * 4 <= groups:
        short *= 2
    return groups // short


def solution(mesh):
    tp, groups = mesh.shape["tp"], mesh.shape["dp"]
    span = neighbour_span(groups)
    assert tp == 8 and groups % (2 * span) == 0 and span % 2 == 0

    def local_layer(x_blk, ln_gain, ln_bias, w_qkv, w_out, w_up, w_down):
        n_seq, rows, d_model = x_blk.shape
        head = w_qkv.shape[3]
        ff = w_up.shape[1]
        ns, seq, blk = n_seq // 2, rows * tp, 2 * rows
        assert ns == 3 and w_qkv.shape[1:3] == (1, 3)
        chunk = min(512, d_model, ff)
        ln_rows, add_rows = min(64, rows // 2), min(16, rows // 2)
        dims = (span, rows, d_model, head, ff, chunk, ln_rows, add_rows)
        dma = pltpu.SemaphoreType.DMA
        anyspace = pl.BlockSpec(memory_space=pl.ANY)
        vmem = pl.BlockSpec(memory_space=pltpu.VMEM)

        def hbm(*shape):
            return jax.ShapeDtypeStruct(shape, BF16)

        outs = pl.pallas_call(
            functools.partial(layer_kernel, dims),
            name="layer",
            out_shape=(hbm(n_seq, rows, d_model), hbm(ns, seq, d_model), hbm(ns, rows, d_model), hbm(ns, seq, 2 * head),
                       hbm(ns, 4, rows, d_model), hbm(ns, 4, rows, d_model), hbm(ns, 2, rows, d_model)),
            in_specs=[anyspace, vmem, vmem, anyspace, anyspace, anyspace, anyspace],
            out_specs=(anyspace,) * 7,
            scratch_shapes=[
                pltpu.VMEM((3, d_model, 2 * head), BF16),
                pltpu.VMEM((d_model, 2 * ff), BF16),
                pltpu.VMEM((2 * ff + 2 * head, d_model), BF16),
                pltpu.VMEM((2, blk, d_model), BF16),
                pltpu.VMEM((2, blk, d_model), BF16),
                pltpu.VMEM((seq, 4 * head), BF16),
                pltpu.VMEM((2 * head, seq), BF16),
                pltpu.VMEM((2, blk, 2 * head), BF16),
                pltpu.VMEM((SLOTS, blk, 2 * ff + 2 * head), BF16),
                pltpu.VMEM((2, blk, d_model), BF16),
                pltpu.VMEM((3, rows, d_model), BF16),
                pltpu.VMEM((4, rows, d_model), BF16),
                pltpu.VMEM((2, head, blk), F32),
                pltpu.VMEM((2, 1, blk), F32),
                pltpu.VMEM((2, 1, blk), F32),
                dma((4,)), dma((PIECES,)), dma((PIECES,)), dma((PIECES, 4)), dma((PIECES, 4)),
                dma((ns, 2)), dma((ns, 2)), dma((ns, 2)), dma((ns, 2)), dma((ns, 2)), dma((ns, 2)),
                dma((ns, 6)), dma((ns, 6)),
                dma((ns, 4)), dma((ns, 4)), dma((2,)), dma((ns, 2)), dma((ns, 2)), dma((ns,)), dma((ns,)),
                dma((6,)), dma((2,)), dma((2,)), dma((2,)), dma((SLOTS,)), dma((3,)), dma,
            ],
            compiler_params=pltpu.CompilerParams(
                collective_id=0, has_side_effects=True, vmem_limit_bytes=VMEM_LIMIT),
        )(x_blk, ln_gain.reshape(1, d_model), ln_bias.reshape(1, d_model),
          jnp.transpose(w_qkv[:, 0], (1, 0, 2)), w_out, w_up, w_down)
        cut = (4 * n_seq, rows // 4, d_model)
        y = pl.pallas_call(
            residual_kernel, name="residual", in_specs=[anyspace, anyspace], out_specs=anyspace,
            out_shape=hbm(*cut),
            scratch_shapes=[pltpu.VMEM(cut, BF16), pltpu.VMEM(cut, BF16), dma(cut[:1]), dma(cut[:1]), dma(cut[:1])],
            compiler_params=pltpu.CompilerParams(vmem_limit_bytes=VMEM_LIMIT),
        )(x_blk.reshape(cut), outs[0].reshape(cut))
        return y.reshape(n_seq, rows, d_model)

    return jax.shard_map(
        local_layer, mesh=mesh,
        in_specs=(P("dp", "tp", None), P(), P(), P(None, "tp", None, None),
                  P("tp", None), P(None, "tp"), P("tp", None)),
        out_specs=P("dp", "tp", None), check_vma=False)
```
